128 devices in a mesh: data: 1, row: 2 (over core), col: 64 (over z, y, x).
Axes of the slice: x: 4, y: 4, z: 4, core: 2. Of those that a mesh axis runs over, the one named last changes fastest.
Arguments:
- tokens: bfloat16 [16384, 2048], P(('data', 'row', 'col'))
- expert_ids: int32 [16384, 8], P(('data', 'row', 'col'))
- gate_weights: float32 [16384, 8], P(('data', 'row', 'col'))
- w_in: bfloat16 [128, 2048, 768], P(('row', 'col'))
- w_out: bfloat16 [128, 768, 2048], P(('row', 'col'))
Outputs:
- output: bfloat16 [16384, 2048], P(('data', 'row', 'col'))
All inputs are finite; a program needn't handle non-finite values.
Results may differ from the reference program's by a relative error of at most 0.00451473.
Values are sent between devices in bfloat16 or wider.
A program may use at most 1 GiB of HBM per device.

```python
import jax
import jax.numpy as jnp
from jax import lax

D = 2048
FF = 768
EXPERTS = 128
TOP = 8
TOK_DEV = 128
ROW = 2
COL = 64
GROUP = ROW * COL
TOKENS = GROUP * TOK_DEV
CAP = TOKENS * TOP // EXPERTS
AVG_LOAD = TOK_DEV * TOP // EXPERTS


def draw_routing(base_key):
    key_split, key_device = jax.random.split(base_key)
    shuffled = jax.random.permutation(key_split, EXPERTS)
    hot_set = shuffled[: EXPERTS // 2]
    cold_set = shuffled[EXPERTS // 2:]

    def one_device(device_index):
        device_key = jax.random.fold_in(key_device, device_index)
        key_shift, key_order, key_rows = jax.random.split(device_key, 3)
        shift_by = jax.random.randint(key_shift, (EXPERTS // 2,), 0, AVG_LOAD + 1)
        shift_by = shift_by.at[0].set(AVG_LOAD)
        counts = jnp.zeros((EXPERTS,), jnp.int32)
        counts = counts.at[hot_set].set(AVG_LOAD + shift_by).at[cold_set].set(AVG_LOAD - shift_by)
        expert_order = jax.random.permutation(key_order, EXPERTS)
        run_end = jnp.cumsum(counts[expert_order])
        position = jnp.arange(TOK_DEV * TOP)
        run_index = jnp.searchsorted(run_end, position, side='right')
        id_table = expert_order[run_index].reshape(TOP, TOK_DEV).T
        row_order = jax.random.permutation(key_rows, TOK_DEV)
        return id_table[row_order]

    return lax.map(one_device, jnp.arange(GROUP)).reshape(TOKENS, TOP).astype(jnp.int32)


def setup_inputs(seed: int = 0, part: int = 0) -> dict:
    base_key = jax.random.key(seed)
    key_tok, key_ids, key_gate, key_in, key_out = jax.random.split(base_key, 5)
    tokens = jax.random.normal(jax.random.fold_in(key_tok, part), (TOKENS, D), jnp.float32)
    expert_ids = draw_routing(jax.random.fold_in(key_ids, part))
    gate_weights = jax.random.uniform(jax.random.fold_in(key_gate, part), (TOKENS, TOP), jnp.float32, 0.25, 1.25) * TOP ** -0.5
    w_in = jax.random.normal(key_in, (EXPERTS, D, FF), jnp.float32) * D ** -0.5
    w_out = jax.random.normal(key_out, (EXPERTS, FF, D), jnp.float32) * FF ** -0.5
    return {'tokens': tokens.astype(jnp.bfloat16), 'expert_ids': expert_ids, 'gate_weights': gate_weights, 'w_in': w_in.astype(jnp.bfloat16), 'w_out': w_out.astype(jnp.bfloat16)}


def reference(tokens, expert_ids, gate_weights, w_in, w_out):
    flat_ids = expert_ids.reshape(-1)
    pair_count = flat_ids.shape[0]
    sort_order = jnp.argsort(flat_ids, stable=True)
    counts = jnp.bincount(flat_ids, length=EXPERTS)
    starts = jnp.cumsum(counts) - counts
    sorted_rank = jnp.arange(pair_count) - starts[flat_ids[sort_order]]
    pair_rank = jnp.zeros((pair_count,), jnp.int32).at[sort_order].set(sorted_rank)
    slot_of_pair = jnp.where(pair_rank < CAP, flat_ids * CAP + pair_rank, EXPERTS * CAP)
    token_of_pair = jnp.arange(pair_count) // TOP
    slot_token = jnp.full((EXPERTS * CAP,), TOKENS, jnp.int32).at[slot_of_pair].set(token_of_pair, mode='drop')
    padded = jnp.concatenate([tokens, jnp.zeros((1, D), tokens.dtype)], axis=0)

    def expert_ffn(operands):
        rows_index, w_first, w_second = operands
        buffer = padded[rows_index]
        hidden = jax.nn.gelu(jnp.dot(buffer, w_first, preferred_element_type=jnp.float32)).astype(jnp.bfloat16)
        return jnp.dot(hidden, w_second, preferred_element_type=jnp.float32).astype(jnp.bfloat16)

    expert_out = lax.map(expert_ffn, (slot_token.reshape(EXPERTS, CAP), w_in, w_out))
    out_pad = jnp.concatenate([expert_out.reshape(EXPERTS * CAP, D), jnp.zeros((1, D), expert_out.dtype)], axis=0)

    def combine(operands):
        block_tok, block_slot, block_gate = operands
        gathered = out_pad[block_slot]
        weighted = jnp.einsum('tk,tkd->td', block_gate.astype(jnp.float32), gathered.astype(jnp.float32))
        return (block_tok.astype(jnp.float32) + weighted).astype(jnp.bfloat16)

    layer_out = lax.map(combine, (tokens.reshape(GROUP, TOK_DEV, D), slot_of_pair.reshape(GROUP, TOK_DEV, TOP), gate_weights.reshape(GROUP, TOK_DEV, TOP)))
    return layer_out.reshape(TOKENS, D)
```

```python
import functools

import jax
import jax.numpy as jnp
from jax import lax
from jax.experimental import pallas as pl
from jax.experimental.pallas import tpu as pltpu
from jax.sharding import PartitionSpec as P

GRID_AXES = ('row', 'col')
F32 = jnp.float32
BF16 = jnp.bfloat16
I32 = jnp.int32


def kernel(side, cap, slots, tokens_ref, ids_ref, gates_ref, w_in_hbm, w_out_hbm, out_ref,
           w_in, w_out, send, recv, outs, ret, cnt_mine, cnt_all, rank_k, rank_e, gate3, acc,
           w_sem, send_sem, back_sem, cnt_send_sem, cnt_recv_sem, recv_sems, ret_sems):
    plane = side * side
    group = plane
    groups = 2 * side
    n = plane * side * 2
    log = side.bit_length() - 1
    tok, width = tokens_ref.shape
    rows = group * slots
    top = ids_ref.shape[1]

    data = lax.axis_index('data')
    core = lax.axis_index('row')
    col = lax.axis_index('col')
    cz = lax.div(col, plane)
    cy = lax.rem(lax.div(col, side), side)
    cx = lax.rem(col, side)
    me = core * (plane * side) + col

    def steps(k):
        j, m = lax.div(k, group), lax.rem(k, group)
        dc, jj = lax.div(j, side), lax.rem(j, side)
        dy, dx = lax.div(m, side), lax.rem(m, side)
        dz = lax.rem(jj + dx + dy, side)
        return dc, dz, dy, dx

    def ahead(k):
        dc, dz, dy, dx = steps(k)
        to = lax.rem(cz + dz, side) * plane + lax.rem(cy + dy, side) * side + lax.rem(cx + dx, side)
        return (data, lax.rem(core + dc, 2), to)

    def behind(k):
        dc, dz, dy, dx = steps(k)
        to = (lax.rem(cz + side - dz, side) * plane + lax.rem(cy + side - dy, side) * side
              + lax.rem(cx + side - dx, side))
        return (data, lax.rem(core + dc, 2), to)

    def expert_of(k):
        j, m = k >> (2 * log), k & (group - 1)
        dc, jj = j >> log, j & (side - 1)
        dy, dx = m >> log, m & (side - 1)
        dz = (jj + dx + dy) & (side - 1)
        to = ((cz + dz) & (side - 1)) * plane + ((cy + dy) & (side - 1)) * side + ((cx + dx) & (side - 1))
        return ((core + dc) & 1) * (plane * side) + to

    def iota(shape, dim):
        return lax.broadcasted_iota(I32, shape, dim)

    load_in = pltpu.make_async_copy(w_in_hbm, w_in, w_sem.at[0])
    load_out = pltpu.make_async_copy(w_out_hbm, w_out, w_sem.at[1])
    load_in.start()
    load_out.start()

    lane = iota((tok, n), 1)
    chosen = jnp.zeros((tok, n), F32)
    gates = jnp.zeros((tok, n), F32)
    for j in range(top):
        hit = ids_ref[:, j:j + 1] == lane
        chosen = jnp.where(hit, 1.0, chosen)
        gates = jnp.where(hit, gates_ref[:, j:j + 1], gates)
    cnt_mine[...] = jnp.sum(chosen, axis=0, keepdims=True).astype(I32)
    cnt_all[pl.ds(me, 1)] = cnt_mine[...][None]

    @pl.loop(1, n)
    def _(k):
        pltpu.make_async_remote_copy(cnt_mine, cnt_all.at[me], cnt_send_sem, cnt_recv_sem,
                                     device_id=ahead(k), device_id_type=pl.DeviceIdType.MESH).start()

    earlier = (iota((tok, tok), 1) < iota((tok, tok), 0)).astype(BF16)
    rank = jnp.dot(earlier, chosen.astype(BF16), preferred_element_type=F32)
    rank = jnp.where(chosen > 0, rank, -1.0)
    rank_e[...] = rank
    gate3[...] = gates
    order = (expert_of(iota((n, n), 0)) == iota((n, n), 1)).astype(BF16)
    rank_k[...] = lax.dot_general(order, rank.astype(BF16), (((1,), (1,)), ((), ())), preferred_element_type=F32)

    def block_copy(k):
        return pltpu.make_async_remote_copy(send.at[k], recv.at[k], send_sem, recv_sems.at[lax.div(k, group)],
                                            device_id=ahead(k), device_id_type=pl.DeviceIdType.MESH)

    def back_copy(k):
        return pltpu.make_async_remote_copy(outs.at[k], ret.at[k], back_sem, ret_sems.at[lax.div(k, group)],
                                            device_id=behind(k), device_id_type=pl.DeviceIdType.MESH)

    @pl.loop(0, groups)
    def _(j):
        first = j * group
        place = rank_k[pl.ds(first, group), :]
        pick = place[:, None, :] == iota((group, slots, tok), 1).astype(F32)
        pick = jnp.where(pick, 1.0, 0.0).reshape(rows, tok).astype(BF16)
        picked = jnp.dot(pick, tokens_ref[...], preferred_element_type=F32).astype(BF16)
        send[pl.ds(first, group)] = picked.reshape(group, slots, width)

        @pl.loop(jnp.where(j == 0, 1, first), first + group)
        def _(k):
            block_copy(k).start()

    recv[0] = send[0]
    load_in.wait()
    load_out.wait()

    def wait_group(buf, sem, first, count):
        part = buf.at[pl.ds(first, count)]
        pltpu.make_async_copy(part, part, sem).wait()

    def expert(j):
        first = j * group
        x = recv[pl.ds(first, group)].reshape(rows, width)
        hidden = jax.nn.gelu(jnp.dot(x, w_in[...], preferred_element_type=F32)).astype(BF16)
        o = jnp.dot(hidden, w_out[...], preferred_element_type=F32).astype(BF16)
        outs[pl.ds(first, group)] = o.reshape(group, slots, width)

        @pl.loop(jnp.where(j == 0, 1, first), first + group)
        def _(k):
            back_copy(k).start()

    @pl.loop(0, groups)
    def _(j):
        @pl.when(j == 0)
        def _():
            wait_group(recv, recv_sems.at[0], 1, group - 1)

        @pl.when(j > 0)
        def _():
            wait_group(recv, recv_sems.at[j], j * group, group)

        expert(j)

    ret[0] = outs[0]

    wait_group(cnt_all, cnt_recv_sem, 0, n - 1)
    seen = jnp.where(iota((n, 1, n), 0) < me, cnt_all[...], 0)
    before = jnp.sum(seen, axis=0).astype(F32)
    room = jnp.clip(cap - before, 0.0, float(slots))
    rank = rank_e[...]
    rank = jnp.where(rank < room, rank, -1.0)
    gates = gate3[...]
    high = gates.astype(BF16)
    left = gates - high.astype(F32)
    mid = left.astype(BF16)
    low = (left - mid.astype(F32)).astype(BF16)
    parts = jnp.concatenate([high, mid, low], axis=0)
    rank = rank.astype(BF16)
    room_col = jnp.broadcast_to(room, (n, n)).T.astype(BF16)

    acc[...] = tokens_ref[...].astype(F32)

    def combine(j):
        first = j * group
        spread = (expert_of(first + iota((n, rows), 1) // slots) == iota((n, rows), 0)).astype(BF16)
        at = jnp.dot(rank, spread, preferred_element_type=F32)
        here = at == (iota((tok, rows), 1) % slots).astype(F32)
        scale = jnp.dot(parts, spread, preferred_element_type=F32)
        here3 = jnp.concatenate([here.astype(F32)] * 3, axis=0)
        scale = (scale * here3).astype(BF16)
        fits = lax.dot_general(spread, room_col, (((0,), (0,)), ((), ())), preferred_element_type=F32)
        fits = (iota((rows, n), 0) % slots).astype(F32) < fits
        got = ret[pl.ds(first, group)].reshape(rows, width)
        got = jnp.where(fits[:, :1], got, jnp.zeros_like(got))
        mixed = jnp.dot(scale, got, preferred_element_type=F32)
        acc[...] += mixed[:tok] + (mixed[tok:2 * tok] + mixed[2 * tok:])

    @pl.loop(0, groups)
    def _(j):
        @pl.when(j == 0)
        def _():
            wait_group(ret, ret_sems.at[0], 1, group - 1)

        @pl.when(j > 0)
        def _():
            wait_group(ret, ret_sems.at[j], j * group, group)

        combine(j)

    out_ref[...] = acc[...].astype(BF16)
    wait_group(send, send_sem, 1, n - 1)
    wait_group(outs, back_sem, 1, n - 1)

    @pl.loop(1, n)
    def _(k):
        pltpu.make_async_copy(cnt_mine, cnt_mine, cnt_send_sem).wait()


def solution(mesh):
    group_size = mesh.shape['row'] * mesh.shape['col']
    side = round(mesh.shape['col'] ** (1 / 3))

    def device_fn(tokens, expert_ids, gate_weights, w_in, w_out):
        tok, width = tokens.shape
        top = expert_ids.shape[1]
        ff = w_in.shape[2]
        n = group_size
        cap = tok * top
        slots = 2 * tok * top // n
        groups, group = 2 * side, side * side
        vmem = pl.BlockSpec(memory_space=pltpu.VMEM)
        anyspace = pl.BlockSpec(memory_space=pl.ANY)
        blocks = pltpu.VMEM((n, slots, width), BF16)
        return pl.pallas_call(
            functools.partial(kernel, side, cap, slots),
            out_shape=jax.ShapeDtypeStruct((tok, width), BF16),
            in_specs=[vmem, vmem, vmem, anyspace, anyspace],
            out_specs=vmem,
            scratch_shapes=[
                pltpu.VMEM((width, ff), BF16),
                pltpu.VMEM((ff, width), BF16),
                blocks, blocks, blocks, blocks,
                pltpu.VMEM((1, n), I32),
                pltpu.VMEM((n, 1, n), I32),
                pltpu.VMEM((n, tok), F32),
                pltpu.VMEM((tok, n), F32),
                pltpu.VMEM((tok, n), F32),
                pltpu.VMEM((tok, width), F32),
                pltpu.SemaphoreType.DMA((2,)),
                pltpu.SemaphoreType.DMA,
                pltpu.SemaphoreType.DMA,
                pltpu.SemaphoreType.DMA,
                pltpu.SemaphoreType.DMA,
                pltpu.SemaphoreType.DMA((groups,)),
                pltpu.SemaphoreType.DMA((groups,)),
            ],
            compiler_params=pltpu.CompilerParams(has_side_effects=True, vmem_limit_bytes=60 * 1024 * 1024),
            name='expert_layer',
        )(tokens, expert_ids, gate_weights, w_in.reshape(width, ff), w_out.reshape(ff, width))

    token_spec = P(('data', 'row', 'col'), None)
    expert_spec = P(GRID_AXES, None, None)
    return jax.shard_map(device_fn, mesh=mesh, in_specs=(token_spec, token_spec, token_spec, expert_spec, expert_spec), out_specs=token_spec, check_vma=False)
```

```python
import functools

import jax
import jax.numpy as jnp
from jax import lax
from jax.experimental import pallas as pl
from jax.experimental.pallas import tpu as pltpu
from jax.sharding import PartitionSpec as P

GRID_AXES = ('row', 'col')
F32 = jnp.float32
BF16 = jnp.bfloat16
I32 = jnp.int32
SIDE = 4
N = 2 * SIDE ** 3
MESH = pl.DeviceIdType.MESH
Z, Y, X = 0, 1, 2
AXES = ((Z, Y, X), (Y, X, Z), (X, Z, Y))


def iota(shape, dim):
    return lax.broadcasted_iota(I32, shape, dim)


def kernel(cols, cap, slots, tokens_ref, ids_ref, gates_ref, ids_t_ref, w_in_hbm, w_out_hbm, out_ref,
           w_in, w_out, tok0, tok1, tok2, blk0, blk1, blk2, recv, ret, ids_all, places,
           cnt_mine, cnt_all, rank_e, gate_e, acc,
           w_sem, ids_send, ids_recv, cnt_send, cnt_recv, tok_send_a, tok_send_b, tok_recv, blk_send, blk_recv, back_send, ret_recv):
    toks, blks = (tok0, tok1, tok2), (blk0, blk1, blk2)
    tok, width = tokens_ref.shape
    top = ids_ref.shape[1]
    data = lax.axis_index('data')
    core = lax.axis_index('row')
    col = lax.axis_index('col')
    here = (lax.div(col, 16), lax.rem(lax.div(col, 4), 4), lax.rem(col, 4))
    me = core * 64 + col

    def device(d_core, d):
        at = [lax.rem(here[a] + d[a], 4) if a in d else here[a] for a in range(3)]
        return (data, lax.rem(core + d_core, 2), at[0] * 16 + at[1] * 4 + at[2])

    def part(p):
        return pl.ds(cols[p][0], cols[p][1])

    load_in = pltpu.make_async_copy(w_in_hbm, w_in, w_sem.at[0])
    load_out = pltpu.make_async_copy(w_out_hbm, w_out, w_sem.at[1])

    cnt_lane = iota((tok, N), 1)
    chosen = jnp.zeros((tok, N), F32)
    gates = jnp.zeros((tok, N), F32)
    for j in range(top):
        hit = ids_ref[:, j:j + 1] == cnt_lane
        chosen = jnp.where(hit, 1.0, chosen)
        gates = jnp.where(hit, gates_ref[:, j:j + 1], gates)
    cnt_mine[...] = jnp.sum(chosen, axis=0, keepdims=True).astype(I32)
    cnt_all[pl.ds(me, 1)] = cnt_mine[...][None]

    for p in range(3):
        d1, d2, d3 = AXES[p]

        @pl.loop(1, 16)
        def _(i):
            pltpu.make_async_remote_copy(
                ids_t_ref, ids_all.at[p, i], ids_send.at[p], ids_recv.at[p],
                device_id=device(0, {d2: lax.div(i, 4), d1: lax.rem(i, 4)}), device_id_type=MESH).start()

    def token_copy(p, src, dst, sem, axis, step, send_sem):
        return pltpu.make_async_remote_copy(src, dst, send_sem.at[p], sem, device_id=device(0, {axis: step}), device_id_type=MESH)

    for p in range(3):
        mine = tokens_ref.at[:, part(p)]
        for step in (1, 3):
            token_copy(p, mine, toks[p].at[0, step], tok_recv.at[p, step], AXES[p][0], step, tok_send_a).start()

    def gather_on(p, a, src):
        for step in (1, 3):
            token_copy(p, src, toks[p].at[step, a], tok_recv.at[p, 4 * step + a], AXES[p][1], step, tok_send_b).start()

    for p in range(3):
        gather_on(p, 0, tokens_ref.at[:, part(p)])

    @pl.loop(1, N)
    def _(k):
        pltpu.make_async_remote_copy(
            cnt_mine, cnt_all.at[me], cnt_send, cnt_recv,
            device_id=device(lax.div(k, 64), {Z: lax.rem(lax.div(k, 16), 4), Y: lax.rem(lax.div(k, 4), 4), X: lax.rem(k, 4)}),
            device_id_type=MESH).start()

    load_in.start()
    load_out.start()

    def wait_for(ref, sem):
        pltpu.make_async_copy(ref, ref, sem).wait()

    def arrived(p, b, a):
        wait_for(toks[p].at[b, a], tok_recv.at[p, 4 * b + a])

    for p in range(3):
        toks[p][0, 0] = tokens_ref[:, part(p)]
        ids_all[p, 0] = ids_t_ref[...]

    earlier = (iota((tok, tok), 1) < iota((tok, tok), 0)).astype(BF16)
    rank = jnp.dot(earlier, chosen.astype(BF16), preferred_element_type=F32)
    rank_e[...] = jnp.where(chosen > 0, rank, -1.0)
    gate_e[...] = gates

    half = tok // 2
    for p in range(3):
        t = toks[p]
        for step, rows in ((1, pl.ds(0, half)), (3, pl.ds(half, half))):
            arrived(p, 0, step)
            token_copy(p, t.at[0, step, rows], t.at[0, 2, rows], tok_recv.at[p, 2], AXES[p][0], step, tok_send_a).start()
            gather_on(p, step, t.at[0, step])

    later = (iota((tok, tok), 0) < iota((tok, tok), 1)).astype(BF16)
    for p in range(3):
        d1, d2, d3 = AXES[p]
        wait_for(ids_all.at[p, pl.ds(1, 15)], ids_recv.at[p])
        dest = iota((8, tok), 0)
        weight = (16, 4, 1)[d3]
        expert = (((core + (dest >> 2)) & 1) * 64 + col + (((here[d3] + (dest & 3)) & 3) - here[d3]) * weight)[None]
        mark = jnp.zeros((16, 8, tok), F32)
        for j in range(top):
            mark = jnp.where(ids_all[p, :, j:j + 1, :] == expert, 1.0, mark)
        mark = mark.reshape(128, tok)
        place = jnp.dot(mark.astype(BF16), later, preferred_element_type=F32)
        places[p] = jnp.where(mark > 0, place, -1.0)

    for p in range(3):
        arrived(p, 0, 2)
        gather_on(p, 2, toks[p].at[0, 2])

    def where_in(p, d_core, s1, s2, s3):
        at = [None] * 3
        for axis, s in zip(AXES[p], (s1, s2, s3)):
            at[axis] = s
        return (d_core, *at)

    def build(p, b):
        t, blk = toks[p], blks[p]

        @pl.loop(0, 4)
        def _(a):
            place = places[p, pl.ds((4 * b + a) * 8, 8), :]
            pick = place[:, None, :] == iota((8, slots, tok), 1).astype(F32)
            pick = jnp.where(pick, 1.0, 0.0).reshape(8 * slots, tok).astype(BF16)
            rows = jnp.dot(pick, t[b, a], preferred_element_type=F32).astype(BF16).reshape(8, slots, cols[p][1])
            blk[b, :, a] = rows
            recv[where_in(p, 0, a, b, 0) + (slice(None), part(p))] = rows[0]

        for h in range(2):
            @pl.loop(1, 8)
            def _(d):
                d_core, s3 = lax.div(d, 4), lax.rem(d, 4)
                high = {AXES[p][0]: h, AXES[p][1]: b // 2, AXES[p][2]: lax.div(s3, 2)}
                cube = high[Z] * 4 + high[Y] * 2 + high[X]
                pltpu.make_async_remote_copy(
                    blk.at[b, d, pl.ds(2 * h, 2)],
                    recv.at[where_in(p, d_core, pl.ds(2 * h, 2), b, s3) + (slice(None), part(p))],
                    blk_send.at[p], blk_recv.at[p, cube],
                    device_id=device(d_core, {AXES[p][2]: s3}), device_id_type=MESH).start()

    for p in range(3):
        build(p, 0)

    for p in range(3):
        t = toks[p]
        for step, pieces in ((1, (0, 1)), (3, (3, 2))):
            for a in pieces:
                arrived(p, step, a)
                token_copy(p, t.at[step, a], t.at[2, a], tok_recv.at[p, 8 + a], AXES[p][1], step, tok_send_b).start()

    for step, rest in ((1, (3, 2)), (3, (0, 1))):
        for p in range(3):
            for a in rest:
                arrived(p, step, a)
            build(p, step)

    load_in.wait()
    load_out.wait()

    def expert(j):
        hz, hy, hx = lax.div(j, 4), lax.rem(lax.div(j, 2), 2), lax.rem(j, 2)
        cube = (slice(None), pl.ds(2 * hz, 2), pl.ds(2 * hy, 2), pl.ds(2 * hx, 2))
        x = recv[cube].reshape(16 * slots, width)
        hidden = jax.nn.gelu(jnp.dot(x, w_in[...], preferred_element_type=F32)).astype(BF16)
        o = jnp.dot(hidden, w_out[...], preferred_element_type=F32).astype(BF16)
        recv[cube] = o.reshape(2, 2, 2, 2, slots, width)

        @pl.loop(jnp.where(j == 0, 1, 0), 16)
        def _(i):
            d_core = lax.div(i, 8)
            sz = 2 * hz + lax.rem(lax.div(i, 4), 2)
            sy = 2 * hy + lax.rem(lax.div(i, 2), 2)
            sx = 2 * hx + lax.rem(i, 2)
            pltpu.make_async_remote_copy(
                recv.at[d_core, sz, sy, sx], ret.at[j * 16 + i], back_send, ret_recv.at[j],
                device_id=device(d_core, {Z: 4 - sz, Y: 4 - sy, X: 4 - sx}), device_id_type=MESH).start()

    def wait_cube(j):
        high = (j // 4, (j // 2) % 2, j % 2)
        for p in range(3):
            near = high[AXES[p][2]] == 0
            wait_for(blks[p].at[0, pl.ds(0, 3 if near else 4)], blk_recv.at[p, j])

    wait_cube(0)
    expert(0)
    ret[0] = recv[0, 0, 0, 0]

    for p in range(3):
        for a in range(4):
            arrived(p, 2, a)
        build(p, 2)

    for j in range(1, 8):
        wait_cube(j)
    pl.loop(1, 8)(expert)

    wait_for(cnt_all.at[pl.ds(0, N - 1)], cnt_recv)
    before = jnp.sum(jnp.where(iota((N, 1, N), 0) < me, cnt_all[...], 0), axis=0).astype(F32)
    room = jnp.clip(cap - before, 0.0, float(slots))
    rank = rank_e[...]
    rank = jnp.where(rank < room, rank, -1.0).astype(BF16)
    gates = gate_e[...]
    high = gates.astype(BF16)
    left = gates - high.astype(F32)
    mid = left.astype(BF16)
    low = (left - mid.astype(F32)).astype(BF16)
    thirds = jnp.concatenate([high, mid, low], axis=0)
    room_col = jnp.broadcast_to(room, (N, N)).T.astype(BF16)
    acc[...] = tokens_ref[...].astype(F32)
    rows = 16 * slots

    def combine(j):
        i = iota((N, rows), 1) // slots
        hz, hy, hx = lax.div(j, 4), lax.rem(lax.div(j, 2), 2), lax.rem(j, 2)
        there = (((core + (i >> 3)) & 1) * 64 + ((here[Z] + 2 * hz + ((i >> 2) & 1)) & 3) * 16
                 + ((here[Y] + 2 * hy + ((i >> 1) & 1)) & 3) * 4 + ((here[X] + 2 * hx + (i & 1)) & 3))
        spread = (there == iota((N, rows), 0)).astype(BF16)
        at = jnp.dot(rank, spread, preferred_element_type=F32)
        hit = (at == (iota((tok, rows), 1) % slots).astype(F32)).astype(F32)
        scale = jnp.dot(thirds, spread, preferred_element_type=F32)
        scale = (scale * jnp.concatenate([hit] * 3, axis=0)).astype(BF16)
        fits = lax.dot_general(spread, room_col, (((0,), (0,)), ((), ())), preferred_element_type=F32)
        fits = (iota((rows, N), 0) % slots).astype(F32) < fits
        got = ret[pl.ds(16 * j, 16)].reshape(rows, width)
        got = jnp.where(fits[:, :1], got, jnp.zeros_like(got))
        mixed = jnp.dot(scale, got, preferred_element_type=F32)
        acc[...] += mixed[:tok] + (mixed[tok:2 * tok] + mixed[2 * tok:])

    @pl.loop(0, 8)
    def _(j):
        @pl.when(j == 0)
        def _():
            wait_for(ret.at[pl.ds(1, 15)], ret_recv.at[0])

        @pl.when(j > 0)
        def _():
            wait_for(ret.at[pl.ds(16 * j, 16)], ret_recv.at[j])

        combine(j)

    out_ref[...] = acc[...].astype(BF16)

    wait_for(ret.at[pl.ds(1, N - 1)], back_send)
    wait_for(cnt_all.at[pl.ds(0, N - 1)], cnt_send)
    for p in range(3):
        wait_for(blks[p].at[:, pl.ds(1, 7)], blk_send.at[p])
        wait_for(ids_all.at[p, pl.ds(1, 15)], ids_send.at[p])
        wait_for(toks[p].at[0, pl.ds(0, 3)], tok_send_a.at[p])
        wait_for(toks[p].at[pl.ds(0, 3)], tok_send_b.at[p])


def solution(mesh):
    def device_fn(tokens, expert_ids, gate_weights, w_in, w_out):
        tok, width = tokens.shape
        top = expert_ids.shape[1]
        ff = w_in.shape[2]
        cap = tok * top
        slots = 2 * tok * top // N
        tiles = width // 128
        sizes = [128 * (tiles // 3 + (1 if p < tiles % 3 else 0)) for p in range(3)]
        cols = [(sum(sizes[:p]), sizes[p]) for p in range(3)]
        vmem = pl.BlockSpec(memory_space=pltpu.VMEM)
        anyspace = pl.BlockSpec(memory_space=pl.ANY)
        dma = pltpu.SemaphoreType.DMA
        return pl.pallas_call(
            functools.partial(kernel, cols, cap, slots),
            out_shape=jax.ShapeDtypeStruct((tok, width), BF16),
            in_specs=[vmem, vmem, vmem, vmem, anyspace, anyspace],
            out_specs=vmem,
            scratch_shapes=[
                pltpu.VMEM((width, ff), BF16),
                pltpu.VMEM((ff, width), BF16),
                *[pltpu.VMEM((4, 4, tok, s), BF16) for s in sizes],
                *[pltpu.VMEM((4, 8, 4, slots, s), BF16) for s in sizes],
                pltpu.VMEM((2, 4, 4, 4, slots, width), BF16),
                pltpu.VMEM((N, slots, width), BF16),
                pltpu.VMEM((3, 16, top, tok), I32),
                pltpu.VMEM((3, 128, tok), F32),
                pltpu.VMEM((1, N), I32),
                pltpu.VMEM((N, 1, N), I32),
                pltpu.VMEM((tok, N), F32),
                pltpu.VMEM((tok, N), F32),
                pltpu.VMEM((tok, width), F32),
                dma((2,)), dma((3,)), dma((3,)), dma, dma, dma((3,)), dma((3,)), dma((3, 16)),
                dma((3,)), dma((3, 8)), dma, dma((8,)),
            ],
            compiler_params=pltpu.CompilerParams(has_side_effects=True, vmem_limit_bytes=62 * 1024 * 1024),
            name='expert_layer',
        )(tokens, expert_ids, gate_weights, expert_ids.T, w_in.reshape(width, ff), w_out.reshape(ff, width))

    token_spec = P(('data', 'row', 'col'), None)
    expert_spec = P(GRID_AXES, None, None)
    return jax.shard_map(device_fn, mesh=mesh, in_specs=(token_spec, token_spec, token_spec, expert_spec, expert_spec), out_specs=token_spec, check_vma=False)
```

```python
import functools

import jax
import jax.numpy as jnp
from jax import lax
from jax.experimental import pallas as pl
from jax.experimental.pallas import tpu as pltpu
from jax.sharding import PartitionSpec as P

GRID_AXES = ('row', 'col')
F32 = jnp.float32
BF16 = jnp.bfloat16
I32 = jnp.int32
SIDE = 4
N = 2 * SIDE ** 3
MESH = pl.DeviceIdType.MESH
Z, Y, X = 0, 1, 2
AXES = ((Z, Y, X), (Y, X, Z), (X, Z, Y))


def iota(shape, dim):
    return lax.broadcasted_iota(I32, shape, dim)


def kernel(cols, cap, slots, tokens_ref, ids_ref, gates_ref, w_in_hbm, w_out_hbm, out_ref,
           w_in, w_out, tok0, tok1, tok2, blk0, blk1, blk2, recv, mid0, mid1, mid2, end0, end1, end2,
           sum0, sum1, sum2, got0, got1, got2, ids_all, gates_all, places, cnt_mine, cnt_all, acc,
           w_sem, ids_send, ids_recv, gate_send, gate_recv, cnt_send, cnt_recv, tok_send_a, tok_send_b, tok_recv,
           blk_send, blk_recv, mid_send, mid_recv, end_send, end_recv, sum_send, sum_recv):
    toks, blks = (tok0, tok1, tok2), (blk0, blk1, blk2)
    mids, ends = (mid0, mid1, mid2), (end0, end1, end2)
    sums, gots = (sum0, sum1, sum2), (got0, got1, got2)
    tok, width = tokens_ref.shape
    top = ids_ref.shape[0]
    data = lax.axis_index('data')
    core = lax.axis_index('row')
    col = lax.axis_index('col')
    here = (lax.div(col, 16), lax.rem(lax.div(col, 4), 4), lax.rem(col, 4))
    me = core * 64 + col
    weight = (16, 4, 1)

    def device(d_core, d):
        at = [lax.rem(here[a] + d[a], 4) if a in d else here[a] for a in range(3)]
        return (data, lax.rem(core + d_core, 2), at[0] * 16 + at[1] * 4 + at[2])

    def number(d_core, d):
        n = ((core + d_core) & 1) * 64
        for a in range(3):
            n = n + (((here[a] + d[a]) & 3) if a in d else here[a]) * weight[a]
        return n

    def part(p):
        return pl.ds(cols[p][0], cols[p][1])

    def send(src, dst, send_sem, recv_sem, to):
        pltpu.make_async_remote_copy(src, dst, send_sem, recv_sem, device_id=to, device_id_type=MESH).start()

    def wait_for(ref, sem):
        pltpu.make_async_copy(ref, ref, sem).wait()

    load_in = pltpu.make_async_copy(w_in_hbm, w_in, w_sem.at[0])
    load_out = pltpu.make_async_copy(w_out_hbm, w_out, w_sem.at[1])

    for p in range(3):
        for step in (1, 3):
            send(tokens_ref.at[:, part(p)], toks[p].at[0, step], tok_send_a.at[p], tok_recv.at[p, step], device(0, {AXES[p][0]: step}))

    mark = jnp.zeros((N, tok), F32)
    for j in range(top):
        mark = jnp.where(ids_ref[j:j + 1, :] == iota((N, tok), 0), 1.0, mark)
    counts = lax.dot_general(jnp.ones((8, tok), BF16), mark.astype(BF16), (((1,), (1,)), ((), ())), preferred_element_type=F32)
    cnt_mine[...] = counts[:1]
    cnt_all[pl.ds(me, 1)] = counts[:1][None]

    @pl.loop(1, N)
    def _(k):
        d = {Z: lax.rem(lax.div(k, 16), 4), Y: lax.rem(lax.div(k, 4), 4), X: lax.rem(k, 4)}
        send(cnt_mine, cnt_all.at[me], cnt_send, cnt_recv, device(lax.div(k, 64), d))

    for p in range(3):
        d1, d2, d3 = AXES[p]

        @pl.loop(1, 16)
        def _(i):
            send(ids_ref, ids_all.at[p, i], ids_send.at[p], ids_recv.at[p], device(0, {d2: lax.div(i, 4), d1: lax.rem(i, 4)}))

        @pl.loop(1, 4)
        def _(i):
            send(gates_ref, gates_all.at[p, i], gate_send.at[p], gate_recv.at[p], device(0, {d1: i}))

    def gather_on(p, a, src):
        for step in (1, 3):
            send(src, toks[p].at[step, a], tok_send_b.at[p], tok_recv.at[p, 4 * step + a], device(0, {AXES[p][1]: step}))

    for p in range(3):
        gather_on(p, 0, tokens_ref.at[:, part(p)])

    load_in.start()
    load_out.start()

    def arrived(p, b, a):
        wait_for(toks[p].at[b, a], tok_recv.at[p, 4 * b + a])

    for p in range(3):
        toks[p][0, 0] = tokens_ref[:, part(p)]
        ids_all[p, 0] = ids_ref[...]
        gates_all[p, 0] = gates_ref[...]

    half = tok // 2
    for p in range(3):
        t = toks[p]
        for step, rows in ((1, pl.ds(0, half)), (3, pl.ds(half, half))):
            arrived(p, 0, step)
            send(t.at[0, step, rows], t.at[0, 2, rows], tok_send_a.at[p], tok_recv.at[p, 2], device(0, {AXES[p][0]: step}))
            gather_on(p, step, t.at[0, step])

    wait_for(cnt_all.at[pl.ds(0, N - 1)], cnt_recv)
    below = (iota((N, N), 1) < iota((N, N), 0)).astype(BF16)
    before = jnp.dot(below, jnp.sum(cnt_all[...], axis=1).astype(BF16), preferred_element_type=F32)
    room = jnp.clip(cap - before, 0.0, float(slots)).astype(BF16)

    later = (iota((tok, tok), 0) < iota((tok, tok), 1)).astype(BF16)
    for p in range(3):
        d1, d2, d3 = AXES[p]
        wait_for(ids_all.at[p, pl.ds(1, 15)], ids_recv.at[p])
        dest = iota((8, tok), 0)
        expert_id = number(dest >> 2, {d3: dest & 3})[None]
        mark = jnp.zeros((16, 8, tok), F32)
        for j in range(top):
            mark = jnp.where(ids_all[p, :, j:j + 1, :] == expert_id, 1.0, mark)
        mark = mark.reshape(128, tok)
        place = jnp.dot(mark.astype(BF16), later, preferred_element_type=F32)
        i = iota((128, N), 0)
        source = number(0, {d2: 4 - (i >> 5), d1: 4 - ((i >> 3) & 3)})
        mine = jnp.dot((source == iota((128, N), 1)).astype(BF16), room, preferred_element_type=F32)
        target = number((i >> 2) & 1, {d3: i & 3})
        mine = jnp.sum(jnp.where(target == iota((128, N), 1), mine, 0.0), axis=1, keepdims=True)
        places[p] = jnp.where((mark > 0) & (place < mine), place, -1.0)

    for p in range(3):
        arrived(p, 0, 2)
        gather_on(p, 2, toks[p].at[0, 2])

    def where_in(p, d_core, s1, s2, s3):
        at = [None] * 3
        for axis, s in zip(AXES[p], (s1, s2, s3)):
            at[axis] = s
        return (d_core, *at)

    def build(p, b):
        t, blk = toks[p], blks[p]

        @pl.loop(0, 4)
        def _(a):
            place = places[p, pl.ds((4 * b + a) * 8, 8), :]
            pick = place[:, None, :] == iota((8, slots, tok), 1).astype(F32)
            pick = jnp.where(pick, 1.0, 0.0).reshape(8 * slots, tok).astype(BF16)
            rows = jnp.dot(pick, t[b, a], preferred_element_type=F32).astype(BF16).reshape(8, slots, cols[p][1])
            blk[b, :, a] = rows
            recv[where_in(p, 0, a, b, 0) + (slice(None), part(p))] = rows[0]

        for h in range(2):
            @pl.loop(1, 8)
            def _(d):
                d_core, s3 = lax.div(d, 4), lax.rem(d, 4)
                high = {AXES[p][0]: h, AXES[p][1]: b // 2, AXES[p][2]: lax.div(s3, 2)}
                cube = high[Z] * 4 + high[Y] * 2 + high[X]
                send(blk.at[b, d, pl.ds(2 * h, 2)],
                     recv.at[where_in(p, d_core, pl.ds(2 * h, 2), b, s3) + (slice(None), part(p))],
                     blk_send.at[p], blk_recv.at[p, cube], device(d_core, {AXES[p][2]: s3}))

    for p in range(3):
        build(p, 0)

    for p in range(3):
        t = toks[p]
        for step, pieces in ((1, (0, 1)), (3, (3, 2))):
            for a in pieces:
                arrived(p, step, a)
                send(t.at[step, a], t.at[2, a], tok_send_b.at[p], tok_recv.at[p, 8 + a], device(0, {AXES[p][1]: step}))

    for step, rest in ((1, (3, 2)), (3, (0, 1))):
        for p in range(3):
            for a in rest:
                arrived(p, step, a)
            build(p, step)

    load_in.wait()
    load_out.wait()

    def halves(j):
        return (lax.div(j, 4), lax.rem(lax.div(j, 2), 2), lax.rem(j, 2))

    def wait_blocks(p, h3, refs, sem):
        @pl.when(h3 == 0)
        def _():
            wait_for(refs.at[0, pl.ds(0, 3)], sem)

        @pl.when(h3 == 1)
        def _():
            wait_for(refs.at[0, pl.ds(0, 4)], sem)

    def expert(j):
        high = halves(j)
        pair = [pl.ds(2 * h, 2) for h in high]
        for p in range(3):
            wait_blocks(p, high[AXES[p][2]], blks[p], blk_recv.at[p, j])
        cube = (slice(None), *pair)
        x = recv[cube].reshape(16 * slots, width)
        hidden = jax.nn.gelu(jnp.dot(x, w_in[...], preferred_element_type=F32)).astype(BF16)
        o = jnp.dot(hidden, w_out[...], preferred_element_type=F32).astype(BF16)
        recv[cube] = o.reshape(2, 2, 2, 2, slots, width)

        for p in range(3):
            d3 = AXES[p][2]
            rest = [pair[a] for a in range(3) if a != d3]

            def along(s3):
                return tuple(s3 if a == d3 else pair[a] for a in range(3))

            @pl.when(high[d3] == 0)
            def _():
                mids[p][(*rest, 0)] = recv[(0, *along(0), slice(None), part(p))]

            @pl.loop(jnp.where(high[d3] == 0, 1, 0), 4)
            def _(i):
                d_core, s3 = lax.div(i, 2), 2 * high[d3] + lax.rem(i, 2)
                send(recv.at[(d_core, *along(s3), slice(None), part(p))], mids[p].at[(*rest, d_core * 4 + s3)],
                     mid_send.at[p], mid_recv.at[p, j], device(d_core, {d3: 4 - s3}))

    def middle(p, s1, s2):
        d1, d2 = AXES[p][:2]
        return (s1, s2) if d1 < d2 else (s2, s1)

    def pass_on(j):
        high = halves(j)
        for p in range(3):
            d1, d2, d3 = AXES[p]

            @pl.when(high[d3] == 1)
            def _():
                wait_blocks(p, 0, blks[p], mid_recv.at[p, j - (4, 2, 1)[d3]])
                wait_blocks(p, 1, blks[p], mid_recv.at[p, j])
                first = pl.ds(2 * high[d1], 2)

                @pl.when(high[d2] == 0)
                def _():
                    ends[p][first, 0] = mids[p][middle(p, first, 0)]

                @pl.loop(jnp.where(high[d2] == 0, 1, 2 * high[d2]), 2 * high[d2] + 2)
                def _(s2):
                    send(mids[p].at[middle(p, first, s2)], ends[p].at[first, s2],
                         end_send.at[p], end_recv.at[p, high[d1]], device(0, {d2: 4 - s2}))

    def combine(p, h):
        d1, d2, d3 = AXES[p]
        e = iota((32, tok), 0)
        expert_id = number((e >> 2) & 1, {d2: e >> 3, d3: e & 3})
        scales = []
        for s1 in (2 * h, 2 * h + 1):
            mark = jnp.zeros((32, tok), F32)
            gate = jnp.zeros((32, tok), F32)
            for j in range(top):
                hit = ids_all[p, s1, j:j + 1, :] == expert_id
                mark = jnp.where(hit, 1.0, mark)
                gate = jnp.where(hit, gates_all[p, s1, j:j + 1, :], gate)
            place = jnp.dot(mark.astype(BF16), later, preferred_element_type=F32)
            place = jnp.where(mark > 0, place, -1.0)
            scale = jnp.where(place[:, None, :] == iota((32, slots, tok), 1).astype(F32), gate[:, None, :], 0.0)
            scale = scale.reshape(32 * slots, tok).T
            high = scale.astype(BF16)
            left = scale - high.astype(F32)
            mid = left.astype(BF16)
            low = (left - mid.astype(F32)).astype(BF16)
            scales.append(jnp.concatenate([high, mid, low], axis=0))
        wait_for(ends[p].at[pl.ds(2 * h, 2), pl.ds(1, 3)], end_recv.at[p, h])
        for s1 in (2 * h, 2 * h + 1):
            rows = ends[p][s1].reshape(32 * slots, cols[p][1])
            mixed = jnp.dot(scales[s1 - 2 * h], rows, preferred_element_type=F32)
            mixed = mixed[:tok] + (mixed[tok:2 * tok] + mixed[2 * tok:])
            if s1 == 0:
                acc[:, part(p)] = tokens_ref[:, part(p)].astype(F32) + mixed
            else:
                sums[p][s1 - 1] = mixed
                send(sums[p].at[s1 - 1], gots[p].at[s1 - 1], sum_send.at[p], sum_recv.at[p, s1 - 1], device(0, {d1: 4 - s1}))

    pl.loop(0, 1)(expert)

    for p in range(3):
        for a in range(4):
            arrived(p, 2, a)
        build(p, 2)

    for p in range(3):
        wait_for(gates_all.at[p, pl.ds(1, 3)], gate_recv.at[p])

    @pl.loop(1, 8)
    def _(j):
        expert(j)
        pass_on(j - 1)

    pl.loop(7, 8)(pass_on)
    for h in range(2):
        for p in range(3):
            combine(p, h)

    for p in range(3):
        total = acc[:, part(p)]
        for i in range(3):
            wait_for(gots[p].at[i], sum_recv.at[p, i])
            total = total + gots[p][i]
        out_ref[:, part(p)] = total.astype(BF16)

    wait_for(cnt_all.at[pl.ds(0, N - 1)], cnt_send)
    for p in range(3):
        wait_for(ids_all.at[p, pl.ds(1, 15)], ids_send.at[p])
        wait_for(gates_all.at[p, pl.ds(1, 3)], gate_send.at[p])
        wait_for(toks[p].at[0, pl.ds(0, 3)], tok_send_a.at[p])
        wait_for(toks[p].at[pl.ds(0, 3)], tok_send_b.at[p])
        wait_for(blks[p].at[:, pl.ds(1, 7)], blk_send.at[p])
        wait_for(mids[p].at[:, :, pl.ds(1, 7)], mid_send.at[p])
        wait_for(ends[p].at[:, pl.ds(1, 3)], end_send.at[p])
        wait_for(sums[p], sum_send.at[p])


def solution(mesh):
    def device_fn(tokens, expert_ids, gate_weights, w_in, w_out):
        tok, width = tokens.shape
        top = expert_ids.shape[1]
        ff = w_in.shape[2]
        cap = tok * top
        slots = 2 * tok * top // N
        tiles = width // 128
        sizes = [128 * (tiles // 3 + (1 if p < tiles % 3 else 0)) for p in range(3)]
        cols = [(sum(sizes[:p]), sizes[p]) for p in range(3)]
        vmem = pl.BlockSpec(memory_space=pltpu.VMEM)
        anyspace = pl.BlockSpec(memory_space=pl.ANY)
        dma = pltpu.SemaphoreType.DMA
        return pl.pallas_call(
            functools.partial(kernel, cols, cap, slots),
            out_shape=jax.ShapeDtypeStruct((tok, width), BF16),
            in_specs=[vmem, vmem, vmem, anyspace, anyspace],
            out_specs=vmem,
            scratch_shapes=[
                pltpu.VMEM((width, ff), BF16),
                pltpu.VMEM((ff, width), BF16),
                *[pltpu.VMEM((4, 4, tok, s), BF16) for s in sizes],
                *[pltpu.VMEM((4, 8, 4, slots, s), BF16) for s in sizes],
                pltpu.VMEM((2, 4, 4, 4, slots, width), BF16),
                *[pltpu.VMEM((4, 4, 8, slots, s), BF16) for s in sizes],
                *[pltpu.VMEM((4, 4, 8, slots, s), BF16) for s in sizes],
                *[pltpu.VMEM((3, tok, s), F32) for s in sizes],
                *[pltpu.VMEM((3, tok, s), F32) for s in sizes],
                pltpu.VMEM((3, 16, top, tok), I32),
                pltpu.VMEM((3, 4, top, tok), F32),
                pltpu.VMEM((3, 128, tok), F32),
                pltpu.VMEM((1, N), F32),
                pltpu.VMEM((N, 1, N), F32),
                pltpu.VMEM((tok, width), F32),
                dma((2,)), dma((3,)), dma((3,)), dma((3,)), dma((3,)), dma, dma, dma((3,)), dma((3,)), dma((3, 16)),
                dma((3,)), dma((3, 8)), dma((3,)), dma((3, 8)), dma((3,)), dma((3, 2)), dma((3,)), dma((3, 3)),
            ],
            compiler_params=pltpu.CompilerParams(has_side_effects=True, vmem_limit_bytes=67043328),
            name='expert_layer',
        )(tokens, expert_ids.T, gate_weights.T, w_in.reshape(width, ff), w_out.reshape(ff, width))

    token_spec = P(('data', 'row', 'col'), None)
    expert_spec = P(GRID_AXES, None, None)
    return jax.shard_map(device_fn, mesh=mesh, in_specs=(token_spec, token_spec, token_spec, expert_spec, expert_spec), out_specs=token_spec, check_vma=False)
```

```python
import functools

import jax
import jax.numpy as jnp
from jax import lax
from jax.experimental import pallas as pl
from jax.experimental.pallas import tpu as pltpu
from jax.sharding import PartitionSpec as P

GRID_AXES = ('row', 'col')
F32 = jnp.float32
BF16 = jnp.bfloat16
I32 = jnp.int32
SIDE = 4
N = 2 * SIDE ** 3
MESH = pl.DeviceIdType.MESH
Z, Y, X = 0, 1, 2
AXES = ((Z, Y, X), (Y, X, Z), (X, Z, Y))


def iota(shape, dim):
    return lax.broadcasted_iota(I32, shape, dim)


def kernel(cols, cap, slots, tokens_ref, ids_ref, gates_ref, w_in_hbm, w_out_hbm, out_ref,
           w_in, w_out, tok0, tok1, tok2, blk0, blk1, blk2, recv, mid0, mid1, mid2, end0, end1, end2,
           sum0, sum1, sum2, got0, got1, got2, ids_all, gates_all, places, scales, cnt_mine, cnt_all, acc,
           w_sem, ids_send, ids_recv, gate_send, gate_recv, cnt_send, cnt_recv, tok_send_a, tok_send_b, tok_recv,
           blk_send, blk_recv, mid_send, mid_recv, end_send, end_recv, sum_send, sum_recv):
    toks, blks = (tok0, tok1, tok2), (blk0, blk1, blk2)
    mids, ends = (mid0, mid1, mid2), (end0, end1, end2)
    sums, gots = (sum0, sum1, sum2), (got0, got1, got2)
    tok, width = tokens_ref.shape
    top = ids_ref.shape[0]
    data = lax.axis_index('data')
    core = lax.axis_index('row')
    col = lax.axis_index('col')
    here = (lax.div(col, 16), lax.rem(lax.div(col, 4), 4), lax.rem(col, 4))
    me = core * 64 + col
    weight = (16, 4, 1)

    def device(d_core, d):
        at = [lax.rem(here[a] + d[a], 4) if a in d else here[a] for a in range(3)]
        return (data, lax.rem(core + d_core, 2), at[0] * 16 + at[1] * 4 + at[2])

    def number(d_core, d):
        n = ((core + d_core) & 1) * 64
        for a in range(3):
            n = n + (((here[a] + d[a]) & 3) if a in d else here[a]) * weight[a]
        return n

    def part(p):
        return pl.ds(cols[p][0], cols[p][1])

    def send(src, dst, send_sem, recv_sem, to):
        pltpu.make_async_remote_copy(src, dst, send_sem, recv_sem, device_id=to, device_id_type=MESH).start()

    def wait_for(ref, sem):
        pltpu.make_async_copy(ref, ref, sem).wait()

    load_in = pltpu.make_async_copy(w_in_hbm, w_in, w_sem.at[0])
    load_out = pltpu.make_async_copy(w_out_hbm, w_out, w_sem.at[1])

    def across(k):
        return device(lax.div(k, 64), {Z: lax.rem(lax.div(k, 16), 4), Y: lax.rem(lax.div(k, 4), 4), X: lax.rem(k, 4)})

    barrier = pltpu.get_barrier_semaphore()

    @pl.loop(1, N)
    def _(k):
        pl.semaphore_signal(barrier, inc=1, device_id=across(k), device_id_type=MESH)

    mark = jnp.zeros((N, tok), F32)
    for j in range(top):
        mark = jnp.where(ids_ref[j:j + 1, :] == iota((N, tok), 0), 1.0, mark)
    counts = lax.dot_general(jnp.ones((8, tok), BF16), mark.astype(BF16), (((1,), (1,)), ((), ())), preferred_element_type=F32)
    cnt_mine[...] = counts[:1]
    cnt_all[pl.ds(me, 1)] = counts[:1][None]
    for p in range(3):
        toks[p][0, 0] = tokens_ref[:, part(p)]
        ids_all[p, 0] = ids_ref[...]
        gates_all[p, 0] = gates_ref[...]
    load_in.start()
    load_out.start()
    pl.semaphore_wait(barrier, N - 1)

    for p in range(3):
        for step in (1, 3):
            send(tokens_ref.at[:, part(p)], toks[p].at[0, step], tok_send_a.at[p], tok_recv.at[p, step], device(0, {AXES[p][0]: step}))

    def gather_on(p, a, src):
        for step in (1, 3):
            send(src, toks[p].at[step, a], tok_send_b.at[p], tok_recv.at[p, 4 * step + a], device(0, {AXES[p][1]: step}))

    for p in range(3):
        gather_on(p, 0, tokens_ref.at[:, part(p)])

    @pl.loop(1, N)
    def _(k):
        send(cnt_mine, cnt_all.at[me], cnt_send, cnt_recv, across(k))

    for p in range(3):
        d1, d2, d3 = AXES[p]

        @pl.loop(1, 16)
        def _(i):
            send(ids_ref, ids_all.at[p, i], ids_send.at[p], ids_recv.at[p], device(0, {d2: lax.div(i, 4), d1: lax.rem(i, 4)}))

        @pl.loop(1, 4)
        def _(i):
            send(gates_ref, gates_all.at[p, i], gate_send.at[p], gate_recv.at[p], device(0, {d1: i}))

    def arrived(p, b, a):
        wait_for(toks[p].at[b, a], tok_recv.at[p, 4 * b + a])

    half = tok // 2
    for p in range(3):
        t = toks[p]
        for step, rows in ((1, pl.ds(0, half)), (3, pl.ds(half, half))):
            arrived(p, 0, step)
            send(t.at[0, step, rows], t.at[0, 2, rows], tok_send_a.at[p], tok_recv.at[p, 2], device(0, {AXES[p][0]: step}))
            gather_on(p, step, t.at[0, step])

    wait_for(cnt_all.at[pl.ds(0, N - 1)], cnt_recv)
    below = (iota((N, N), 1) < iota((N, N), 0)).astype(BF16)
    before = jnp.dot(below, jnp.sum(cnt_all[...], axis=1).astype(BF16), preferred_element_type=F32)
    room = jnp.clip(cap - before, 0.0, float(slots)).astype(BF16)

    later = (iota((tok, tok), 0) < iota((tok, tok), 1)).astype(BF16)
    for p in range(3):
        d1, d2, d3 = AXES[p]
        wait_for(ids_all.at[p, pl.ds(1, 15)], ids_recv.at[p])
        dest = iota((8, tok), 0)
        expert_id = number(dest >> 2, {d3: dest & 3})[None]
        mark = jnp.zeros((16, 8, tok), F32)
        for j in range(top):
            mark = jnp.where(ids_all[p, :, j:j + 1, :] == expert_id, 1.0, mark)
        mark = mark.reshape(128, tok)
        place = jnp.dot(mark.astype(BF16), later, preferred_element_type=F32)
        i = iota((128, N), 0)
        source = number(0, {d2: 4 - (i >> 5), d1: 4 - ((i >> 3) & 3)})
        mine = jnp.dot((source == iota((128, N), 1)).astype(BF16), room, preferred_element_type=F32)
        target = number((i >> 2) & 1, {d3: i & 3})
        mine = jnp.sum(jnp.where(target == iota((128, N), 1), mine, 0.0), axis=1, keepdims=True)
        places[p] = jnp.where((mark > 0) & (place < mine), place, -1.0)

    for p in range(3):
        arrived(p, 0, 2)
        gather_on(p, 2, toks[p].at[0, 2])

    def where_in(p, d_core, s1, s2, s3):
        at = [None] * 3
        for axis, s in zip(AXES[p], (s1, s2, s3)):
            at[axis] = s
        return (d_core, *at)

    def build(p, b):
        t, blk = toks[p], blks[p]

        @pl.loop(0, 4)
        def _(a):
            place = places[p, pl.ds((4 * b + a) * 8, 8), :]
            pick = place[:, None, :] == iota((8, slots, tok), 1).astype(F32)
            pick = jnp.where(pick, 1.0, 0.0).reshape(8 * slots, tok).astype(BF16)
            rows = jnp.dot(pick, t[b, a], preferred_element_type=F32).astype(BF16).reshape(8, slots, cols[p][1])
            blk[b, :, a] = rows
            recv[where_in(p, 0, a, b, 0) + (slice(None), part(p))] = rows[0]

        for h in range(2):
            @pl.loop(1, 8)
            def _(d):
                d_core, s3 = lax.div(d, 4), lax.rem(d, 4)
                high = {AXES[p][0]: h, AXES[p][1]: b // 2, AXES[p][2]: lax.div(s3, 2)}
                cube = high[Z] * 4 + high[Y] * 2 + high[X]
                send(blk.at[b, d, pl.ds(2 * h, 2)],
                     recv.at[where_in(p, d_core, pl.ds(2 * h, 2), b, s3) + (slice(None), part(p))],
                     blk_send.at[p], blk_recv.at[p, cube], device(d_core, {AXES[p][2]: s3}))

    for p in range(3):
        build(p, 0)

    for p in range(3):
        t = toks[p]
        for step, pieces in ((1, (0, 2)), (3, (1, 3))):
            for a in pieces:
                arrived(p, step, a)
                send(t.at[step, a], t.at[2, a], tok_send_b.at[p], tok_recv.at[p, 8 + a], device(0, {AXES[p][1]: step}))

    for step, rest in ((1, (1, 3)), (3, (0, 2))):
        for p in range(3):
            for a in rest:
                arrived(p, step, a)
            build(p, step)

    load_in.wait()
    load_out.wait()

    def halves(j):
        return (lax.div(j, 4), lax.rem(lax.div(j, 2), 2), lax.rem(j, 2))

    def wait_blocks(p, h3, refs, sem):
        @pl.when(h3 == 0)
        def _():
            wait_for(refs.at[0, pl.ds(0, 3)], sem)

        @pl.when(h3 == 1)
        def _():
            wait_for(refs.at[0, pl.ds(0, 4)], sem)

    def expert(j):
        high = halves(j)
        pair = [pl.ds(2 * h, 2) for h in high]
        for p in range(3):
            wait_blocks(p, high[AXES[p][2]], blks[p], blk_recv.at[p, j])
        cube = (slice(None), *pair)
        x = recv[cube].reshape(16 * slots, width)
        hidden = jax.nn.gelu(jnp.dot(x, w_in[...], preferred_element_type=F32)).astype(BF16)
        o = jnp.dot(hidden, w_out[...], preferred_element_type=F32).astype(BF16)
        recv[cube] = o.reshape(2, 2, 2, 2, slots, width)

        for p in range(3):
            d3 = AXES[p][2]
            rest = [pair[a] for a in range(3) if a != d3]

            def along(s3):
                return tuple(s3 if a == d3 else pair[a] for a in range(3))

            @pl.when(high[d3] == 0)
            def _():
                mids[p][(*rest, 0)] = recv[(0, *along(0), slice(None), part(p))]

            @pl.loop(jnp.where(high[d3] == 0, 1, 0), 4)
            def _(i):
                d_core, s3 = lax.div(i, 2), 2 * high[d3] + lax.rem(i, 2)
                send(recv.at[(d_core, *along(s3), slice(None), part(p))], mids[p].at[(*rest, d_core * 4 + s3)],
                     mid_send.at[p], mid_recv.at[p, j], device(d_core, {d3: 4 - s3}))

    def middle(p, s1, s2):
        d1, d2 = AXES[p][:2]
        return (s1, s2) if d1 < d2 else (s2, s1)

    def pass_on(j):
        high = halves(j)
        for p in range(3):
            d1, d2, d3 = AXES[p]

            @pl.when(high[d3] == 1)
            def _():
                wait_blocks(p, 0, blks[p], mid_recv.at[p, j - (4, 2, 1)[d3]])
                wait_blocks(p, 1, blks[p], mid_recv.at[p, j])
                first = pl.ds(2 * high[d1], 2)

                @pl.when(high[d2] == 0)
                def _():
                    ends[p][first, 0] = mids[p][middle(p, first, 0)]

                @pl.loop(jnp.where(high[d2] == 0, 1, 2 * high[d2]), 2 * high[d2] + 2)
                def _(s2):
                    send(mids[p].at[middle(p, first, s2)], ends[p].at[first, s2],
                         end_send.at[p], end_recv.at[p, high[d1]], device(0, {d2: 4 - s2}))

    def weigh(p):
        d1, d2, d3 = AXES[p]
        e = iota((32, tok), 0)
        expert_id = number((e >> 2) & 1, {d2: e >> 3, d3: e & 3})

        @pl.loop(0, 4)
        def _(s1):
            ids, gts = ids_all[p, s1], gates_all[p, s1]
            mark = jnp.zeros((32, tok), F32)
            gate = jnp.zeros((32, tok), F32)
            for j in range(top):
                hit = ids[j:j + 1, :] == expert_id
                mark = jnp.where(hit, 1.0, mark)
                gate = jnp.where(hit, gts[j:j + 1, :], gate)
            place = jnp.dot(mark.astype(BF16), later, preferred_element_type=F32)
            place = jnp.where(mark > 0, place, -1.0)
            scale = jnp.where(place[:, None, :] == iota((32, slots, tok), 1).astype(F32), gate[:, None, :], 0.0)
            scale = scale.reshape(32 * slots, tok).T
            high = scale.astype(BF16)
            left = scale - high.astype(F32)
            mid = left.astype(BF16)
            low = (left - mid.astype(F32)).astype(BF16)
            scales[4 * p + s1] = jnp.concatenate([high, mid, low], axis=0)

    def combine(p, h):
        wait_for(ends[p].at[pl.ds(2 * h, 2), pl.ds(1, 3)], end_recv.at[p, h])
        for s1 in (2 * h + 1, 2 * h):
            rows = ends[p][s1].reshape(32 * slots, cols[p][1])
            mixed = jnp.dot(scales[4 * p + s1], rows, preferred_element_type=F32)
            mixed = mixed[:tok] + (mixed[tok:2 * tok] + mixed[2 * tok:])
            if s1 == 0:
                acc[:, part(p)] = tokens_ref[:, part(p)].astype(F32) + mixed
            else:
                sums[p][s1 - 1] = mixed
                send(sums[p].at[s1 - 1], gots[p].at[s1 - 1], sum_send.at[p], sum_recv.at[p, s1 - 1], device(0, {AXES[p][0]: 4 - s1}))

    pl.loop(0, 1)(expert)

    for p in range(3):
        for a in range(4):
            arrived(p, 2, a)
        build(p, 2)

    for p in range(3):
        wait_for(gates_all.at[p, pl.ds(1, 3)], gate_recv.at[p])

    @pl.loop(1, 8)
    def _(j):
        expert(j)

        @pl.when(j > 3)
        def _():
            pass_on(j - 3)

    pl.loop(5, 8)(pass_on)
    for p in range(3):
        weigh(p)
    for h in range(2):
        for p in range(3):
            combine(p, h)

    for p in range(3):
        total = acc[:, part(p)]
        for i in range(3):
            wait_for(gots[p].at[i], sum_recv.at[p, i])
            total = total + gots[p][i]
        out_ref[:, part(p)] = total.astype(BF16)

    wait_for(cnt_all.at[pl.ds(0, N - 1)], cnt_send)
    for p in range(3):
        wait_for(ids_all.at[p, pl.ds(1, 15)], ids_send.at[p])
        wait_for(gates_all.at[p, pl.ds(1, 3)], gate_send.at[p])
        wait_for(toks[p].at[0, pl.ds(0, 3)], tok_send_a.at[p])
        wait_for(toks[p].at[pl.ds(0, 3)], tok_send_b.at[p])
        wait_for(blks[p].at[:, pl.ds(1, 7)], blk_send.at[p])
        wait_for(mids[p].at[:, :, pl.ds(1, 7)], mid_send.at[p])
        wait_for(ends[p].at[:, pl.ds(1, 3)], end_send.at[p])
        wait_for(sums[p], sum_send.at[p])


def solution(mesh):
    def device_fn(tokens, expert_ids, gate_weights, w_in, w_out):
        tok, width = tokens.shape
        top = expert_ids.shape[1]
        ff = w_in.shape[2]
        cap = tok * top
        slots = 2 * tok * top // N
        tiles = width // 128
        sizes = [128 * (tiles // 3 + (1 if p < tiles % 3 else 0)) for p in range(3)]
        cols = [(sum(sizes[:p]), sizes[p]) for p in range(3)]
        vmem = pl.BlockSpec(memory_space=pltpu.VMEM)
        anyspace = pl.BlockSpec(memory_space=pl.ANY)
        dma = pltpu.SemaphoreType.DMA
        return pl.pallas_call(
            functools.partial(kernel, cols, cap, slots),
            out_shape=jax.ShapeDtypeStruct((tok, width), BF16),
            in_specs=[vmem, vmem, vmem, anyspace, anyspace],
            out_specs=vmem,
            scratch_shapes=[
                pltpu.VMEM((width, ff), BF16),
                pltpu.VMEM((ff, width), BF16),
                *[pltpu.VMEM((4, 4, tok, s), BF16) for s in sizes],
                *[pltpu.VMEM((4, 8, 4, slots, s), BF16) for s in sizes],
                pltpu.VMEM((2, 4, 4, 4, slots, width), BF16),
                *[pltpu.VMEM((4, 4, 8, slots, s), BF16) for s in sizes],
                *[pltpu.VMEM((4, 4, 8, slots, s), BF16) for s in sizes],
                *[pltpu.VMEM((3, tok, s), F32) for s in sizes],
                *[pltpu.VMEM((3, tok, s), F32) for s in sizes],
                pltpu.VMEM((3, 16, top, tok), I32),
                pltpu.VMEM((3, 4, top, tok), F32),
                pltpu.VMEM((3, 128, tok), F32),
                pltpu.VMEM((12, 3 * tok, 32 * slots), BF16),
                pltpu.VMEM((1, N), F32),
                pltpu.VMEM((N, 1, N), F32),
                pltpu.VMEM((tok, width), F32),
                dma((2,)), dma((3,)), dma((3,)), dma((3,)), dma((3,)), dma, dma, dma((3,)), dma((3,)), dma((3, 16)),
                dma((3,)), dma((3, 8)), dma((3,)), dma((3, 8)), dma((3,)), dma((3, 2)), dma((3,)), dma((3, 3)),
            ],
            compiler_params=pltpu.CompilerParams(collective_id=0, has_side_effects=True, vmem_limit_bytes=67043328),
            name='expert_layer',
        )(tokens, expert_ids.T, gate_weights.T, w_in.reshape(width, ff), w_out.reshape(ff, width))

    token_spec = P(('data', 'row', 'col'), None)
    expert_spec = P(GRID_AXES, None, None)
    return jax.shard_map(device_fn, mesh=mesh, in_specs=(token_spec, token_spec, token_spec, expert_spec, expert_spec), out_specs=token_spec, check_vma=False)
```

```python
import functools

import jax
import jax.numpy as jnp
from jax import lax
from jax.experimental import pallas as pl
from jax.experimental.pallas import tpu as pltpu
from jax.sharding import PartitionSpec as P

GRID_AXES = ('row', 'col')
F32 = jnp.float32
BF16 = jnp.bfloat16
I32 = jnp.int32
SIDE = 4
N = 2 * SIDE ** 3
MESH = pl.DeviceIdType.MESH
Z, Y, X = 0, 1, 2
AXES = ((Z, Y, X), (Y, X, Z), (X, Z, Y))


def iota(shape, dim):
    return lax.broadcasted_iota(I32, shape, dim)


def kernel(cols, cap, slots, tokens_ref, ids_ref, gates_ref, w_in_hbm, w_out_hbm, out_ref,
           w_in, w_out, tok0, tok1, tok2, blk0, blk1, blk2, recv, mid0, mid1, mid2, end0, end1, end2,
           sum0, sum1, sum2, got0, got1, got2, ids_all, gates_all, places, scales, cnt_mine, cnt_all, acc,
           w_sem, ids_send, ids_recv, gate_send, gate_recv, cnt_send, cnt_recv, tok_send_a, tok_send_b, tok_recv,
           blk_send, blk_recv, mid_send, mid_recv, end_send, end_recv, sum_send, sum_recv):
    toks, blks = (tok0, tok1, tok2), (blk0, blk1, blk2)
    mids, ends = (mid0, mid1, mid2), (end0, end1, end2)
    sums, gots = (sum0, sum1, sum2), (got0, got1, got2)
    tok, width = tokens_ref.shape
    top = ids_ref.shape[0]
    data = lax.axis_index('data')
    core = lax.axis_index('row')
    col = lax.axis_index('col')
    here = (lax.div(col, 16), lax.rem(lax.div(col, 4), 4), lax.rem(col, 4))
    me = core * 64 + col
    weight = (16, 4, 1)

    def device(d_core, d):
        at = [lax.rem(here[a] + d[a], 4) if a in d else here[a] for a in range(3)]
        return (data, lax.rem(core + d_core, 2), at[0] * 16 + at[1] * 4 + at[2])

    def number(d_core, d):
        n = ((core + d_core) & 1) * 64
        for a in range(3):
            n = n + (((here[a] + d[a]) & 3) if a in d else here[a]) * weight[a]
        return n

    def part(p):
        return pl.ds(cols[p][0], cols[p][1])

    def send(src, dst, send_sem, recv_sem, to):
        pltpu.make_async_remote_copy(src, dst, send_sem, recv_sem, device_id=to, device_id_type=MESH).start()

    def wait_for(ref, sem):
        pltpu.make_async_copy(ref, ref, sem).wait()

    load_in = pltpu.make_async_copy(w_in_hbm, w_in, w_sem.at[0])
    load_out = pltpu.make_async_copy(w_out_hbm, w_out, w_sem.at[1])

    def across(k):
        return device(lax.div(k, 64), {Z: lax.rem(lax.div(k, 16), 4), Y: lax.rem(lax.div(k, 4), 4), X: lax.rem(k, 4)})

    barrier = pltpu.get_barrier_semaphore()

    @pl.loop(1, N)
    def _(k):
        pl.semaphore_signal(barrier, inc=1, device_id=across(k), device_id_type=MESH)

    mark = jnp.zeros((N, tok), F32)
    for j in range(top):
        mark = jnp.where(ids_ref[j:j + 1, :] == iota((N, tok), 0), 1.0, mark)
    counts = lax.dot_general(jnp.ones((8, tok), BF16), mark.astype(BF16), (((1,), (1,)), ((), ())), preferred_element_type=F32)
    cnt_mine[...] = counts[:1]
    cnt_all[pl.ds(me, 1)] = counts[:1][None]
    for p in range(3):
        toks[p][0, 0] = tokens_ref[:, part(p)]
        ids_all[p, 0] = ids_ref[...]
        gates_all[p, 0] = gates_ref[...]
    load_in.start()
    load_out.start()
    pl.semaphore_wait(barrier, N - 1)

    for p in range(3):
        for step in (1, 3):
            send(tokens_ref.at[:, part(p)], toks[p].at[0, step], tok_send_a.at[p], tok_recv.at[p, step], device(0, {AXES[p][0]: step}))

    def gather_on(p, a, src):
        for step in (1, 3):
            send(src, toks[p].at[step, a], tok_send_b.at[p], tok_recv.at[p, 4 * step + a], device(0, {AXES[p][1]: step}))

    for p in range(3):
        gather_on(p, 0, tokens_ref.at[:, part(p)])

    @pl.loop(1, N)
    def _(k):
        send(cnt_mine, cnt_all.at[me], cnt_send, cnt_recv, across(k))

    for p in range(3):
        d1, d2, d3 = AXES[p]

        @pl.loop(1, 16)
        def _(i):
            send(ids_ref, ids_all.at[p, i], ids_send.at[p], ids_recv.at[p], device(0, {d2: lax.div(i, 4), d1: lax.rem(i, 4)}))

        @pl.loop(1, 4)
        def _(i):
            send(gates_ref, gates_all.at[p, i], gate_send.at[p], gate_recv.at[p], device(0, {d1: i}))

    def arrived(p, b, a):
        wait_for(toks[p].at[b, a], tok_recv.at[p, 4 * b + a])

    half = tok // 2
    for p in range(3):
        t = toks[p]
        for step, rows in ((1, pl.ds(0, half)), (3, pl.ds(half, half))):
            arrived(p, 0, step)
            send(t.at[0, step, rows], t.at[0, 2, rows], tok_send_a.at[p], tok_recv.at[p, 2], device(0, {AXES[p][0]: step}))
            gather_on(p, step, t.at[0, step])

    wait_for(cnt_all.at[pl.ds(0, N - 1)], cnt_recv)
    below = (iota((N, N), 1) < iota((N, N), 0)).astype(BF16)
    before = jnp.dot(below, jnp.sum(cnt_all[...], axis=1).astype(BF16), preferred_element_type=F32)
    room = jnp.clip(cap - before, 0.0, float(slots)).astype(BF16)

    later = (iota((tok, tok), 0) < iota((tok, tok), 1)).astype(BF16)
    for p in range(3):
        d1, d2, d3 = AXES[p]
        wait_for(ids_all.at[p, pl.ds(1, 15)], ids_recv.at[p])
        dest = iota((8, tok), 0)
        expert_id = number(dest >> 2, {d3: dest & 3})[None]
        mark = jnp.zeros((16, 8, tok), F32)
        for j in range(top):
            mark = jnp.where(ids_all[p, :, j:j + 1, :] == expert_id, 1.0, mark)
        mark = mark.reshape(128, tok)
        place = jnp.dot(mark.astype(BF16), later, preferred_element_type=F32)
        i = iota((128, N), 0)
        source = number(0, {d2: 4 - (i >> 5), d1: 4 - ((i >> 3) & 3)})
        mine = jnp.dot((source == iota((128, N), 1)).astype(BF16), room, preferred_element_type=F32)
        target = number((i >> 2) & 1, {d3: i & 3})
        mine = jnp.sum(jnp.where(target == iota((128, N), 1), mine, 0.0), axis=1, keepdims=True)
        places[p] = jnp.where((mark > 0) & (place < mine), place, -1.0)

    for p in range(3):
        arrived(p, 0, 2)
        gather_on(p, 2, toks[p].at[0, 2])

    def where_in(p, d_core, s1, s2, s3):
        at = [None] * 3
        for axis, s in zip(AXES[p], (s1, s2, s3)):
            at[axis] = s
        return (d_core, *at)

    def build(p, b):
        t, blk = toks[p], blks[p]

        @pl.loop(0, 4)
        def _(a):
            place = places[p, pl.ds((4 * b + a) * 8, 8), :]
            pick = place[:, None, :] == iota((8, slots, tok), 1).astype(F32)
            pick = jnp.where(pick, 1.0, 0.0).reshape(8 * slots, tok).astype(BF16)
            rows = jnp.dot(pick, t[b, a], preferred_element_type=F32).astype(BF16).reshape(8, slots, cols[p][1])
            blk[b, :, a] = rows
            recv[where_in(p, 0, a, b, 0) + (slice(None), part(p))] = rows[0]

        for h in range(2):
            @pl.loop(1, 8)
            def _(d):
                d_core, s3 = lax.div(d, 4), lax.rem(d, 4)
                high = {AXES[p][0]: h, AXES[p][1]: b // 2, AXES[p][2]: lax.div(s3, 2)}
                cube = high[Z] * 4 + high[Y] * 2 + high[X]
                send(blk.at[b, d, pl.ds(2 * h, 2)],
                     recv.at[where_in(p, d_core, pl.ds(2 * h, 2), b, s3) + (slice(None), part(p))],
                     blk_send.at[p], blk_recv.at[p, cube], device(d_core, {AXES[p][2]: s3}))

    for p in range(3):
        build(p, 0)

    for p in range(3):
        t = toks[p]
        for step, pieces in ((1, (0, 2)), (3, (1, 3))):
            for a in pieces:
                arrived(p, step, a)
                send(t.at[step, a], t.at[2, a], tok_send_b.at[p], tok_recv.at[p, 8 + a], device(0, {AXES[p][1]: step}))

    for step, rest in ((1, (1, 3)), (3, (0, 2))):
        for p in range(3):
            for a in rest:
                arrived(p, step, a)
            build(p, step)

    load_in.wait()
    load_out.wait()

    def halves(j):
        return (lax.div(j, 4), lax.rem(lax.div(j, 2), 2), lax.rem(j, 2))

    def wait_blocks(p, h3, refs, sem):
        @pl.when(h3 == 0)
        def _():
            wait_for(refs.at[0, pl.ds(0, 3)], sem)

        @pl.when(h3 == 1)
        def _():
            wait_for(refs.at[0, pl.ds(0, 4)], sem)

    def expert(j):
        high = halves(j)
        pair = [pl.ds(2 * h, 2) for h in high]
        for p in range(3):
            wait_blocks(p, high[AXES[p][2]], blks[p], blk_recv.at[p, j])
        cube = (slice(None), *pair)
        x = recv[cube].reshape(16 * slots, width)
        hidden = jax.nn.gelu(jnp.dot(x, w_in[...], preferred_element_type=F32)).astype(BF16)
        o = jnp.dot(hidden, w_out[...], preferred_element_type=F32).astype(BF16)
        recv[cube] = o.reshape(2, 2, 2, 2, slots, width)

    def hand_out(j):
        high = halves(j)
        pair = [pl.ds(2 * h, 2) for h in high]
        for p in range(3):
            d3 = AXES[p][2]
            rest = [pair[a] for a in range(3) if a != d3]

            def along(s3):
                return tuple(s3 if a == d3 else pair[a] for a in range(3))

            @pl.when(high[d3] == 0)
            def _():
                mids[p][(*rest, 0)] = recv[(0, *along(0), slice(None), part(p))]

            @pl.loop(jnp.where(high[d3] == 0, 1, 0), 4)
            def _(i):
                d_core, s3 = lax.div(i, 2), 2 * high[d3] + lax.rem(i, 2)
                send(recv.at[(d_core, *along(s3), slice(None), part(p))], mids[p].at[(*rest, d_core * 4 + s3)],
                     mid_send.at[p], mid_recv.at[p, j], device(d_core, {d3: 4 - s3}))

    def middle(p, s1, s2):
        d1, d2 = AXES[p][:2]
        return (s1, s2) if d1 < d2 else (s2, s1)

    def pass_on(j):
        high = halves(j)
        for p in range(3):
            d1, d2, d3 = AXES[p]

            @pl.when(high[d3] == 0)
            def _():
                wait_blocks(p, 1, blks[p], mid_recv.at[p, j + (4, 2, 1)[d3]])
                wait_blocks(p, 0, blks[p], mid_recv.at[p, j])
                first = pl.ds(2 * high[d1], 2)

                @pl.when(high[d2] == 0)
                def _():
                    ends[p][first, 0] = mids[p][middle(p, first, 0)]

                @pl.loop(jnp.where(high[d2] == 0, 1, 2 * high[d2]), 2 * high[d2] + 2)
                def _(s2):
                    send(mids[p].at[middle(p, first, s2)], ends[p].at[first, s2],
                         end_send.at[p], end_recv.at[p, high[d1]], device(0, {d2: 4 - s2}))

    def weigh(p):
        d1, d2, d3 = AXES[p]
        e = iota((32, tok), 0)
        expert_id = number((e >> 2) & 1, {d2: e >> 3, d3: e & 3})

        @pl.loop(0, 4)
        def _(s1):
            ids, gts = ids_all[p, s1], gates_all[p, s1]
            mark = jnp.zeros((32, tok), F32)
            gate = jnp.zeros((32, tok), F32)
            for j in range(top):
                hit = ids[j:j + 1, :] == expert_id
                mark = jnp.where(hit, 1.0, mark)
                gate = jnp.where(hit, gts[j:j + 1, :], gate)
            place = jnp.dot(mark.astype(BF16), later, preferred_element_type=F32)
            place = jnp.where(mark > 0, place, -1.0)
            scale = jnp.where(place[:, None, :] == iota((32, slots, tok), 1).astype(F32), gate[:, None, :], 0.0)
            scale = scale.reshape(32 * slots, tok).T
            high = scale.astype(BF16)
            left = scale - high.astype(F32)
            mid = left.astype(BF16)
            low = (left - mid.astype(F32)).astype(BF16)
            scales[4 * p + s1] = jnp.concatenate([high, mid, low], axis=0)

    def combine(p, h):
        wait_for(ends[p].at[pl.ds(2 * h, 2), pl.ds(1, 3)], end_recv.at[p, h])
        for s1 in (2 * h + 1, 2 * h):
            rows = ends[p][s1].reshape(32 * slots, cols[p][1])
            mixed = jnp.dot(scales[4 * p + s1], rows, preferred_element_type=F32)
            mixed = mixed[:tok] + (mixed[tok:2 * tok] + mixed[2 * tok:])
            if s1 == 0:
                acc[:, part(p)] = tokens_ref[:, part(p)].astype(F32) + mixed
            else:
                sums[p][s1 - 1] = mixed
                send(sums[p].at[s1 - 1], gots[p].at[s1 - 1], sum_send.at[p], sum_recv.at[p, s1 - 1], device(0, {AXES[p][0]: 4 - s1}))

    pl.loop(0, 1)(expert)

    for p in range(3):
        for a in range(4):
            arrived(p, 2, a)
        build(p, 2)

    for p in range(3):
        wait_for(gates_all.at[p, pl.ds(1, 3)], gate_recv.at[p])

    @pl.loop(0, 7)
    def _(i):
        expert(7 - i)
        hand_out(7 - i)

        @pl.when(i > 2)
        def _():
            pass_on(10 - i)

    pl.loop(0, 1)(hand_out)

    @pl.loop(0, 4)
    def _(i):
        pass_on(3 - i)

    for p in range(3):
        weigh(p)
    for h in (1, 0):
        for p in range(3):
            combine(p, h)

    for p in range(3):
        total = acc[:, part(p)]
        for i in range(3):
            wait_for(gots[p].at[i], sum_recv.at[p, i])
            total = total + gots[p][i]
        out_ref[:, part(p)] = total.astype(BF16)

    wait_for(cnt_all.at[pl.ds(0, N - 1)], cnt_send)
    for p in range(3):
        wait_for(ids_all.at[p, pl.ds(1, 15)], ids_send.at[p])
        wait_for(gates_all.at[p, pl.ds(1, 3)], gate_send.at[p])
        wait_for(toks[p].at[0, pl.ds(0, 3)], tok_send_a.at[p])
        wait_for(toks[p].at[pl.ds(0, 3)], tok_send_b.at[p])
        wait_for(blks[p].at[:, pl.ds(1, 7)], blk_send.at[p])
        wait_for(mids[p].at[:, :, pl.ds(1, 7)], mid_send.at[p])
        wait_for(ends[p].at[:, pl.ds(1, 3)], end_send.at[p])
        wait_for(sums[p], sum_send.at[p])


def solution(mesh):
    def device_fn(tokens, expert_ids, gate_weights, w_in, w_out):
        tok, width = tokens.shape
        top = expert_ids.shape[1]
        ff = w_in.shape[2]
        cap = tok * top
        slots = 2 * tok * top // N
        tiles = width // 128
        sizes = [128 * (tiles // 3 + (1 if p < tiles % 3 else 0)) for p in range(3)]
        cols = [(sum(sizes[:p]), sizes[p]) for p in range(3)]
        vmem = pl.BlockSpec(memory_space=pltpu.VMEM)
        anyspace = pl.BlockSpec(memory_space=pl.ANY)
        dma = pltpu.SemaphoreType.DMA
        return pl.pallas_call(
            functools.partial(kernel, cols, cap, slots),
            out_shape=jax.ShapeDtypeStruct((tok, width), BF16),
            in_specs=[vmem, vmem, vmem, anyspace, anyspace],
            out_specs=vmem,
            scratch_shapes=[
                pltpu.VMEM((width, ff), BF16),
                pltpu.VMEM((ff, width), BF16),
                *[pltpu.VMEM((4, 4, tok, s), BF16) for s in sizes],
                *[pltpu.VMEM((4, 8, 4, slots, s), BF16) for s in sizes],
                pltpu.VMEM((2, 4, 4, 4, slots, width), BF16),
                *[pltpu.VMEM((4, 4, 8, slots, s), BF16) for s in sizes],
                *[pltpu.VMEM((4, 4, 8, slots, s), BF16) for s in sizes],
                *[pltpu.VMEM((3, tok, s), F32) for s in sizes],
                *[pltpu.VMEM((3, tok, s), F32) for s in sizes],
                pltpu.VMEM((3, 16, top, tok), I32),
                pltpu.VMEM((3, 4, top, tok), F32),
                pltpu.VMEM((3, 128, tok), F32),
                pltpu.VMEM((12, 3 * tok, 32 * slots), BF16),
                pltpu.VMEM((1, N), F32),
                pltpu.VMEM((N, 1, N), F32),
                pltpu.VMEM((tok, width), F32),
                dma((2,)), dma((3,)), dma((3,)), dma((3,)), dma((3,)), dma, dma, dma((3,)), dma((3,)), dma((3, 16)),
                dma((3,)), dma((3, 8)), dma((3,)), dma((3, 8)), dma((3,)), dma((3, 2)), dma((3,)), dma((3, 3)),
            ],
            compiler_params=pltpu.CompilerParams(collective_id=0, has_side_effects=True, vmem_limit_bytes=67043328),
            name='expert_layer',
        )(tokens, expert_ids.T, gate_weights.T, w_in.reshape(width, ff), w_out.reshape(ff, width))

    token_spec = P(('data', 'row', 'col'), None)
    expert_spec = P(GRID_AXES, None, None)
    return jax.shard_map(device_fn, mesh=mesh, in_specs=(token_spec, token_spec, token_spec, expert_spec, expert_spec), out_specs=token_spec, check_vma=False)
```

```python
import functools

import jax
import jax.numpy as jnp
from jax import lax
from jax.experimental import pallas as pl
from jax.experimental.pallas import tpu as pltpu
from jax.sharding import PartitionSpec as P

GRID_AXES = ('row', 'col')
F32 = jnp.float32
BF16 = jnp.bfloat16
I32 = jnp.int32
SIDE = 4
N = 2 * SIDE ** 3
MESH = pl.DeviceIdType.MESH
Z, Y, X = 0, 1, 2
AXES = ((Z, Y, X), (Y, X, Z), (X, Z, Y))


def iota(shape, dim):
    return lax.broadcasted_iota(I32, shape, dim)


def kernel(cols, cap, slots, tokens_ref, ids_ref, gates_ref, w_in_hbm, w_out_hbm, out_ref,
           w_in, w_out, tok0, tok1, tok2, blk0, blk1, blk2, recv, mid0, mid1, mid2, end0, end1, end2,
           sum0, sum1, sum2, got0, got1, got2, info, info_all, places, scales, cnt_out, cnt_in, cnt_row, acc,
           w_sem, info_send_a, info_send_b, info_recv, cnt_send, cnt_recv, line_sem, tok_send_a, tok_send_b, tok_recv,
           blk_send, blk_recv, mid_send, mid_recv, end_send, end_recv, sum_send, sum_recv):
    toks, blks = (tok0, tok1, tok2), (blk0, blk1, blk2)
    mids, ends = (mid0, mid1, mid2), (end0, end1, end2)
    sums, gots = (sum0, sum1, sum2), (got0, got1, got2)
    tok, width = tokens_ref.shape
    top = ids_ref.shape[0]
    data = lax.axis_index('data')
    core = lax.axis_index('row')
    col = lax.axis_index('col')
    here = (lax.div(col, 16), lax.rem(lax.div(col, 4), 4), lax.rem(col, 4))
    me = core * 64 + col
    weight = (16, 4, 1)

    def device(d_core, d):
        at = [lax.rem(here[a] + d[a], 4) if a in d else here[a] for a in range(3)]
        return (data, lax.rem(core + d_core, 2), at[0] * 16 + at[1] * 4 + at[2])

    def number(d_core, d):
        n = ((core + d_core) & 1) * 64
        for a in range(3):
            n = n + (((here[a] + d[a]) & 3) if a in d else here[a]) * weight[a]
        return n

    def part(p):
        return pl.ds(cols[p][0], cols[p][1])

    def send(src, dst, send_sem, recv_sem, to):
        pltpu.make_async_remote_copy(src, dst, send_sem, recv_sem, device_id=to, device_id_type=MESH).start()

    def wait_for(ref, sem):
        pltpu.make_async_copy(ref, ref, sem).wait()

    load_in = pltpu.make_async_copy(w_in_hbm, w_in, w_sem.at[0])
    load_out = pltpu.make_async_copy(w_out_hbm, w_out, w_sem.at[1])

    near = [device(0, {a: step}) for a in range(3) for step in (1, 3)] + [device(1, {})]
    barrier = pltpu.get_barrier_semaphore()
    for to in near:
        pl.semaphore_signal(barrier, inc=1, device_id=to, device_id_type=MESH)
    load_in.start()
    load_out.start()
    info[:top] = ids_ref[...].astype(F32)
    info[top:] = gates_ref[...]
    pl.semaphore_wait(barrier, len(near))

    for p in range(3):
        for step in (1, 3):
            to = device(0, {AXES[p][0]: step})
            send(info, info_all.at[p, step], info_send_a.at[p], info_recv.at[p, step], to)
            send(tokens_ref.at[:, part(p)], toks[p].at[0, step], tok_send_a.at[p], tok_recv.at[p, step], to)

    ids = pl.ds(0, top)

    def gather_on(p, a, src, ids_src):
        for step in (1, 3):
            to = device(0, {AXES[p][1]: step})
            send(ids_src, info_all.at[p, 4 * step + a, ids], info_send_b.at[p], info_recv.at[p, 4 * step + a], to)
            send(src, toks[p].at[step, a], tok_send_b.at[p], tok_recv.at[p, 4 * step + a], to)

    for p in range(3):
        gather_on(p, 0, tokens_ref.at[:, part(p)], info.at[ids])
    for p in range(3):
        toks[p][0, 0] = tokens_ref[:, part(p)]
        info_all[p, 0] = info[...]

    def arrived(p, b, a):
        what = info_all.at[p, a] if b == 0 else info_all.at[p, 4 * b + a, ids]
        wait_for(what, info_recv.at[p, 4 * b + a])
        wait_for(toks[p].at[b, a], tok_recv.at[p, 4 * b + a])

    half = tok // 2
    for p in range(3):
        t = toks[p]
        for step, rows in ((1, pl.ds(0, half)), (3, pl.ds(half, half))):
            arrived(p, 0, step)
            to = device(0, {AXES[p][0]: step})
            if step == 1:
                send(info_all.at[p, 1], info_all.at[p, 2], info_send_a.at[p], info_recv.at[p, 2], to)
            send(t.at[0, step, rows], t.at[0, 2, rows], tok_send_a.at[p], tok_recv.at[p, 2], to)
            gather_on(p, step, t.at[0, step], info_all.at[p, step, ids])

    for p in range(3):
        arrived(p, 0, 2)
        gather_on(p, 2, toks[p].at[0, 2], info_all.at[p, 2, ids])

    pl.semaphore_signal(line_sem, inc=1, device_id=near[6], device_id_type=MESH)
    pl.semaphore_wait(line_sem, 1)

    later = (iota((tok, tok), 0) < iota((tok, tok), 1)).astype(BF16)

    def where_in(p, d_core, s1, s2, s3):
        at = [None] * 3
        for axis, s in zip(AXES[p], (s1, s2, s3)):
            at[axis] = s
        return (d_core, *at)

    def build(p, b):
        t, blk = toks[p], blks[p]
        d3 = AXES[p][2]
        dest = iota((8, tok), 0)
        expert_id = number(dest >> 2, {d3: dest & 3}).astype(F32)[None]
        mark = jnp.zeros((4, 8, tok), F32)
        for j in range(top):
            mark = jnp.where(info_all[p, pl.ds(4 * b, 4), j:j + 1, :] == expert_id, 1.0, mark)
        mark = mark.reshape(32, tok)
        place = jnp.dot(mark.astype(BF16), later, preferred_element_type=F32)
        places[...] = jnp.where(mark > 0, place, -1.0)
        if p == 0:
            wide = [jnp.zeros((32, tok), F32)] * 4
            wide[b] = mark
            wide = jnp.concatenate(wide, axis=0).astype(BF16)
            cnt_out[b] = lax.dot_general(jnp.ones((8, tok), BF16), wide, (((1,), (1,)), ((), ())), preferred_element_type=F32)
            cnt_in[0, b] = cnt_out[b]

            @pl.loop(1, 8)
            def _(d):
                send(cnt_out.at[b], cnt_in.at[d, b], cnt_send, cnt_recv, device(lax.div(d, 4), {d3: lax.rem(d, 4)}))

        @pl.loop(0, 4)
        def _(a):
            place = places[pl.ds(a * 8, 8), :]
            pick = place[:, None, :] == iota((8, slots, tok), 1).astype(F32)
            pick = jnp.where(pick, 1.0, 0.0).reshape(8 * slots, tok).astype(BF16)
            rows = jnp.dot(pick, t[b, a], preferred_element_type=F32).astype(BF16).reshape(8, slots, cols[p][1])
            blk[b, :, a] = rows
            recv[where_in(p, 0, a, b, 0) + (slice(None), part(p))] = rows[0]

        for h in range(2):
            @pl.loop(1, 8)
            def _(d):
                d_core, s3 = lax.div(d, 4), lax.rem(d, 4)
                high = {AXES[p][0]: h, AXES[p][1]: b // 2, AXES[p][2]: lax.div(s3, 2)}
                cube = high[Z] * 4 + high[Y] * 2 + high[X]
                send(blk.at[b, d, pl.ds(2 * h, 2)],
                     recv.at[where_in(p, d_core, pl.ds(2 * h, 2), b, s3) + (slice(None), part(p))],
                     blk_send.at[p], blk_recv.at[p, cube], device(d_core, {AXES[p][2]: s3}))

    for p in range(3):
        build(p, 0)

    for p in range(3):
        t = toks[p]
        for step, pieces in ((1, (0, 2)), (3, (1, 3))):
            for a in pieces:
                arrived(p, step, a)
                to = device(0, {AXES[p][1]: step})
                send(info_all.at[p, 4 * step + a, ids], info_all.at[p, 8 + a, ids], info_send_b.at[p], info_recv.at[p, 8 + a], to)
                send(t.at[step, a], t.at[2, a], tok_send_b.at[p], tok_recv.at[p, 8 + a], to)

    for step, rest in ((1, (1, 3)), (3, (0, 2))):
        for p in range(3):
            for a in rest:
                arrived(p, step, a)
            build(p, step)

    load_in.wait()
    load_out.wait()

    def halves(j):
        return (lax.div(j, 4), lax.rem(lax.div(j, 2), 2), lax.rem(j, 2))

    def wait_blocks(p, h3, refs, sem):
        @pl.when(h3 == 0)
        def _():
            wait_for(refs.at[0, pl.ds(0, 3)], sem)

        @pl.when(h3 == 1)
        def _():
            wait_for(refs.at[0, pl.ds(0, 4)], sem)

    def expert(j):
        high = halves(j)
        pair = [pl.ds(2 * h, 2) for h in high]
        for p in range(3):
            wait_blocks(p, high[AXES[p][2]], blks[p], blk_recv.at[p, j])
        cube = (slice(None), *pair)
        x = recv[cube].reshape(16 * slots, width)
        hidden = jax.nn.gelu(jnp.dot(x, w_in[...], preferred_element_type=F32)).astype(BF16)
        o = jnp.dot(hidden, w_out[...], preferred_element_type=F32).astype(BF16)
        recv[cube] = o.reshape(2, 2, 2, 2, slots, width)

    def drop(j):
        high = halves(j)
        cube = (slice(None), *[pl.ds(2 * h, 2) for h in high])
        rows = 16 * slots
        r = iota((rows, N), 0)
        i = r // slots
        taker = number((i >> 3) & 1, {Z: 4 - (2 * high[Z] + ((i >> 2) & 1)), Y: 4 - (2 * high[Y] + ((i >> 1) & 1)), X: 4 - (2 * high[X] + (i & 1))})
        c = iota((rows, N), 1)
        d1, d2, d3 = AXES[0]
        source = number((c >> 2) & 1, {d1: 4 - ((c >> 3) & 3), d2: 4 - (c >> 5), d3: 4 - (c & 3)})
        before = jnp.sum(jnp.where(source < taker, cnt_row[...], 0.0), axis=1, keepdims=True)
        keep = before + (iota((rows, 1), 0) % slots).astype(F32) < float(cap)
        o = recv[cube].reshape(rows, width)
        recv[cube] = jnp.where(keep, o, jnp.zeros_like(o)).reshape(2, 2, 2, 2, slots, width)

    def hand_out(j):
        high = halves(j)
        pair = [pl.ds(2 * h, 2) for h in high]
        for p in range(3):
            d3 = AXES[p][2]
            rest = [pair[a] for a in range(3) if a != d3]

            def along(s3):
                return tuple(s3 if a == d3 else pair[a] for a in range(3))

            @pl.when(high[d3] == 0)
            def _():
                mids[p][(*rest, 0)] = recv[(0, *along(0), slice(None), part(p))]

            @pl.loop(jnp.where(high[d3] == 0, 1, 0), 4)
            def _(i):
                d_core, s3 = lax.div(i, 2), 2 * high[d3] + lax.rem(i, 2)
                send(recv.at[(d_core, *along(s3), slice(None), part(p))], mids[p].at[(*rest, d_core * 4 + s3)],
                     mid_send.at[p], mid_recv.at[p, j], device(d_core, {d3: 4 - s3}))

    def middle(p, s1, s2):
        d1, d2 = AXES[p][:2]
        return (s1, s2) if d1 < d2 else (s2, s1)

    def pass_on(j):
        high = halves(j)
        for p in range(3):
            d1, d2, d3 = AXES[p]

            @pl.when(high[d3] == 0)
            def _():
                wait_blocks(p, 1, blks[p], mid_recv.at[p, j + (4, 2, 1)[d3]])
                wait_blocks(p, 0, blks[p], mid_recv.at[p, j])
                first = pl.ds(2 * high[d1], 2)

                @pl.when(high[d2] == 0)
                def _():
                    ends[p][first, 0] = mids[p][middle(p, first, 0)]

                @pl.loop(jnp.where(high[d2] == 0, 1, 2 * high[d2]), 2 * high[d2] + 2)
                def _(s2):
                    send(mids[p].at[middle(p, first, s2)], ends[p].at[first, s2],
                         end_send.at[p], end_recv.at[p, high[d1]], device(0, {d2: 4 - s2}))

    def weigh(p):
        d1, d2, d3 = AXES[p]
        e = iota((32, tok), 0)
        expert_id = number((e >> 2) & 1, {d2: e >> 3, d3: e & 3}).astype(F32)

        @pl.loop(0, 4)
        def _(s1):
            ids, gts = info_all[p, s1, :top], info_all[p, s1, top:]
            mark = jnp.zeros((32, tok), F32)
            gate = jnp.zeros((32, tok), F32)
            for j in range(top):
                hit = ids[j:j + 1, :] == expert_id
                mark = jnp.where(hit, 1.0, mark)
                gate = jnp.where(hit, gts[j:j + 1, :], gate)
            place = jnp.dot(mark.astype(BF16), later, preferred_element_type=F32)
            place = jnp.where(mark > 0, place, -1.0)
            scale = jnp.where(place[:, None, :] == iota((32, slots, tok), 1).astype(F32), gate[:, None, :], 0.0)
            scale = scale.reshape(32 * slots, tok).T
            high = scale.astype(BF16)
            left = scale - high.astype(F32)
            mid = left.astype(BF16)
            low = (left - mid.astype(F32)).astype(BF16)
            scales[4 * p + s1] = jnp.concatenate([high, mid, low], axis=0)

    def combine(p, h):
        wait_for(ends[p].at[pl.ds(2 * h, 2), pl.ds(1, 3)], end_recv.at[p, h])
        for s1 in (2 * h + 1, 2 * h):
            rows = ends[p][s1].reshape(32 * slots, cols[p][1])
            mixed = jnp.dot(scales[4 * p + s1], rows, preferred_element_type=F32)
            mixed = mixed[:tok] + (mixed[tok:2 * tok] + mixed[2 * tok:])
            if s1 == 0:
                acc[:, part(p)] = tokens_ref[:, part(p)].astype(F32) + mixed
            else:
                sums[p][s1 - 1] = mixed
                send(sums[p].at[s1 - 1], gots[p].at[s1 - 1], sum_send.at[p], sum_recv.at[p, s1 - 1], device(0, {AXES[p][0]: 4 - s1}))

    pl.loop(0, 1)(expert)

    for p in range(3):
        for a in range(4):
            arrived(p, 2, a)
        build(p, 2)

    wait_for(cnt_in.at[pl.ds(1, 7)], cnt_recv)
    row = jnp.zeros((1, N), F32)
    for d in range(8):
        both = sum(cnt_in[d, b][:1] for b in range(4))
        row = row + jnp.where(iota((1, N), 1) % 8 == d, both, 0.0)
    cnt_row[...] = row

    @pl.loop(0, 7)
    def _(i):
        expert(7 - i)
        drop(7 - i)
        hand_out(7 - i)

        @pl.when(i > 2)
        def _():
            pass_on(10 - i)

    pl.loop(0, 1)(drop)
    pl.loop(0, 1)(hand_out)

    @pl.loop(0, 4)
    def _(i):
        pass_on(3 - i)

    for p in range(3):
        weigh(p)
    for h in (1, 0):
        for p in range(3):
            combine(p, h)

    for p in range(3):
        total = acc[:, part(p)]
        for i in range(3):
            wait_for(gots[p].at[i], sum_recv.at[p, i])
            total = total + gots[p][i]
        out_ref[:, part(p)] = total.astype(BF16)

    wait_for(cnt_in.at[pl.ds(1, 7)], cnt_send)
    for p in range(3):
        wait_for(info_all.at[p, pl.ds(0, 3)], info_send_a.at[p])
        wait_for(info_all.at[p, pl.ds(0, 12), ids], info_send_b.at[p])
        wait_for(toks[p].at[0, pl.ds(0, 3)], tok_send_a.at[p])
        wait_for(toks[p].at[pl.ds(0, 3)], tok_send_b.at[p])
        wait_for(blks[p].at[:, pl.ds(1, 7)], blk_send.at[p])
        wait_for(mids[p].at[:, :, pl.ds(1, 7)], mid_send.at[p])
        wait_for(ends[p].at[:, pl.ds(1, 3)], end_send.at[p])
        wait_for(sums[p], sum_send.at[p])


def solution(mesh):
    def device_fn(tokens, expert_ids, gate_weights, w_in, w_out):
        tok, width = tokens.shape
        top = expert_ids.shape[1]
        ff = w_in.shape[2]
        cap = tok * top
        slots = 2 * tok * top // N
        tiles = width // 128
        sizes = [128 * (tiles // 3 + (1 if p < tiles % 3 else 0)) for p in range(3)]
        cols = [(sum(sizes[:p]), sizes[p]) for p in range(3)]
        vmem = pl.BlockSpec(memory_space=pltpu.VMEM)
        anyspace = pl.BlockSpec(memory_space=pl.ANY)
        dma = pltpu.SemaphoreType.DMA
        return pl.pallas_call(
            functools.partial(kernel, cols, cap, slots),
            out_shape=jax.ShapeDtypeStruct((tok, width), BF16),
            in_specs=[vmem, vmem, vmem, anyspace, anyspace],
            out_specs=vmem,
            scratch_shapes=[
                pltpu.VMEM((width, ff), BF16),
                pltpu.VMEM((ff, width), BF16),
                *[pltpu.VMEM((4, 4, tok, s), BF16) for s in sizes],
                *[pltpu.VMEM((4, 8, 4, slots, s), BF16) for s in sizes],
                pltpu.VMEM((2, 4, 4, 4, slots, width), BF16),
                *[pltpu.VMEM((4, 4, 8, slots, s), BF16) for s in sizes],
                *[pltpu.VMEM((4, 4, 8, slots, s), BF16) for s in sizes],
                *[pltpu.VMEM((3, tok, s), F32) for s in sizes],
                *[pltpu.VMEM((3, tok, s), F32) for s in sizes],
                pltpu.VMEM((2 * top, tok), F32),
                pltpu.VMEM((3, 16, 2 * top, tok), F32),
                pltpu.VMEM((32, tok), F32),
                pltpu.VMEM((12, 3 * tok, 32 * slots), BF16),
                pltpu.VMEM((4, 8, N), F32),
                pltpu.VMEM((8, 4, 8, N), F32),
                pltpu.VMEM((1, N), F32),
                pltpu.VMEM((tok, width), F32),
                dma((2,)), dma((3,)), dma((3,)), dma((3, 16)), dma, dma, pltpu.SemaphoreType.REGULAR, dma((3,)), dma((3,)), dma((3, 16)),
                dma((3,)), dma((3, 8)), dma((3,)), dma((3, 8)), dma((3,)), dma((3, 2)), dma((3,)), dma((3, 3)),
            ],
            compiler_params=pltpu.CompilerParams(collective_id=0, has_side_effects=True, vmem_limit_bytes=67043328),
            name='expert_layer',
        )(tokens, expert_ids.T, gate_weights.T, w_in.reshape(width, ff), w_out.reshape(ff, width))

    token_spec = P(('data', 'row', 'col'), None)
    expert_spec = P(GRID_AXES, None, None)
    return jax.shard_map(device_fn, mesh=mesh, in_specs=(token_spec, token_spec, token_spec, expert_spec, expert_spec), out_specs=token_spec, check_vma=False)
```

```python
import functools

import jax
import jax.numpy as jnp
from jax import lax
from jax.experimental import pallas as pl
from jax.experimental.pallas import tpu as pltpu
from jax.sharding import PartitionSpec as P

GRID_AXES = ('row', 'col')
F32 = jnp.float32
BF16 = jnp.bfloat16
I32 = jnp.int32
SIDE = 4
N = 2 * SIDE ** 3
MESH = pl.DeviceIdType.MESH
Z, Y, X = 0, 1, 2
AXES = ((Z, Y, X), (Y, X, Z), (X, Z, Y))


def iota(shape, dim):
    return lax.broadcasted_iota(I32, shape, dim)


def kernel(cols, cap, slots, tokens_ref, ids_ref, gates_ref, w_in_hbm, w_out_hbm, out_ref,
           w_in, w_out, tok0, tok1, tok2, blk0, blk1, blk2, recv, mid0, mid1, mid2, end0, end1, end2,
           sum0, sum1, sum2, got0, got1, got2, info, info_all, places, scales, cnt_out, cnt_in, cnt_row, acc,
           w_sem, info_send_a, info_send_b, info_recv, cnt_send, cnt_recv, line_sem, tok_send_a, tok_send_b, tok_recv,
           blk_send, blk_recv, mid_send, mid_recv, end_send, end_recv, sum_send, sum_recv):
    toks, blks = (tok0, tok1, tok2), (blk0, blk1, blk2)
    mids, ends = (mid0, mid1, mid2), (end0, end1, end2)
    sums, gots = (sum0, sum1, sum2), (got0, got1, got2)
    tok, width = tokens_ref.shape
    top = ids_ref.shape[0]
    data = lax.axis_index('data')
    core = lax.axis_index('row')
    col = lax.axis_index('col')
    here = (lax.div(col, 16), lax.rem(lax.div(col, 4), 4), lax.rem(col, 4))
    me = core * 64 + col
    weight = (16, 4, 1)

    def device(d_core, d):
        at = [lax.rem(here[a] + d[a], 4) if a in d else here[a] for a in range(3)]
        return (data, lax.rem(core + d_core, 2), at[0] * 16 + at[1] * 4 + at[2])

    def number(d_core, d):
        n = ((core + d_core) & 1) * 64
        for a in range(3):
            n = n + (((here[a] + d[a]) & 3) if a in d else here[a]) * weight[a]
        return n

    def part(p):
        return pl.ds(cols[p][0], cols[p][1])

    def send(src, dst, send_sem, recv_sem, to):
        pltpu.make_async_remote_copy(src, dst, send_sem, recv_sem, device_id=to, device_id_type=MESH).start()

    def wait_for(ref, sem):
        pltpu.make_async_copy(ref, ref, sem).wait()

    load_in = pltpu.make_async_copy(w_in_hbm, w_in, w_sem.at[0])
    load_out = pltpu.make_async_copy(w_out_hbm, w_out, w_sem.at[1])

    near = [device(0, {a: step}) for a in range(3) for step in (1, 3)] + [device(1, {})]
    barrier = pltpu.get_barrier_semaphore()
    for to in near:
        pl.semaphore_signal(barrier, inc=1, device_id=to, device_id_type=MESH)
    load_in.start()
    load_out.start()
    info[:top] = ids_ref[...].astype(F32)
    info[top:] = gates_ref[...]
    pl.semaphore_wait(barrier, len(near))

    for p in range(3):
        for step in (1, 3):
            to = device(0, {AXES[p][0]: step})
            send(info, info_all.at[p, step], info_send_a.at[p], info_recv.at[p, step], to)
            send(tokens_ref.at[:, part(p)], toks[p].at[0, step], tok_send_a.at[p], tok_recv.at[p, step], to)

    ids = pl.ds(0, top)

    def gather_on(p, a, src, ids_src):
        for step in (1, 3):
            to = device(0, {AXES[p][1]: step})
            send(ids_src, info_all.at[p, 4 * step + a, ids], info_send_b.at[p], info_recv.at[p, 4 * step + a], to)
            send(src, toks[p].at[step, a], tok_send_b.at[p], tok_recv.at[p, 4 * step + a], to)

    for p in range(3):
        gather_on(p, 0, tokens_ref.at[:, part(p)], info.at[ids])
    for p in range(3):
        toks[p][0, 0] = tokens_ref[:, part(p)]
        info_all[p, 0] = info[...]

    def arrived(p, b, a):
        what = info_all.at[p, a] if b == 0 else info_all.at[p, 4 * b + a, ids]
        wait_for(what, info_recv.at[p, 4 * b + a])
        wait_for(toks[p].at[b, a], tok_recv.at[p, 4 * b + a])

    half = tok // 2
    for p in range(3):
        t = toks[p]
        for step, rows in ((1, pl.ds(0, half)), (3, pl.ds(half, half))):
            arrived(p, 0, step)
            to = device(0, {AXES[p][0]: step})
            if step == 1:
                send(info_all.at[p, 1], info_all.at[p, 2], info_send_a.at[p], info_recv.at[p, 2], to)
            send(t.at[0, step, rows], t.at[0, 2, rows], tok_send_a.at[p], tok_recv.at[p, 2], to)
            gather_on(p, step, t.at[0, step], info_all.at[p, step, ids])

    for p in range(3):
        arrived(p, 0, 2)
        gather_on(p, 2, toks[p].at[0, 2], info_all.at[p, 2, ids])

    pl.semaphore_signal(line_sem, inc=1, device_id=near[6], device_id_type=MESH)
    pl.semaphore_wait(line_sem, 1)

    later = (iota((tok, tok), 0) < iota((tok, tok), 1)).astype(BF16)

    def where_in(p, d_core, s1, s2, s3):
        at = [None] * 3
        for axis, s in zip(AXES[p], (s1, s2, s3)):
            at[axis] = s
        return (d_core, *at)

    def build(p, b):
        t, blk = toks[p], blks[p]
        d3 = AXES[p][2]
        dest = iota((8, tok), 0)
        expert_id = number(dest >> 2, {d3: dest & 3}).astype(F32)[None]
        mark = jnp.zeros((4, 8, tok), F32)
        for j in range(top):
            mark = jnp.where(info_all[p, pl.ds(4 * b, 4), j:j + 1, :] == expert_id, 1.0, mark)
        mark = mark.reshape(32, tok)
        place = jnp.dot(mark.astype(BF16), later, preferred_element_type=F32)
        places[...] = jnp.where(mark > 0, place, -1.0)
        if p == 0:
            wide = [jnp.zeros((32, tok), F32)] * 4
            wide[b] = mark
            wide = jnp.concatenate(wide, axis=0).astype(BF16)
            cnt_out[b] = lax.dot_general(jnp.ones((8, tok), BF16), wide, (((1,), (1,)), ((), ())), preferred_element_type=F32)
            cnt_in[0, b] = cnt_out[b]

            @pl.loop(1, 8)
            def _(d):
                send(cnt_out.at[b], cnt_in.at[d, b], cnt_send, cnt_recv, device(lax.div(d, 4), {d3: lax.rem(d, 4)}))

        @pl.loop(0, 4)
        def _(a):
            place = places[pl.ds(a * 8, 8), :]
            pick = place[:, None, :] == iota((8, slots, tok), 1).astype(F32)
            pick = jnp.where(pick, 1.0, 0.0).reshape(8 * slots, tok).astype(BF16)
            rows = jnp.dot(pick, t[b, a], preferred_element_type=F32).astype(BF16).reshape(8, slots, cols[p][1])
            blk[b, :, a] = rows
            recv[where_in(p, 0, a, b, 0) + (slice(None), part(p))] = rows[0]

        for h in range(2):
            @pl.loop(1, 8)
            def _(d):
                d_core, s3 = lax.div(d, 4), lax.rem(d, 4)
                high = {AXES[p][0]: h, AXES[p][1]: b // 2, AXES[p][2]: lax.div(s3, 2)}
                cube = high[Z] * 4 + high[Y] * 2 + high[X]
                send(blk.at[b, d, pl.ds(2 * h, 2)],
                     recv.at[where_in(p, d_core, pl.ds(2 * h, 2), b, s3) + (slice(None), part(p))],
                     blk_send.at[p], blk_recv.at[p, cube], device(d_core, {AXES[p][2]: s3}))

    def relay(p, step, a):
        t, to = toks[p], device(0, {AXES[p][1]: step})
        arrived(p, step, a)
        send(info_all.at[p, 4 * step + a, ids], info_all.at[p, 8 + a, ids], info_send_b.at[p], info_recv.at[p, 8 + a], to)
        send(t.at[step, a], t.at[2, a], tok_send_b.at[p], tok_recv.at[p, 8 + a], to)

    for p in range(3):
        relay(p, 1, 0)
    for p in range(3):
        build(p, 0)

    for p, step, a in [(p, step, a) for step, a in ((3, 1), (3, 3), (1, 2)) for p in range(3)]:
        relay(p, step, a)

    for step, rest in ((1, (1, 3)), (3, (0, 2))):
        for p in range(3):
            for a in rest:
                arrived(p, step, a)
            build(p, step)

    load_in.wait()
    load_out.wait()

    def halves(j):
        return (lax.div(j, 4), lax.rem(lax.div(j, 2), 2), lax.rem(j, 2))

    def wait_blocks(p, h3, refs, sem):
        @pl.when(h3 == 0)
        def _():
            wait_for(refs.at[0, pl.ds(0, 3)], sem)

        @pl.when(h3 == 1)
        def _():
            wait_for(refs.at[0, pl.ds(0, 4)], sem)

    def expert(j):
        high = halves(j)
        pair = [pl.ds(2 * h, 2) for h in high]
        for p in range(3):
            wait_blocks(p, high[AXES[p][2]], blks[p], blk_recv.at[p, j])
        cube = (slice(None), *pair)
        x = recv[cube].reshape(16 * slots, width)
        hidden = jax.nn.gelu(jnp.dot(x, w_in[...], preferred_element_type=F32)).astype(BF16)
        o = jnp.dot(hidden, w_out[...], preferred_element_type=F32).astype(BF16)
        recv[cube] = o.reshape(2, 2, 2, 2, slots, width)

    def drop(j):
        high = halves(j)
        cube = (slice(None), *[pl.ds(2 * h, 2) for h in high])
        rows = 16 * slots
        r = iota((rows, N), 0)
        i = r // slots
        taker = number((i >> 3) & 1, {Z: 4 - (2 * high[Z] + ((i >> 2) & 1)), Y: 4 - (2 * high[Y] + ((i >> 1) & 1)), X: 4 - (2 * high[X] + (i & 1))})
        c = iota((rows, N), 1)
        d1, d2, d3 = AXES[0]
        source = number((c >> 2) & 1, {d1: 4 - ((c >> 3) & 3), d2: 4 - (c >> 5), d3: 4 - (c & 3)})
        before = jnp.sum(jnp.where(source < taker, cnt_row[...], 0.0), axis=1, keepdims=True)
        keep = before + (iota((rows, 1), 0) % slots).astype(F32) < float(cap)
        o = recv[cube].reshape(rows, width)
        recv[cube] = jnp.where(keep, o, jnp.zeros_like(o)).reshape(2, 2, 2, 2, slots, width)

    def hand_out(j):
        high = halves(j)
        pair = [pl.ds(2 * h, 2) for h in high]
        for p in range(3):
            d3 = AXES[p][2]
            rest = [pair[a] for a in range(3) if a != d3]

            def along(s3):
                return tuple(s3 if a == d3 else pair[a] for a in range(3))

            @pl.when(high[d3] == 0)
            def _():
                mids[p][(*rest, 0)] = recv[(0, *along(0), slice(None), part(p))]

            @pl.loop(jnp.where(high[d3] == 0, 1, 0), 4)
            def _(i):
                d_core, s3 = lax.div(i, 2), 2 * high[d3] + lax.rem(i, 2)
                send(recv.at[(d_core, *along(s3), slice(None), part(p))], mids[p].at[(*rest, d_core * 4 + s3)],
                     mid_send.at[p], mid_recv.at[p, j], device(d_core, {d3: 4 - s3}))

    def middle(p, s1, s2):
        d1, d2 = AXES[p][:2]
        return (s1, s2) if d1 < d2 else (s2, s1)

    def pass_on(j):
        high = halves(j)
        for p in range(3):
            d1, d2, d3 = AXES[p]

            @pl.when(high[d3] == 0)
            def _():
                wait_blocks(p, 1, blks[p], mid_recv.at[p, j + (4, 2, 1)[d3]])
                wait_blocks(p, 0, blks[p], mid_recv.at[p, j])
                first = pl.ds(2 * high[d1], 2)

                @pl.when(high[d2] == 0)
                def _():
                    ends[p][first, 0] = mids[p][middle(p, first, 0)]

                @pl.loop(jnp.where(high[d2] == 0, 1, 2 * high[d2]), 2 * high[d2] + 2)
                def _(s2):
                    send(mids[p].at[middle(p, first, s2)], ends[p].at[first, s2],
                         end_send.at[p], end_recv.at[p, high[d1]], device(0, {d2: 4 - s2}))

    def weigh(p):
        d1, d2, d3 = AXES[p]
        e = iota((32, tok), 0)
        expert_id = number((e >> 2) & 1, {d2: e >> 3, d3: e & 3}).astype(F32)

        @pl.loop(0, 4)
        def _(s1):
            ids, gts = info_all[p, s1, :top], info_all[p, s1, top:]
            mark = jnp.zeros((32, tok), F32)
            gate = jnp.zeros((32, tok), F32)
            for j in range(top):
                hit = ids[j:j + 1, :] == expert_id
                mark = jnp.where(hit, 1.0, mark)
                gate = jnp.where(hit, gts[j:j + 1, :], gate)
            place = jnp.dot(mark.astype(BF16), later, preferred_element_type=F32)
            place = jnp.where(mark > 0, place, -1.0)
            scale = jnp.where(place[:, None, :] == iota((32, slots, tok), 1).astype(F32), gate[:, None, :], 0.0)
            scale = scale.reshape(32 * slots, tok).T
            high = scale.astype(BF16)
            left = scale - high.astype(F32)
            mid = left.astype(BF16)
            low = (left - mid.astype(F32)).astype(BF16)
            scales[4 * p + s1] = jnp.concatenate([high, mid, low], axis=0)

    def combine(p, s1):
        rows = ends[p][s1].reshape(32 * slots, cols[p][1])
        mixed = jnp.dot(scales[4 * p + s1], rows, preferred_element_type=F32)
        mixed = mixed[:tok] + (mixed[tok:2 * tok] + mixed[2 * tok:])
        if s1 == 0:
            acc[:, part(p)] = tokens_ref[:, part(p)].astype(F32) + mixed
        else:
            sums[p][s1 - 1] = mixed
            send(sums[p].at[s1 - 1], gots[p].at[s1 - 1], sum_send.at[p], sum_recv.at[p, s1 - 1], device(0, {AXES[p][0]: 4 - s1}))

    pl.loop(0, 1)(expert)

    for p in range(3):
        for a in range(4):
            arrived(p, 2, a)
        build(p, 2)

    wait_for(cnt_in.at[pl.ds(1, 7)], cnt_recv)
    row = jnp.zeros((1, N), F32)
    for d in range(8):
        both = sum(cnt_in[d, b][:1] for b in range(4))
        row = row + jnp.where(iota((1, N), 1) % 8 == d, both, 0.0)
    cnt_row[...] = row
    pl.loop(0, 1)(drop)
    pl.loop(0, 1)(hand_out)

    @pl.loop(0, 7)
    def _(i):
        expert(7 - i)
        drop(7 - i)
        hand_out(7 - i)

        @pl.when(i > 2)
        def _():
            pass_on(10 - i)

    @pl.loop(0, 4)
    def _(i):
        pass_on(3 - i)

    for p in range(3):
        weigh(p)
    for p in range(3):
        wait_for(ends[p].at[pl.ds(2, 2), pl.ds(1, 3)], end_recv.at[p, 1])
        combine(p, 2)
        combine(p, 3)
    for p in range(3):
        wait_for(ends[p].at[pl.ds(0, 2), pl.ds(1, 3)], end_recv.at[p, 0])
        combine(p, 1)
    for p in range(3):
        combine(p, 0)

    for p in range(3):
        total = acc[:, part(p)]
        for i in range(3):
            wait_for(gots[p].at[i], sum_recv.at[p, i])
            total = total + gots[p][i]
        out_ref[:, part(p)] = total.astype(BF16)

    wait_for(cnt_in.at[pl.ds(1, 7)], cnt_send)
    for p in range(3):
        wait_for(info_all.at[p, pl.ds(0, 3)], info_send_a.at[p])
        wait_for(info_all.at[p, pl.ds(0, 12), ids], info_send_b.at[p])
        wait_for(toks[p].at[0, pl.ds(0, 3)], tok_send_a.at[p])
        wait_for(toks[p].at[pl.ds(0, 3)], tok_send_b.at[p])
        wait_for(blks[p].at[:, pl.ds(1, 7)], blk_send.at[p])
        wait_for(mids[p].at[:, :, pl.ds(1, 7)], mid_send.at[p])
        wait_for(ends[p].at[:, pl.ds(1, 3)], end_send.at[p])
        wait_for(sums[p], sum_send.at[p])


def solution(mesh):
    def device_fn(tokens, expert_ids, gate_weights, w_in, w_out):
        tok, width = tokens.shape
        top = expert_ids.shape[1]
        ff = w_in.shape[2]
        cap = tok * top
        slots = 2 * tok * top // N
        tiles = width // 128
        sizes = [128 * (tiles // 3 + (1 if p < tiles % 3 else 0)) for p in range(3)]
        cols = [(sum(sizes[:p]), sizes[p]) for p in range(3)]
        vmem = pl.BlockSpec(memory_space=pltpu.VMEM)
        anyspace = pl.BlockSpec(memory_space=pl.ANY)
        dma = pltpu.SemaphoreType.DMA
        return pl.pallas_call(
            functools.partial(kernel, cols, cap, slots),
            out_shape=jax.ShapeDtypeStruct((tok, width), BF16),
            in_specs=[vmem, vmem, vmem, anyspace, anyspace],
            out_specs=vmem,
            scratch_shapes=[
                pltpu.VMEM((width, ff), BF16),
                pltpu.VMEM((ff, width), BF16),
                *[pltpu.VMEM((4, 4, tok, s), BF16) for s in sizes],
                *[pltpu.VMEM((4, 8, 4, slots, s), BF16) for s in sizes],
                pltpu.VMEM((2, 4, 4, 4, slots, width), BF16),
                *[pltpu.VMEM((4, 4, 8, slots, s), BF16) for s in sizes],
                *[pltpu.VMEM((4, 4, 8, slots, s), BF16) for s in sizes],
                *[pltpu.VMEM((3, tok, s), F32) for s in sizes],
                *[pltpu.VMEM((3, tok, s), F32) for s in sizes],
                pltpu.VMEM((2 * top, tok), F32),
                pltpu.VMEM((3, 16, 2 * top, tok), F32),
                pltpu.VMEM((32, tok), F32),
                pltpu.VMEM((12, 3 * tok, 32 * slots), BF16),
                pltpu.VMEM((4, 8, N), F32),
                pltpu.VMEM((8, 4, 8, N), F32),
                pltpu.VMEM((1, N), F32),
                pltpu.VMEM((tok, width), F32),
                dma((2,)), dma((3,)), dma((3,)), dma((3, 16)), dma, dma, pltpu.SemaphoreType.REGULAR, dma((3,)), dma((3,)), dma((3, 16)),
                dma((3,)), dma((3, 8)), dma((3,)), dma((3, 8)), dma((3,)), dma((3, 2)), dma((3,)), dma((3, 3)),
            ],
            compiler_params=pltpu.CompilerParams(collective_id=0, has_side_effects=True, vmem_limit_bytes=67043328),
            name='expert_layer',
        )(tokens, expert_ids.T, gate_weights.T, w_in.reshape(width, ff), w_out.reshape(ff, width))

    token_spec = P(('data', 'row', 'col'), None)
    expert_spec = P(GRID_AXES, None, None)
    return jax.shard_map(device_fn, mesh=mesh, in_specs=(token_spec, token_spec, token_spec, expert_spec, expert_spec), out_specs=token_spec, check_vma=False)
```

```python
import functools

import jax
import jax.numpy as jnp
from jax import lax
from jax.experimental import pallas as pl
from jax.experimental.pallas import tpu as pltpu
from jax.sharding import PartitionSpec as P

GRID_AXES = ('row', 'col')
F32 = jnp.float32
BF16 = jnp.bfloat16
I32 = jnp.int32
SIDE = 4
N = 2 * SIDE ** 3
MESH = pl.DeviceIdType.MESH
Z, Y, X = 0, 1, 2
AXES = ((Z, Y, X), (Y, X, Z), (X, Z, Y))


def iota(shape, dim):
    return lax.broadcasted_iota(I32, shape, dim)


def kernel(cols, cap, slots, tokens_ref, ids_ref, gates_ref, w_in_hbm, w_out_hbm, out_ref,
           w_in, w_out, tok0, tok1, tok2, blk0, blk1, blk2, recv, mid0, mid1, mid2, end0, end1, end2,
           sum0, sum1, sum2, got0, got1, got2, info, info_all, places, scales, cnt_out, cnt_in, cnt_row, acc,
           w_sem, info_send_a, info_send_b, info_recv, cnt_send, cnt_recv, line_sem, tok_send_a, tok_send_b, tok_recv,
           blk_send, blk_recv, mid_send, mid_recv, end_send, end_recv, sum_send, sum_recv):
    toks, blks = (tok0, tok1, tok2), (blk0, blk1, blk2)
    mids, ends = (mid0, mid1, mid2), (end0, end1, end2)
    sums, gots = (sum0, sum1, sum2), (got0, got1, got2)
    tok, width = tokens_ref.shape
    top = ids_ref.shape[0]
    data = lax.axis_index('data')
    core = lax.axis_index('row')
    col = lax.axis_index('col')
    here = (lax.div(col, 16), lax.rem(lax.div(col, 4), 4), lax.rem(col, 4))
    me = core * 64 + col
    weight = (16, 4, 1)

    def device(d_core, d):
        at = [lax.rem(here[a] + d[a], 4) if a in d else here[a] for a in range(3)]
        return (data, lax.rem(core + d_core, 2), at[0] * 16 + at[1] * 4 + at[2])

    def number(d_core, d):
        n = ((core + d_core) & 1) * 64
        for a in range(3):
            n = n + (((here[a] + d[a]) & 3) if a in d else here[a]) * weight[a]
        return n

    def part(p):
        return pl.ds(cols[p][0], cols[p][1])

    def send(src, dst, send_sem, recv_sem, to):
        pltpu.make_async_remote_copy(src, dst, send_sem, recv_sem, device_id=to, device_id_type=MESH).start()

    def wait_for(ref, sem):
        pltpu.make_async_copy(ref, ref, sem).wait()

    load_in = pltpu.make_async_copy(w_in_hbm, w_in, w_sem.at[0])
    load_out = pltpu.make_async_copy(w_out_hbm, w_out, w_sem.at[1])

    near = [device(0, {a: step}) for a in range(3) for step in (1, 3)] + [device(1, {})]
    barrier = pltpu.get_barrier_semaphore()
    for to in near:
        pl.semaphore_signal(barrier, inc=1, device_id=to, device_id_type=MESH)
    load_in.start()
    load_out.start()
    info[:top] = ids_ref[...].astype(F32)
    info[top:] = gates_ref[...]
    pl.semaphore_wait(barrier, len(near))

    for p in range(3):
        for step in (1, 3):
            to = device(0, {AXES[p][0]: step})
            send(info, info_all.at[p, step], info_send_a.at[p], info_recv.at[p, step], to)
            send(tokens_ref.at[:, part(p)], toks[p].at[0, step], tok_send_a.at[p], tok_recv.at[p, step], to)

    ids = pl.ds(0, top)

    def gather_on(p, a, src, ids_src):
        for step in (1, 3):
            to = device(0, {AXES[p][1]: step})
            send(ids_src, info_all.at[p, 4 * step + a, ids], info_send_b.at[p], info_recv.at[p, 4 * step + a], to)
            send(src, toks[p].at[step, a], tok_send_b.at[p], tok_recv.at[p, 4 * step + a], to)

    for p in range(3):
        gather_on(p, 0, tokens_ref.at[:, part(p)], info.at[ids])
    for p in range(3):
        toks[p][0, 0] = tokens_ref[:, part(p)]
        info_all[p, 0] = info[...]

    def arrived(p, b, a):
        what = info_all.at[p, a] if b == 0 else info_all.at[p, 4 * b + a, ids]
        wait_for(what, info_recv.at[p, 4 * b + a])
        wait_for(toks[p].at[b, a], tok_recv.at[p, 4 * b + a])

    half = tok // 2
    for p in range(3):
        t = toks[p]
        for step, rows in ((1, pl.ds(0, half)), (3, pl.ds(half, half))):
            arrived(p, 0, step)
            to = device(0, {AXES[p][0]: step})
            if step == 1:
                send(info_all.at[p, 1], info_all.at[p, 2], info_send_a.at[p], info_recv.at[p, 2], to)
            send(t.at[0, step, rows], t.at[0, 2, rows], tok_send_a.at[p], tok_recv.at[p, 2], to)
            gather_on(p, step, t.at[0, step], info_all.at[p, step, ids])

    for p in range(3):
        arrived(p, 0, 2)
        gather_on(p, 2, toks[p].at[0, 2], info_all.at[p, 2, ids])

    pl.semaphore_signal(line_sem, inc=1, device_id=near[6], device_id_type=MESH)
    pl.semaphore_wait(line_sem, 1)

    later = (iota((tok, tok), 0) < iota((tok, tok), 1)).astype(BF16)

    def where_in(p, d_core, s1, s2, s3):
        at = [None] * 3
        for axis, s in zip(AXES[p], (s1, s2, s3)):
            at[axis] = s
        return (d_core, *at)

    def build(p, b):
        t, blk = toks[p], blks[p]
        d3 = AXES[p][2]
        dest = iota((8, tok), 0)
        expert_id = number(dest >> 2, {d3: dest & 3}).astype(F32)[None]
        mark = jnp.zeros((4, 8, tok), F32)
        for j in range(top):
            mark = jnp.where(info_all[p, pl.ds(4 * b, 4), j:j + 1, :] == expert_id, 1.0, mark)
        mark = mark.reshape(32, tok)
        place = jnp.dot(mark.astype(BF16), later, preferred_element_type=F32)
        places[...] = jnp.where(mark > 0, place, -1.0)
        if p == 0:
            wide = [jnp.zeros((32, tok), F32)] * 4
            wide[b] = mark
            wide = jnp.concatenate(wide, axis=0).astype(BF16)
            cnt_out[b] = lax.dot_general(jnp.ones((8, tok), BF16), wide, (((1,), (1,)), ((), ())), preferred_element_type=F32)
            cnt_in[0, b] = cnt_out[b]

            @pl.loop(1, 8)
            def _(d):
                send(cnt_out.at[b], cnt_in.at[d, b], cnt_send, cnt_recv, device(lax.div(d, 4), {d3: lax.rem(d, 4)}))

        @pl.loop(0, 4)
        def _(a):
            place = places[pl.ds(a * 8, 8), :]
            pick = place[:, None, :] == iota((8, slots, tok), 1).astype(F32)
            pick = jnp.where(pick, 1.0, 0.0).reshape(8 * slots, tok).astype(BF16)
            rows = jnp.dot(pick, t[b, a], preferred_element_type=F32).astype(BF16).reshape(8, slots, cols[p][1])
            blk[b, :, a] = rows
            recv[where_in(p, 0, a, b, 0) + (slice(None), part(p))] = rows[0]

    def post(b):
        for h in range(2):
            @pl.loop(1, 8)
            def _(d):
                d_core, s3 = lax.div(d, 4), lax.rem(d, 4)
                for p in range(3):
                    high = {AXES[p][0]: h, AXES[p][1]: b // 2, AXES[p][2]: lax.div(s3, 2)}
                    cube = high[Z] * 4 + high[Y] * 2 + high[X]
                    send(blks[p].at[b, d, pl.ds(2 * h, 2)],
                         recv.at[where_in(p, d_core, pl.ds(2 * h, 2), b, s3) + (slice(None), part(p))],
                         blk_send.at[p], blk_recv.at[p, cube], device(d_core, {AXES[p][2]: s3}))

    def relay(p, step, a):
        t, to = toks[p], device(0, {AXES[p][1]: step})
        arrived(p, step, a)
        send(info_all.at[p, 4 * step + a, ids], info_all.at[p, 8 + a, ids], info_send_b.at[p], info_recv.at[p, 8 + a], to)
        send(t.at[step, a], t.at[2, a], tok_send_b.at[p], tok_recv.at[p, 8 + a], to)

    for p in range(3):
        relay(p, 1, 0)
    for p in range(3):
        build(p, 0)
    post(0)

    for p, step, a in [(p, step, a) for step, a in ((3, 1), (3, 3), (1, 2)) for p in range(3)]:
        relay(p, step, a)

    for step, rest in ((1, (1, 3)), (3, (0, 2))):
        for p in range(3):
            for a in rest:
                arrived(p, step, a)
            build(p, step)
        post(step)

    load_in.wait()
    load_out.wait()

    def halves(j):
        return (lax.div(j, 4), lax.rem(lax.div(j, 2), 2), lax.rem(j, 2))

    def wait_blocks(p, h3, refs, sem):
        @pl.when(h3 == 0)
        def _():
            wait_for(refs.at[0, pl.ds(0, 3)], sem)

        @pl.when(h3 == 1)
        def _():
            wait_for(refs.at[0, pl.ds(0, 4)], sem)

    def expert(j):
        high = halves(j)
        pair = [pl.ds(2 * h, 2) for h in high]
        for p in range(3):
            wait_blocks(p, high[AXES[p][2]], blks[p], blk_recv.at[p, j])
        cube = (slice(None), *pair)
        x = recv[cube].reshape(16 * slots, width)
        hidden = jax.nn.gelu(jnp.dot(x, w_in[...], preferred_element_type=F32)).astype(BF16)
        o = jnp.dot(hidden, w_out[...], preferred_element_type=F32).astype(BF16)
        recv[cube] = o.reshape(2, 2, 2, 2, slots, width)

    def drop(j):
        high = halves(j)
        cube = (slice(None), *[pl.ds(2 * h, 2) for h in high])
        rows = 16 * slots
        r = iota((rows, N), 0)
        i = r // slots
        taker = number((i >> 3) & 1, {Z: 4 - (2 * high[Z] + ((i >> 2) & 1)), Y: 4 - (2 * high[Y] + ((i >> 1) & 1)), X: 4 - (2 * high[X] + (i & 1))})
        c = iota((rows, N), 1)
        d1, d2, d3 = AXES[0]
        source = number((c >> 2) & 1, {d1: 4 - ((c >> 3) & 3), d2: 4 - (c >> 5), d3: 4 - (c & 3)})
        before = jnp.sum(jnp.where(source < taker, cnt_row[...], 0.0), axis=1, keepdims=True)
        keep = before + (iota((rows, 1), 0) % slots).astype(F32) < float(cap)
        o = recv[cube].reshape(rows, width)
        recv[cube] = jnp.where(keep, o, jnp.zeros_like(o)).reshape(2, 2, 2, 2, slots, width)

    def hand_out(j):
        high = halves(j)
        pair = [pl.ds(2 * h, 2) for h in high]
        for p in range(3):
            d3 = AXES[p][2]
            rest = [pair[a] for a in range(3) if a != d3]

            def along(s3):
                return tuple(s3 if a == d3 else pair[a] for a in range(3))

            @pl.when(high[d3] == 0)
            def _():
                mids[p][(*rest, 0)] = recv[(0, *along(0), slice(None), part(p))]

        @pl.loop(0, 4)
        def _(i):
            d_core = lax.div(i, 2)
            for p in range(3):
                d3 = AXES[p][2]
                s3 = 2 * high[d3] + lax.rem(i, 2)
                rest = [pair[a] for a in range(3) if a != d3]
                at = tuple(s3 if a == d3 else pair[a] for a in range(3))

                @pl.when(i + high[d3] > 0)
                def _():
                    send(recv.at[(d_core, *at, slice(None), part(p))], mids[p].at[(*rest, d_core * 4 + s3)],
                         mid_send.at[p], mid_recv.at[p, j], device(d_core, {d3: 4 - s3}))

    def middle(p, s1, s2):
        d1, d2 = AXES[p][:2]
        return (s1, s2) if d1 < d2 else (s2, s1)

    def pass_on(j):
        high = halves(j)
        for p in range(3):
            d1, d2, d3 = AXES[p]

            @pl.when(high[d3] == 0)
            def _():
                wait_blocks(p, 1, blks[p], mid_recv.at[p, j + (4, 2, 1)[d3]])
                wait_blocks(p, 0, blks[p], mid_recv.at[p, j])
                first = pl.ds(2 * high[d1], 2)

                @pl.when(high[d2] == 0)
                def _():
                    ends[p][first, 0] = mids[p][middle(p, first, 0)]

                @pl.loop(jnp.where(high[d2] == 0, 1, 2 * high[d2]), 2 * high[d2] + 2)
                def _(s2):
                    send(mids[p].at[middle(p, first, s2)], ends[p].at[first, s2],
                         end_send.at[p], end_recv.at[p, high[d1]], device(0, {d2: 4 - s2}))

    def weigh(p):
        d1, d2, d3 = AXES[p]
        e = iota((32, tok), 0)
        expert_id = number((e >> 2) & 1, {d2: e >> 3, d3: e & 3}).astype(F32)

        @pl.loop(0, 4)
        def _(s1):
            ids, gts = info_all[p, s1, :top], info_all[p, s1, top:]
            mark = jnp.zeros((32, tok), F32)
            gate = jnp.zeros((32, tok), F32)
            for j in range(top):
                hit = ids[j:j + 1, :] == expert_id
                mark = jnp.where(hit, 1.0, mark)
                gate = jnp.where(hit, gts[j:j + 1, :], gate)
            place = jnp.dot(mark.astype(BF16), later, preferred_element_type=F32)
            place = jnp.where(mark > 0, place, -1.0)
            scale = jnp.where(place[:, None, :] == iota((32, slots, tok), 1).astype(F32), gate[:, None, :], 0.0)
            scale = scale.reshape(32 * slots, tok).T
            high = scale.astype(BF16)
            left = scale - high.astype(F32)
            mid = left.astype(BF16)
            low = (left - mid.astype(F32)).astype(BF16)
            scales[4 * p + s1] = jnp.concatenate([high, mid, low], axis=0)

    def combine(p, s1):
        rows = ends[p][s1].reshape(32 * slots, cols[p][1])
        mixed = jnp.dot(scales[4 * p + s1], rows, preferred_element_type=F32)
        mixed = mixed[:tok] + (mixed[tok:2 * tok] + mixed[2 * tok:])
        if s1 == 0:
            acc[:, part(p)] = tokens_ref[:, part(p)].astype(F32) + mixed
        else:
            sums[p][s1 - 1] = mixed
            send(sums[p].at[s1 - 1], gots[p].at[s1 - 1], sum_send.at[p], sum_recv.at[p, s1 - 1], device(0, {AXES[p][0]: 4 - s1}))

    pl.loop(0, 1)(expert)

    for p in range(3):
        for a in range(4):
            arrived(p, 2, a)
        build(p, 2)
    post(2)

    wait_for(cnt_in.at[pl.ds(1, 7)], cnt_recv)
    row = jnp.zeros((1, N), F32)
    for d in range(8):
        both = sum(cnt_in[d, b][:1] for b in range(4))
        row = row + jnp.where(iota((1, N), 1) % 8 == d, both, 0.0)
    cnt_row[...] = row
    pl.loop(0, 1)(drop)
    pl.loop(0, 1)(hand_out)

    @pl.loop(0, 7)
    def _(i):
        expert(7 - i)
        drop(7 - i)
        hand_out(7 - i)

        @pl.when(i > 2)
        def _():
            pass_on(10 - i)

    @pl.loop(0, 4)
    def _(i):
        pass_on(3 - i)

    for p in range(3):
        weigh(p)
    for p in range(3):
        wait_for(ends[p].at[pl.ds(2, 2), pl.ds(1, 3)], end_recv.at[p, 1])
        combine(p, 2)
        combine(p, 3)
    for p in range(3):
        wait_for(ends[p].at[pl.ds(0, 2), pl.ds(1, 3)], end_recv.at[p, 0])
        combine(p, 1)
    for p in range(3):
        combine(p, 0)

    for p in range(3):
        total = acc[:, part(p)]
        for i in range(3):
            wait_for(gots[p].at[i], sum_recv.at[p, i])
            total = total + gots[p][i]
        out_ref[:, part(p)] = total.astype(BF16)

    wait_for(cnt_in.at[pl.ds(1, 7)], cnt_send)
    for p in range(3):
        wait_for(info_all.at[p, pl.ds(0, 3)], info_send_a.at[p])
        wait_for(info_all.at[p, pl.ds(0, 12), ids], info_send_b.at[p])
        wait_for(toks[p].at[0, pl.ds(0, 3)], tok_send_a.at[p])
        wait_for(toks[p].at[pl.ds(0, 3)], tok_send_b.at[p])
        wait_for(blks[p].at[:, pl.ds(1, 7)], blk_send.at[p])
        wait_for(mids[p].at[:, :, pl.ds(1, 7)], mid_send.at[p])
        wait_for(ends[p].at[:, pl.ds(1, 3)], end_send.at[p])
        wait_for(sums[p], sum_send.at[p])


def solution(mesh):
    def device_fn(tokens, expert_ids, gate_weights, w_in, w_out):
        tok, width = tokens.shape
        top = expert_ids.shape[1]
        ff = w_in.shape[2]
        cap = tok * top
        slots = 2 * tok * top // N
        tiles = width // 128
        sizes = [128 * (tiles // 3 + (1 if p < tiles % 3 else 0)) for p in range(3)]
        cols = [(sum(sizes[:p]), sizes[p]) for p in range(3)]
        vmem = pl.BlockSpec(memory_space=pltpu.VMEM)
        anyspace = pl.BlockSpec(memory_space=pl.ANY)
        dma = pltpu.SemaphoreType.DMA
        return pl.pallas_call(
            functools.partial(kernel, cols, cap, slots),
            out_shape=jax.ShapeDtypeStruct((tok, width), BF16),
            in_specs=[vmem, vmem, vmem, anyspace, anyspace],
            out_specs=vmem,
            scratch_shapes=[
                pltpu.VMEM((width, ff), BF16),
                pltpu.VMEM((ff, width), BF16),
                *[pltpu.VMEM((4, 4, tok, s), BF16) for s in sizes],
                *[pltpu.VMEM((4, 8, 4, slots, s), BF16) for s in sizes],
                pltpu.VMEM((2, 4, 4, 4, slots, width), BF16),
                *[pltpu.VMEM((4, 4, 8, slots, s), BF16) for s in sizes],
                *[pltpu.VMEM((4, 4, 8, slots, s), BF16) for s in sizes],
                *[pltpu.VMEM((3, tok, s), F32) for s in sizes],
                *[pltpu.VMEM((3, tok, s), F32) for s in sizes],
                pltpu.VMEM((2 * top, tok), F32),
                pltpu.VMEM((3, 16, 2 * top, tok), F32),
                pltpu.VMEM((32, tok), F32),
                pltpu.VMEM((12, 3 * tok, 32 * slots), BF16),
                pltpu.VMEM((4, 8, N), F32),
                pltpu.VMEM((8, 4, 8, N), F32),
                pltpu.VMEM((1, N), F32),
                pltpu.VMEM((tok, width), F32),
                dma((2,)), dma((3,)), dma((3,)), dma((3, 16)), dma, dma, pltpu.SemaphoreType.REGULAR, dma((3,)), dma((3,)), dma((3, 16)),
                dma((3,)), dma((3, 8)), dma((3,)), dma((3, 8)), dma((3,)), dma((3, 2)), dma((3,)), dma((3, 3)),
            ],
            compiler_params=pltpu.CompilerParams(collective_id=0, has_side_effects=True, vmem_limit_bytes=67043328),
            name='expert_layer',
        )(tokens, expert_ids.T, gate_weights.T, w_in.reshape(width, ff), w_out.reshape(ff, width))

    token_spec = P(('data', 'row', 'col'), None)
    expert_spec = P(GRID_AXES, None, None)
    return jax.shard_map(device_fn, mesh=mesh, in_specs=(token_spec, token_spec, token_spec, expert_spec, expert_spec), out_specs=token_spec, check_vma=False)
```

```python
import functools

import jax
import jax.numpy as jnp
from jax import lax
from jax.experimental import pallas as pl
from jax.experimental.pallas import tpu as pltpu
from jax.sharding import PartitionSpec as P

GRID_AXES = ('row', 'col')
F32 = jnp.float32
BF16 = jnp.bfloat16
I32 = jnp.int32
SIDE = 4
N = 2 * SIDE ** 3
MESH = pl.DeviceIdType.MESH
Z, Y, X = 0, 1, 2
AXES = ((Z, Y, X), (Y, X, Z), (X, Z, Y))


def iota(shape, dim):
    return lax.broadcasted_iota(I32, shape, dim)


def kernel(cols, cap, slots, tokens_ref, ids_ref, gates_ref, w_in_hbm, w_out_hbm, out_ref,
           w_in, w_out, tok0, tok1, tok2, blk0, blk1, blk2, recv, mid0, mid1, mid2, end0, end1, end2,
           sum0, sum1, sum2, got0, got1, got2, info, info_all, places, scales, cnt_out, cnt_in, cnt_row, acc,
           w_sem, info_send_a, info_send_b, info_recv, cnt_send, cnt_recv, line_sem, tok_send_a, tok_send_b, tok_recv,
           blk_send, blk_recv, mid_send, mid_recv, end_send, end_recv, sum_send, sum_recv):
    toks, blks = (tok0, tok1, tok2), (blk0, blk1, blk2)
    mids, ends = (mid0, mid1, mid2), (end0, end1, end2)
    sums, gots = (sum0, sum1, sum2), (got0, got1, got2)
    tok, width = tokens_ref.shape
    top = ids_ref.shape[0]
    data = lax.axis_index('data')
    core = lax.axis_index('row')
    col = lax.axis_index('col')
    here = (lax.div(col, 16), lax.rem(lax.div(col, 4), 4), lax.rem(col, 4))
    me = core * 64 + col
    weight = (16, 4, 1)

    def device(d_core, d):
        at = [lax.rem(here[a] + d[a], 4) if a in d else here[a] for a in range(3)]
        return (data, lax.rem(core + d_core, 2), at[0] * 16 + at[1] * 4 + at[2])

    def number(d_core, d):
        n = ((core + d_core) & 1) * 64
        for a in range(3):
            n = n + (((here[a] + d[a]) & 3) if a in d else here[a]) * weight[a]
        return n

    def part(p):
        return pl.ds(cols[p][0], cols[p][1])

    def send(src, dst, send_sem, recv_sem, to):
        pltpu.make_async_remote_copy(src, dst, send_sem, recv_sem, device_id=to, device_id_type=MESH).start()

    def wait_for(ref, sem):
        pltpu.make_async_copy(ref, ref, sem).wait()

    load_in = pltpu.make_async_copy(w_in_hbm, w_in, w_sem.at[0])
    load_out = pltpu.make_async_copy(w_out_hbm, w_out, w_sem.at[1])

    near = [device(0, {a: step}) for a in range(3) for step in (1, 3)] + [device(1, {})]
    barrier = pltpu.get_barrier_semaphore()
    for to in near:
        pl.semaphore_signal(barrier, inc=1, device_id=to, device_id_type=MESH)
    load_in.start()
    load_out.start()
    info[:top] = ids_ref[...].astype(F32)
    info[top:] = gates_ref[...]
    pl.semaphore_wait(barrier, len(near))

    for p in range(3):
        for step in (1, 3):
            to = device(0, {AXES[p][0]: step})
            send(info, info_all.at[p, step], info_send_a.at[p], info_recv.at[p, step], to)
            send(tokens_ref.at[:, part(p)], toks[p].at[0, step], tok_send_a.at[p], tok_recv.at[p, step], to)

    ids = pl.ds(0, top)

    def gather_on(p, a, src, ids_src):
        for step in (1, 3):
            to = device(0, {AXES[p][1]: step})
            send(ids_src, info_all.at[p, 4 * step + a, ids], info_send_b.at[p], info_recv.at[p, 4 * step + a], to)
            send(src, toks[p].at[step, a], tok_send_b.at[p], tok_recv.at[p, 4 * step + a], to)

    for p in range(3):
        gather_on(p, 0, tokens_ref.at[:, part(p)], info.at[ids])
    for p in range(3):
        toks[p][0, 0] = tokens_ref[:, part(p)]
        info_all[p, 0] = info[...]

    def arrived(p, b, a):
        what = info_all.at[p, a] if b == 0 else info_all.at[p, 4 * b + a, ids]
        wait_for(what, info_recv.at[p, 4 * b + a])
        wait_for(toks[p].at[b, a], tok_recv.at[p, 4 * b + a])

    half = tok // 2
    for p in range(3):
        t = toks[p]
        for step, rows in ((1, pl.ds(0, half)), (3, pl.ds(half, half))):
            arrived(p, 0, step)
            to = device(0, {AXES[p][0]: step})
            if step == 1:
                send(info_all.at[p, 1], info_all.at[p, 2], info_send_a.at[p], info_recv.at[p, 2], to)
            send(t.at[0, step, rows], t.at[0, 2, rows], tok_send_a.at[p], tok_recv.at[p, 2], to)
            gather_on(p, step, t.at[0, step], info_all.at[p, step, ids])

    for p in range(3):
        arrived(p, 0, 2)
        gather_on(p, 2, toks[p].at[0, 2], info_all.at[p, 2, ids])

    pl.semaphore_signal(line_sem, inc=1, device_id=near[6], device_id_type=MESH)
    pl.semaphore_wait(line_sem, 1)

    later = (iota((tok, tok), 0) < iota((tok, tok), 1)).astype(BF16)

    def where_in(p, d_core, s1, s2, s3):
        at = [None] * 3
        for axis, s in zip(AXES[p], (s1, s2, s3)):
            at[axis] = s
        return (d_core, *at)

    def build(p, b):
        t, blk = toks[p], blks[p]
        d3 = AXES[p][2]
        dest = iota((8, tok), 0)
        expert_id = number(dest >> 2, {d3: dest & 3}).astype(F32)[None]
        mark = jnp.zeros((4, 8, tok), F32)
        for j in range(top):
            mark = jnp.where(info_all[p, pl.ds(4 * b, 4), j:j + 1, :] == expert_id, 1.0, mark)
        mark = mark.reshape(32, tok)
        place = jnp.dot(mark.astype(BF16), later, preferred_element_type=F32)
        places[...] = jnp.where(mark > 0, place, -1.0)
        if p == 0:
            wide = [jnp.zeros((32, tok), F32)] * 4
            wide[b] = mark
            wide = jnp.concatenate(wide, axis=0).astype(BF16)
            cnt_out[b] = lax.dot_general(jnp.ones((8, tok), BF16), wide, (((1,), (1,)), ((), ())), preferred_element_type=F32)
            cnt_in[0, b] = cnt_out[b]

            @pl.loop(1, 8)
            def _(d):
                send(cnt_out.at[b], cnt_in.at[d, b], cnt_send, cnt_recv, device(lax.div(d, 4), {d3: lax.rem(d, 4)}))

        @pl.loop(0, 4)
        def _(a):
            place = places[pl.ds(a * 8, 8), :]
            pick = place[:, None, :] == iota((8, slots, tok), 1).astype(F32)
            pick = jnp.where(pick, 1.0, 0.0).reshape(8 * slots, tok).astype(BF16)
            rows = jnp.dot(pick, t[b, a], preferred_element_type=F32).astype(BF16).reshape(8, slots, cols[p][1])
            blk[b, :, a] = rows
            recv[where_in(p, 0, a, b, 0) + (slice(None), part(p))] = rows[0]

        for h in range(2):
            @pl.loop(1, 8)
            def _(d):
                d_core, s3 = lax.div(d, 4), lax.rem(d, 4)
                high = {AXES[p][0]: h, AXES[p][1]: b // 2, AXES[p][2]: lax.div(s3, 2)}
                cube = high[Z] * 4 + high[Y] * 2 + high[X]
                send(blk.at[b, d, pl.ds(2 * h, 2)],
                     recv.at[where_in(p, d_core, pl.ds(2 * h, 2), b, s3) + (slice(None), part(p))],
                     blk_send.at[p], blk_recv.at[p, cube], device(d_core, {AXES[p][2]: s3}))

    def relay(p, step, a):
        t, to = toks[p], device(0, {AXES[p][1]: step})
        arrived(p, step, a)
        send(info_all.at[p, 4 * step + a, ids], info_all.at[p, 8 + a, ids], info_send_b.at[p], info_recv.at[p, 8 + a], to)
        send(t.at[step, a], t.at[2, a], tok_send_b.at[p], tok_recv.at[p, 8 + a], to)

    for p in range(3):
        relay(p, 1, 0)
    for p in range(3):
        build(p, 0)

    for p, step, a in [(p, step, a) for step, a in ((3, 1), (3, 3), (1, 2)) for p in range(3)]:
        relay(p, step, a)

    for step, rest in ((1, (1, 3)), (3, (0, 2))):
        for p in range(3):
            for a in rest:
                arrived(p, step, a)
            build(p, step)

    load_in.wait()
    load_out.wait()

    def halves(j):
        return (lax.div(j, 4), lax.rem(lax.div(j, 2), 2), lax.rem(j, 2))

    def wait_blocks(p, h3, refs, sem):
        @pl.when(h3 == 0)
        def _():
            wait_for(refs.at[0, pl.ds(0, 3)], sem)

        @pl.when(h3 == 1)
        def _():
            wait_for(refs.at[0, pl.ds(0, 4)], sem)

    def expert(j):
        high = halves(j)
        pair = [pl.ds(2 * h, 2) for h in high]
        for p in range(3):
            wait_blocks(p, high[AXES[p][2]], blks[p], blk_recv.at[p, j])
        cube = (slice(None), *pair)
        x = recv[cube].reshape(16 * slots, width)
        hidden = jax.nn.gelu(jnp.dot(x, w_in[...], preferred_element_type=F32)).astype(BF16)
        o = jnp.dot(hidden, w_out[...], preferred_element_type=F32).astype(BF16)
        recv[cube] = o.reshape(2, 2, 2, 2, slots, width)

    def drop(j):
        high = halves(j)
        cube = (slice(None), *[pl.ds(2 * h, 2) for h in high])
        rows = 16 * slots
        r = iota((rows, N), 0)
        i = r // slots
        taker = number((i >> 3) & 1, {Z: 4 - (2 * high[Z] + ((i >> 2) & 1)), Y: 4 - (2 * high[Y] + ((i >> 1) & 1)), X: 4 - (2 * high[X] + (i & 1))})
        c = iota((rows, N), 1)
        d1, d2, d3 = AXES[0]
        source = number((c >> 2) & 1, {d1: 4 - ((c >> 3) & 3), d2: 4 - (c >> 5), d3: 4 - (c & 3)})
        before = jnp.sum(jnp.where(source < taker, cnt_row[...], 0.0), axis=1, keepdims=True)
        keep = before + (iota((rows, 1), 0) % slots).astype(F32) < float(cap)
        o = recv[cube].reshape(rows, width)
        recv[cube] = jnp.where(keep, o, jnp.zeros_like(o)).reshape(2, 2, 2, 2, slots, width)

    def hand_out(j):
        high = halves(j)
        pair = [pl.ds(2 * h, 2) for h in high]
        for p in range(3):
            d3 = AXES[p][2]
            rest = [pair[a] for a in range(3) if a != d3]

            def along(s3):
                return tuple(s3 if a == d3 else pair[a] for a in range(3))

            @pl.when(high[d3] == 0)
            def _():
                mids[p][(*rest, 0)] = recv[(0, *along(0), slice(None), part(p))]

            @pl.loop(jnp.where(high[d3] == 0, 1, 0), 4)
            def _(i):
                d_core, s3 = lax.div(i, 2), 2 * high[d3] + lax.rem(i, 2)
                send(recv.at[(d_core, *along(s3), slice(None), part(p))], mids[p].at[(*rest, d_core * 4 + s3)],
                     mid_send.at[p], mid_recv.at[p, j], device(d_core, {d3: 4 - s3}))

    def middle(p, s1, s2):
        d1, d2 = AXES[p][:2]
        return (s1, s2) if d1 < d2 else (s2, s1)

    def second(p, s1, s2, sem):
        send(mids[p].at[middle(p, s1, s2)], ends[p].at[s1, s2], end_send.at[p], end_recv.at[p, sem], device(0, {AXES[p][1]: 4 - s2}))

    def pass_on(j):
        high = halves(j)
        for p in range(3):
            d1, d2, d3 = AXES[p]

            @pl.when(high[d3] == 0)
            def _():
                wait_blocks(p, 1, blks[p], mid_recv.at[p, j + (4, 2, 1)[d3]])
                wait_blocks(p, 0, blks[p], mid_recv.at[p, j])
                first = pl.ds(2 * high[d1], 2)

                @pl.when(high[d2] == 0)
                def _():
                    ends[p][first, 0] = mids[p][middle(p, first, 0)]

                @pl.loop(jnp.where(high[d2] == 0, 1, 2 * high[d2]), 2 * high[d2] + 2)
                def _(s2):
                    @pl.when(high[d1] == 1)
                    def _():
                        second(p, pl.ds(2, 2), s2, 2)

                    @pl.when(high[d1] == 0)
                    def _():
                        second(p, pl.ds(1, 1), s2, 1)

    def weigh(p):
        d1, d2, d3 = AXES[p]
        e = iota((32, tok), 0)
        expert_id = number((e >> 2) & 1, {d2: e >> 3, d3: e & 3}).astype(F32)

        @pl.loop(0, 4)
        def _(s1):
            ids, gts = info_all[p, s1, :top], info_all[p, s1, top:]
            mark = jnp.zeros((32, tok), F32)
            gate = jnp.zeros((32, tok), F32)
            for j in range(top):
                hit = ids[j:j + 1, :] == expert_id
                mark = jnp.where(hit, 1.0, mark)
                gate = jnp.where(hit, gts[j:j + 1, :], gate)
            place = jnp.dot(mark.astype(BF16), later, preferred_element_type=F32)
            place = jnp.where(mark > 0, place, -1.0)
            scale = jnp.where(place[:, None, :] == iota((32, slots, tok), 1).astype(F32), gate[:, None, :], 0.0)
            scale = scale.reshape(32 * slots, tok).T
            high = scale.astype(BF16)
            left = scale - high.astype(F32)
            mid = left.astype(BF16)
            low = (left - mid.astype(F32)).astype(BF16)
            scales[4 * p + s1] = jnp.concatenate([high, mid, low], axis=0)

    def combine(p, s1):
        rows = ends[p][s1].reshape(32 * slots, cols[p][1])
        mixed = jnp.dot(scales[4 * p + s1], rows, preferred_element_type=F32)
        mixed = mixed[:tok] + (mixed[tok:2 * tok] + mixed[2 * tok:])
        if s1 == 0:
            acc[:, part(p)] = tokens_ref[:, part(p)].astype(F32) + mixed
        else:
            sums[p][s1 - 1] = mixed
            send(sums[p].at[s1 - 1], gots[p].at[s1 - 1], sum_send.at[p], sum_recv.at[p, s1 - 1], device(0, {AXES[p][0]: 4 - s1}))

    pl.loop(0, 1)(expert)

    for p in range(3):
        for a in range(4):
            arrived(p, 2, a)
        build(p, 2)

    wait_for(cnt_in.at[pl.ds(1, 7)], cnt_recv)
    row = jnp.zeros((1, N), F32)
    for d in range(8):
        both = sum(cnt_in[d, b][:1] for b in range(4))
        row = row + jnp.where(iota((1, N), 1) % 8 == d, both, 0.0)
    cnt_row[...] = row
    pl.loop(0, 1)(drop)
    pl.loop(0, 1)(hand_out)

    @pl.loop(0, 7)
    def _(i):
        expert(7 - i)
        drop(7 - i)
        hand_out(7 - i)

        @pl.when(i > 2)
        def _():
            pass_on(10 - i)

    @pl.loop(0, 4)
    def _(i):
        pass_on(3 - i)

    for s2 in (1, 3, 2):
        for p in range(3):
            second(p, pl.ds(0, 1), s2, 0)

    for p in range(3):
        weigh(p)
    for p in range(3):
        wait_for(ends[p].at[pl.ds(2, 2), pl.ds(1, 3)], end_recv.at[p, 2])
        combine(p, 2)
        combine(p, 3)
    for p in range(3):
        wait_for(ends[p].at[pl.ds(1, 1), pl.ds(1, 3)], end_recv.at[p, 1])
        combine(p, 1)
    for p in range(3):
        wait_for(ends[p].at[pl.ds(0, 1), pl.ds(1, 3)], end_recv.at[p, 0])
        combine(p, 0)

    for p in range(3):
        total = acc[:, part(p)]
        for i in range(3):
            wait_for(gots[p].at[i], sum_recv.at[p, i])
            total = total + gots[p][i]
        out_ref[:, part(p)] = total.astype(BF16)

    wait_for(cnt_in.at[pl.ds(1, 7)], cnt_send)
    for p in range(3):
        wait_for(info_all.at[p, pl.ds(0, 3)], info_send_a.at[p])
        wait_for(info_all.at[p, pl.ds(0, 12), ids], info_send_b.at[p])
        wait_for(toks[p].at[0, pl.ds(0, 3)], tok_send_a.at[p])
        wait_for(toks[p].at[pl.ds(0, 3)], tok_send_b.at[p])
        wait_for(blks[p].at[:, pl.ds(1, 7)], blk_send.at[p])
        wait_for(mids[p].at[:, :, pl.ds(1, 7)], mid_send.at[p])
        wait_for(ends[p].at[:, pl.ds(1, 3)], end_send.at[p])
        wait_for(sums[p], sum_send.at[p])


def solution(mesh):
    def device_fn(tokens, expert_ids, gate_weights, w_in, w_out):
        tok, width = tokens.shape
        top = expert_ids.shape[1]
        ff = w_in.shape[2]
        cap = tok * top
        slots = 2 * tok * top // N
        tiles = width // 128
        sizes = [128 * (tiles // 3 + (1 if p < tiles % 3 else 0)) for p in range(3)]
        cols = [(sum(sizes[:p]), sizes[p]) for p in range(3)]
        vmem = pl.BlockSpec(memory_space=pltpu.VMEM)
        anyspace = pl.BlockSpec(memory_space=pl.ANY)
        dma = pltpu.SemaphoreType.DMA
        return pl.pallas_call(
            functools.partial(kernel, cols, cap, slots),
            out_shape=jax.ShapeDtypeStruct((tok, width), BF16),
            in_specs=[vmem, vmem, vmem, anyspace, anyspace],
            out_specs=vmem,
            scratch_shapes=[
                pltpu.VMEM((width, ff), BF16),
                pltpu.VMEM((ff, width), BF16),
                *[pltpu.VMEM((4, 4, tok, s), BF16) for s in sizes],
                *[pltpu.VMEM((4, 8, 4, slots, s), BF16) for s in sizes],
                pltpu.VMEM((2, 4, 4, 4, slots, width), BF16),
                *[pltpu.VMEM((4, 4, 8, slots, s), BF16) for s in sizes],
                *[pltpu.VMEM((4, 4, 8, slots, s), BF16) for s in sizes],
                *[pltpu.VMEM((3, tok, s), F32) for s in sizes],
                *[pltpu.VMEM((3, tok, s), F32) for s in sizes],
                pltpu.VMEM((2 * top, tok), F32),
                pltpu.VMEM((3, 16, 2 * top, tok), F32),
                pltpu.VMEM((32, tok), F32),
                pltpu.VMEM((12, 3 * tok, 32 * slots), BF16),
                pltpu.VMEM((4, 8, N), F32),
                pltpu.VMEM((8, 4, 8, N), F32),
                pltpu.VMEM((1, N), F32),
                pltpu.VMEM((tok, width), F32),
                dma((2,)), dma((3,)), dma((3,)), dma((3, 16)), dma, dma, pltpu.SemaphoreType.REGULAR, dma((3,)), dma((3,)), dma((3, 16)),
                dma((3,)), dma((3, 8)), dma((3,)), dma((3, 8)), dma((3,)), dma((3, 3)), dma((3,)), dma((3, 3)),
            ],
            compiler_params=pltpu.CompilerParams(collective_id=0, has_side_effects=True, vmem_limit_bytes=67043328),
            name='expert_layer',
        )(tokens, expert_ids.T, gate_weights.T, w_in.reshape(width, ff), w_out.reshape(ff, width))

    token_spec = P(('data', 'row', 'col'), None)
    expert_spec = P(GRID_AXES, None, None)
    return jax.shard_map(device_fn, mesh=mesh, in_specs=(token_spec, token_spec, token_spec, expert_spec, expert_spec), out_specs=token_spec, check_vma=False)
```

```python
import functools

import jax
import jax.numpy as jnp
from jax import lax
from jax.experimental import pallas as pl
from jax.experimental.pallas import tpu as pltpu
from jax.sharding import PartitionSpec as P

GRID_AXES = ('row', 'col')
F32 = jnp.float32
BF16 = jnp.bfloat16
I32 = jnp.int32
SIDE = 4
N = 2 * SIDE ** 3
MESH = pl.DeviceIdType.MESH
Z, Y, X = 0, 1, 2
AXES = ((Z, Y, X), (Y, X, Z), (X, Z, Y))


def iota(shape, dim):
    return lax.broadcasted_iota(I32, shape, dim)


def kernel(cols, cap, slots, tokens_ref, ids_ref, gates_ref, w_in_hbm, w_out_hbm, out_ref,
           w_in, w_out, tok0, tok1, tok2, blk0, blk1, blk2, recv, mid0, mid1, mid2, end0, end1, end2,
           sum0, sum1, sum2, got0, got1, got2, info, info_all, places, scales, cnt_out, cnt_in, cnt_row, acc,
           w_sem, info_send_a, info_send_b, info_recv, cnt_send, cnt_recv, line_sem, tok_send_a, tok_send_b, tok_recv,
           blk_send, blk_recv, mid_send, mid_recv, end_send, end_recv, sum_send, sum_recv):
    toks, blks = (tok0, tok1, tok2), (blk0, blk1, blk2)
    mids, ends = (mid0, mid1, mid2), (end0, end1, end2)
    sums, gots = (sum0, sum1, sum2), (got0, got1, got2)
    tok, width = tokens_ref.shape
    top = ids_ref.shape[0]
    data = lax.axis_index('data')
    core = lax.axis_index('row')
    col = lax.axis_index('col')
    here = (lax.div(col, 16), lax.rem(lax.div(col, 4), 4), lax.rem(col, 4))
    me = core * 64 + col
    weight = (16, 4, 1)

    def device(d_core, d):
        at = [lax.rem(here[a] + d[a], 4) if a in d else here[a] for a in range(3)]
        return (data, lax.rem(core + d_core, 2), at[0] * 16 + at[1] * 4 + at[2])

    def number(d_core, d):
        n = ((core + d_core) & 1) * 64
        for a in range(3):
            n = n + (((here[a] + d[a]) & 3) if a in d else here[a]) * weight[a]
        return n

    def part(p):
        return pl.ds(cols[p][0], cols[p][1])

    def send(src, dst, send_sem, recv_sem, to):
        pltpu.make_async_remote_copy(src, dst, send_sem, recv_sem, device_id=to, device_id_type=MESH).start()

    def wait_for(ref, sem):
        pltpu.make_async_copy(ref, ref, sem).wait()

    load_in = pltpu.make_async_copy(w_in_hbm, w_in, w_sem.at[0])
    load_out = pltpu.make_async_copy(w_out_hbm, w_out, w_sem.at[1])

    near = [device(0, {a: step}) for a in range(3) for step in (1, 3)] + [device(1, {})]
    barrier = pltpu.get_barrier_semaphore()
    for to in near:
        pl.semaphore_signal(barrier, inc=1, device_id=to, device_id_type=MESH)
    load_in.start()
    load_out.start()
    info[:top] = ids_ref[...].astype(F32)
    info[top:] = gates_ref[...]
    pl.semaphore_wait(barrier, len(near))

    for p in range(3):
        for step in (1, 3):
            to = device(0, {AXES[p][0]: step})
            send(info, info_all.at[p, step], info_send_a.at[p], info_recv.at[p, step], to)
            send(tokens_ref.at[:, part(p)], toks[p].at[0, step], tok_send_a.at[p], tok_recv.at[p, step], to)

    ids = pl.ds(0, top)

    def gather_on(p, a, src, ids_src):
        for step in (1, 3):
            to = device(0, {AXES[p][1]: step})
            send(ids_src, info_all.at[p, 4 * step + a, ids], info_send_b.at[p], info_recv.at[p, 4 * step + a], to)
            send(src, toks[p].at[step, a], tok_send_b.at[p], tok_recv.at[p, 4 * step + a], to)

    for p in range(3):
        gather_on(p, 0, tokens_ref.at[:, part(p)], info.at[ids])
    for p in range(3):
        toks[p][0, 0] = tokens_ref[:, part(p)]
        info_all[p, 0] = info[...]

    def arrived(p, b, a):
        what = info_all.at[p, a] if b == 0 else info_all.at[p, 4 * b + a, ids]
        wait_for(what, info_recv.at[p, 4 * b + a])
        wait_for(toks[p].at[b, a], tok_recv.at[p, 4 * b + a])

    half = tok // 2
    for p in range(3):
        t = toks[p]
        for step, rows in ((1, pl.ds(0, half)), (3, pl.ds(half, half))):
            arrived(p, 0, step)
            to = device(0, {AXES[p][0]: step})
            if step == 1:
                send(info_all.at[p, 1], info_all.at[p, 2], info_send_a.at[p], info_recv.at[p, 2], to)
            send(t.at[0, step, rows], t.at[0, 2, rows], tok_send_a.at[p], tok_recv.at[p, 2], to)
            gather_on(p, step, t.at[0, step], info_all.at[p, step, ids])

    for p in range(3):
        arrived(p, 0, 2)
        gather_on(p, 2, toks[p].at[0, 2], info_all.at[p, 2, ids])

    pl.semaphore_signal(line_sem, inc=1, device_id=near[6], device_id_type=MESH)
    pl.semaphore_wait(line_sem, 1)

    later = (iota((tok, tok), 0) < iota((tok, tok), 1)).astype(BF16)

    def where_in(p, d_core, s1, s2, s3):
        at = [None] * 3
        for axis, s in zip(AXES[p], (s1, s2, s3)):
            at[axis] = s
        return (d_core, *at)

    def build(p, b):
        t, blk = toks[p], blks[p]
        d3 = AXES[p][2]
        dest = iota((8, tok), 0)
        expert_id = number(dest >> 2, {d3: dest & 3}).astype(F32)[None]
        mark = jnp.zeros((4, 8, tok), F32)
        for j in range(top):
            mark = jnp.where(info_all[p, pl.ds(4 * b, 4), j:j + 1, :] == expert_id, 1.0, mark)
        mark = mark.reshape(32, tok)
        place = jnp.dot(mark.astype(BF16), later, preferred_element_type=F32)
        places[...] = jnp.where(mark > 0, place, -1.0)
        if p == 0:
            wide = [jnp.zeros((32, tok), F32)] * 4
            wide[b] = mark
            wide = jnp.concatenate(wide, axis=0).astype(BF16)
            cnt_out[b] = lax.dot_general(jnp.ones((8, tok), BF16), wide, (((1,), (1,)), ((), ())), preferred_element_type=F32)
            cnt_in[0, b] = cnt_out[b]

            @pl.loop(1, 8)
            def _(d):
                send(cnt_out.at[b], cnt_in.at[d, b], cnt_send, cnt_recv, device(lax.div(d, 4), {d3: lax.rem(d, 4)}))

        @pl.loop(0, 4)
        def _(a):
            place = places[pl.ds(a * 8, 8), :]
            pick = place[:, None, :] == iota((8, slots, tok), 1).astype(F32)
            pick = jnp.where(pick, 1.0, 0.0).reshape(8 * slots, tok).astype(BF16)
            rows = jnp.dot(pick, t[b, a], preferred_element_type=F32).astype(BF16).reshape(8, slots, cols[p][1])
            blk[b, :, a] = rows
            recv[where_in(p, 0, a, b, 0) + (slice(None), part(p))] = rows[0]

        for h in range(2):
            @pl.loop(1, 8)
            def _(d):
                d_core, s3 = lax.div(d, 4), lax.rem(d, 4)
                high = {AXES[p][0]: h, AXES[p][1]: b // 2, AXES[p][2]: lax.div(s3, 2)}
                cube = high[Z] * 4 + high[Y] * 2 + high[X]
                send(blk.at[b, d, pl.ds(2 * h, 2)],
                     recv.at[where_in(p, d_core, pl.ds(2 * h, 2), b, s3) + (slice(None), part(p))],
                     blk_send.at[p], blk_recv.at[p, cube], device(d_core, {AXES[p][2]: s3}))

    def relay(p, step, a):
        t, to = toks[p], device(0, {AXES[p][1]: step})
        arrived(p, step, a)
        send(info_all.at[p, 4 * step + a, ids], info_all.at[p, 8 + a, ids], info_send_b.at[p], info_recv.at[p, 8 + a], to)
        send(t.at[step, a], t.at[2, a], tok_send_b.at[p], tok_recv.at[p, 8 + a], to)

    for p in range(3):
        relay(p, 1, 0)
    for p in range(3):
        build(p, 0)

    for p, step, a in [(p, step, a) for step, a in ((3, 1), (3, 3), (1, 2)) for p in range(3)]:
        relay(p, step, a)

    for step, rest in ((1, (1, 3)), (3, (0, 2))):
        for p in range(3):
            for a in rest:
                arrived(p, step, a)
            build(p, step)

    def halves(j):
        return (lax.div(j, 4), lax.rem(lax.div(j, 2), 2), lax.rem(j, 2))

    def wait_blocks(p, h3, refs, sem):
        @pl.when(h3 == 0)
        def _():
            wait_for(refs.at[0, pl.ds(0, 3)], sem)

        @pl.when(h3 == 1)
        def _():
            wait_for(refs.at[0, pl.ds(0, 4)], sem)

    def expert(j):
        high = halves(j)
        pair = [pl.ds(2 * h, 2) for h in high]
        for p in range(3):
            wait_blocks(p, high[AXES[p][2]], blks[p], blk_recv.at[p, j])
        cube = (slice(None), *pair)
        x = recv[cube].reshape(16 * slots, width)
        hidden = jax.nn.gelu(jnp.dot(x, w_in[...], preferred_element_type=F32)).astype(BF16)
        o = jnp.dot(hidden, w_out[...], preferred_element_type=F32).astype(BF16)
        recv[cube] = o.reshape(2, 2, 2, 2, slots, width)

    def drop(j):
        high = halves(j)
        cube = (slice(None), *[pl.ds(2 * h, 2) for h in high])
        rows = 16 * slots
        r = iota((rows, N), 0)
        i = r // slots
        taker = number((i >> 3) & 1, {Z: 4 - (2 * high[Z] + ((i >> 2) & 1)), Y: 4 - (2 * high[Y] + ((i >> 1) & 1)), X: 4 - (2 * high[X] + (i & 1))})
        c = iota((rows, N), 1)
        d1, d2, d3 = AXES[0]
        source = number((c >> 2) & 1, {d1: 4 - ((c >> 3) & 3), d2: 4 - (c >> 5), d3: 4 - (c & 3)})
        before = jnp.sum(jnp.where(source < taker, cnt_row[...], 0.0), axis=1, keepdims=True)
        keep = before + (iota((rows, 1), 0) % slots).astype(F32) < float(cap)
        o = recv[cube].reshape(rows, width)
        recv[cube] = jnp.where(keep, o, jnp.zeros_like(o)).reshape(2, 2, 2, 2, slots, width)

    def hand_out(j):
        high = halves(j)
        pair = [pl.ds(2 * h, 2) for h in high]
        for p in range(3):
            d3 = AXES[p][2]
            rest = [pair[a] for a in range(3) if a != d3]

            def along(s3):
                return tuple(s3 if a == d3 else pair[a] for a in range(3))

            @pl.when(high[d3] == 0)
            def _():
                mids[p][(*rest, 0)] = recv[(0, *along(0), slice(None), part(p))]

            @pl.loop(jnp.where(high[d3] == 0, 1, 0), 4)
            def _(i):
                d_core, s3 = lax.div(i, 2), 2 * high[d3] + lax.rem(i, 2)
                send(recv.at[(d_core, *along(s3), slice(None), part(p))], mids[p].at[(*rest, d_core * 4 + s3)],
                     mid_send.at[p], mid_recv.at[p, j], device(d_core, {d3: 4 - s3}))

    def middle(p, s1, s2):
        d1, d2 = AXES[p][:2]
        return (s1, s2) if d1 < d2 else (s2, s1)

    def second(p, s1, s2, sem):
        send(mids[p].at[middle(p, s1, s2)], ends[p].at[s1, s2], end_send.at[p], end_recv.at[p, sem], device(0, {AXES[p][1]: 4 - s2}))

    def pass_on(j):
        high = halves(j)
        for p in range(3):
            d1, d2, d3 = AXES[p]

            @pl.when(high[d3] == 0)
            def _():
                wait_blocks(p, 1, blks[p], mid_recv.at[p, j + (4, 2, 1)[d3]])
                wait_blocks(p, 0, blks[p], mid_recv.at[p, j])
                first = pl.ds(2 * high[d1], 2)

                @pl.when(high[d2] == 0)
                def _():
                    ends[p][first, 0] = mids[p][middle(p, first, 0)]

                @pl.loop(jnp.where(high[d2] == 0, 1, 2 * high[d2]), 2 * high[d2] + 2)
                def _(s2):
                    @pl.when(high[d1] == 1)
                    def _():
                        second(p, pl.ds(2, 2), s2, 2)

                    @pl.when(high[d1] == 0)
                    def _():
                        second(p, pl.ds(1, 1), s2, 1)

    def weigh(p):
        d1, d2, d3 = AXES[p]
        e = iota((32, tok), 0)
        expert_id = number((e >> 2) & 1, {d2: e >> 3, d3: e & 3}).astype(F32)

        @pl.loop(0, 4)
        def _(s1):
            ids, gts = info_all[p, s1, :top], info_all[p, s1, top:]
            mark = jnp.zeros((32, tok), F32)
            gate = jnp.zeros((32, tok), F32)
            for j in range(top):
                hit = ids[j:j + 1, :] == expert_id
                mark = jnp.where(hit, 1.0, mark)
                gate = jnp.where(hit, gts[j:j + 1, :], gate)
            place = jnp.dot(mark.astype(BF16), later, preferred_element_type=F32)
            place = jnp.where(mark > 0, place, -1.0)
            scale = jnp.where(place[:, None, :] == iota((32, slots, tok), 1).astype(F32), gate[:, None, :], 0.0)
            scale = scale.reshape(32 * slots, tok).T
            high = scale.astype(BF16)
            left = scale - high.astype(F32)
            mid = left.astype(BF16)
            low = (left - mid.astype(F32)).astype(BF16)
            scales[4 * p + s1] = jnp.concatenate([high, mid, low], axis=0)

    def combine(p, s1):
        rows = ends[p][s1].reshape(32 * slots, cols[p][1])
        mixed = jnp.dot(scales[4 * p + s1], rows, preferred_element_type=F32)
        mixed = mixed[:tok] + (mixed[tok:2 * tok] + mixed[2 * tok:])
        if s1 == 0:
            acc[:, part(p)] = tokens_ref[:, part(p)].astype(F32) + mixed
        else:
            sums[p][s1 - 1] = mixed
            send(sums[p].at[s1 - 1], gots[p].at[s1 - 1], sum_send.at[p], sum_recv.at[p, s1 - 1], device(0, {AXES[p][0]: 4 - s1}))

    for p in range(3):
        for a in range(4):
            arrived(p, 2, a)
        build(p, 2)

    load_in.wait()
    load_out.wait()
    pl.loop(0, 1)(expert)

    wait_for(cnt_in.at[pl.ds(1, 7)], cnt_recv)
    row = jnp.zeros((1, N), F32)
    for d in range(8):
        both = sum(cnt_in[d, b][:1] for b in range(4))
        row = row + jnp.where(iota((1, N), 1) % 8 == d, both, 0.0)
    cnt_row[...] = row
    pl.loop(0, 1)(drop)
    pl.loop(0, 1)(hand_out)

    @pl.loop(0, 7)
    def _(i):
        expert(7 - i)
        drop(7 - i)
        hand_out(7 - i)

        @pl.when(i > 2)
        def _():
            pass_on(10 - i)

    @pl.loop(0, 4)
    def _(i):
        pass_on(3 - i)

    for s2 in (1, 3, 2):
        for p in range(3):
            second(p, pl.ds(0, 1), s2, 0)

    for p in range(3):
        weigh(p)
    for p in range(3):
        wait_for(ends[p].at[pl.ds(2, 2), pl.ds(1, 3)], end_recv.at[p, 2])
        combine(p, 2)
        combine(p, 3)
    for p in range(3):
        wait_for(ends[p].at[pl.ds(1, 1), pl.ds(1, 3)], end_recv.at[p, 1])
        combine(p, 1)
    for p in range(3):
        wait_for(ends[p].at[pl.ds(0, 1), pl.ds(1, 3)], end_recv.at[p, 0])
        combine(p, 0)

    for p in range(3):
        total = acc[:, part(p)]
        for i in range(3):
            wait_for(gots[p].at[i], sum_recv.at[p, i])
            total = total + gots[p][i]
        out_ref[:, part(p)] = total.astype(BF16)

    wait_for(cnt_in.at[pl.ds(1, 7)], cnt_send)
    for p in range(3):
        wait_for(info_all.at[p, pl.ds(0, 3)], info_send_a.at[p])
        wait_for(info_all.at[p, pl.ds(0, 12), ids], info_send_b.at[p])
        wait_for(toks[p].at[0, pl.ds(0, 3)], tok_send_a.at[p])
        wait_for(toks[p].at[pl.ds(0, 3)], tok_send_b.at[p])
        wait_for(blks[p].at[:, pl.ds(1, 7)], blk_send.at[p])
        wait_for(mids[p].at[:, :, pl.ds(1, 7)], mid_send.at[p])
        wait_for(ends[p].at[:, pl.ds(1, 3)], end_send.at[p])
        wait_for(sums[p], sum_send.at[p])


def solution(mesh):
    def device_fn(tokens, expert_ids, gate_weights, w_in, w_out):
        tok, width = tokens.shape
        top = expert_ids.shape[1]
        ff = w_in.shape[2]
        cap = tok * top
        slots = 2 * tok * top // N
        tiles = width // 128
        sizes = [128 * (tiles // 3 + (1 if p < tiles % 3 else 0)) for p in range(3)]
        cols = [(sum(sizes[:p]), sizes[p]) for p in range(3)]
        vmem = pl.BlockSpec(memory_space=pltpu.VMEM)
        anyspace = pl.BlockSpec(memory_space=pl.ANY)
        dma = pltpu.SemaphoreType.DMA
        return pl.pallas_call(
            functools.partial(kernel, cols, cap, slots),
            out_shape=jax.ShapeDtypeStruct((tok, width), BF16),
            in_specs=[vmem, vmem, vmem, anyspace, anyspace],
            out_specs=vmem,
            scratch_shapes=[
                pltpu.VMEM((width, ff), BF16),
                pltpu.VMEM((ff, width), BF16),
                *[pltpu.VMEM((4, 4, tok, s), BF16) for s in sizes],
                *[pltpu.VMEM((4, 8, 4, slots, s), BF16) for s in sizes],
                pltpu.VMEM((2, 4, 4, 4, slots, width), BF16),
                *[pltpu.VMEM((4, 4, 8, slots, s), BF16) for s in sizes],
                *[pltpu.VMEM((4, 4, 8, slots, s), BF16) for s in sizes],
                *[pltpu.VMEM((3, tok, s), F32) for s in sizes],
                *[pltpu.VMEM((3, tok, s), F32) for s in sizes],
                pltpu.VMEM((2 * top, tok), F32),
                pltpu.VMEM((3, 16, 2 * top, tok), F32),
                pltpu.VMEM((32, tok), F32),
                pltpu.VMEM((12, 3 * tok, 32 * slots), BF16),
                pltpu.VMEM((4, 8, N), F32),
                pltpu.VMEM((8, 4, 8, N), F32),
                pltpu.VMEM((1, N), F32),
                pltpu.VMEM((tok, width), F32),
                dma((2,)), dma((3,)), dma((3,)), dma((3, 16)), dma, dma, pltpu.SemaphoreType.REGULAR, dma((3,)), dma((3,)), dma((3, 16)),
                dma((3,)), dma((3, 8)), dma((3,)), dma((3, 8)), dma((3,)), dma((3, 3)), dma((3,)), dma((3, 3)),
            ],
            compiler_params=pltpu.CompilerParams(collective_id=0, has_side_effects=True, vmem_limit_bytes=67043328),
            name='expert_layer',
        )(tokens, expert_ids.T, gate_weights.T, w_in.reshape(width, ff), w_out.reshape(ff, width))

    token_spec = P(('data', 'row', 'col'), None)
    expert_spec = P(GRID_AXES, None, None)
    return jax.shard_map(device_fn, mesh=mesh, in_specs=(token_spec, token_spec, token_spec, expert_spec, expert_spec), out_specs=token_spec, check_vma=False)
```

```python
import functools

import jax
import jax.numpy as jnp
from jax import lax
from jax.experimental import pallas as pl
from jax.experimental.pallas import tpu as pltpu
from jax.sharding import PartitionSpec as P

GRID_AXES = ('row', 'col')
F32 = jnp.float32
BF16 = jnp.bfloat16
I32 = jnp.int32
SIDE = 4
N = 2 * SIDE ** 3
MESH = pl.DeviceIdType.MESH
Z, Y, X = 0, 1, 2
AXES = ((Z, Y, X), (Y, X, Z), (X, Z, Y))


def iota(shape, dim):
    return lax.broadcasted_iota(I32, shape, dim)


def kernel(cols, cap, slots, tokens_ref, ids_ref, gates_ref, w_in_hbm, w_out_hbm, out_ref,
           w_in, w_out, tok0, tok1, tok2, blk0, blk1, blk2, recv, mid0, mid1, mid2, end0, end1, end2,
           sum0, sum1, sum2, got0, got1, got2, info, info_all, places, scales, cnt_out, cnt_in, cnt_row, acc,
           w_sem, info_send_a, info_send_b, info_recv, cnt_send, cnt_recv, line_sem, tok_send_a, tok_send_b, tok_recv,
           blk_send, blk_recv, mid_send, mid_recv, end_send, end_recv, sum_send, sum_recv):
    toks, blks = (tok0, tok1, tok2), (blk0, blk1, blk2)
    mids, ends = (mid0, mid1, mid2), (end0, end1, end2)
    sums, gots = (sum0, sum1, sum2), (got0, got1, got2)
    tok, width = tokens_ref.shape
    top = ids_ref.shape[0]
    data = lax.axis_index('data')
    core = lax.axis_index('row')
    col = lax.axis_index('col')
    here = (lax.div(col, 16), lax.rem(lax.div(col, 4), 4), lax.rem(col, 4))
    me = core * 64 + col
    weight = (16, 4, 1)

    def device(d_core, d):
        at = [lax.rem(here[a] + d[a], 4) if a in d else here[a] for a in range(3)]
        return (data, lax.rem(core + d_core, 2), at[0] * 16 + at[1] * 4 + at[2])

    def number(d_core, d):
        n = ((core + d_core) & 1) * 64
        for a in range(3):
            n = n + (((here[a] + d[a]) & 3) if a in d else here[a]) * weight[a]
        return n

    def part(p):
        return pl.ds(cols[p][0], cols[p][1])

    def send(src, dst, send_sem, recv_sem, to):
        pltpu.make_async_remote_copy(src, dst, send_sem, recv_sem, device_id=to, device_id_type=MESH).start()

    def wait_for(ref, sem):
        pltpu.make_async_copy(ref, ref, sem).wait()

    load_in = pltpu.make_async_copy(w_in_hbm, w_in, w_sem.at[0])
    load_out = pltpu.make_async_copy(w_out_hbm, w_out, w_sem.at[1])

    near = [device(0, {a: step}) for a in range(3) for step in (1, 3)] + [device(1, {})]
    barrier = pltpu.get_barrier_semaphore()
    for to in near:
        pl.semaphore_signal(barrier, inc=1, device_id=to, device_id_type=MESH)
    load_in.start()
    load_out.start()
    info[:top] = ids_ref[...].astype(F32)
    info[top:] = gates_ref[...]
    pl.semaphore_wait(barrier, len(near))

    for p in range(3):
        for step in (1, 3):
            to = device(0, {AXES[p][0]: step})
            send(info, info_all.at[p, step], info_send_a.at[p], info_recv.at[p, step], to)
            send(tokens_ref.at[:, part(p)], toks[p].at[0, step], tok_send_a.at[p], tok_recv.at[p, step], to)

    ids = pl.ds(0, top)

    def gather_on(p, a, src, ids_src):
        for step in (1, 3):
            to = device(0, {AXES[p][1]: step})
            send(ids_src, info_all.at[p, 4 * step + a, ids], info_send_b.at[p], info_recv.at[p, 4 * step + a], to)
            send(src, toks[p].at[step, a], tok_send_b.at[p], tok_recv.at[p, 4 * step + a], to)

    for p in range(3):
        gather_on(p, 0, tokens_ref.at[:, part(p)], info.at[ids])
    for p in range(3):
        toks[p][0, 0] = tokens_ref[:, part(p)]
        info_all[p, 0] = info[...]

    def arrived(p, b, a):
        what = info_all.at[p, a] if b == 0 else info_all.at[p, 4 * b + a, ids]
        wait_for(what, info_recv.at[p, 4 * b + a])
        wait_for(toks[p].at[b, a], tok_recv.at[p, 4 * b + a])

    half = tok // 2
    for p in range(3):
        t = toks[p]
        for step, rows in ((1, pl.ds(0, half)), (3, pl.ds(half, half))):
            arrived(p, 0, step)
            to = device(0, {AXES[p][0]: step})
            if step == 1:
                send(info_all.at[p, 1], info_all.at[p, 2], info_send_a.at[p], info_recv.at[p, 2], to)
            send(t.at[0, step, rows], t.at[0, 2, rows], tok_send_a.at[p], tok_recv.at[p, 2], to)
            gather_on(p, step, t.at[0, step], info_all.at[p, step, ids])

    for p in range(3):
        arrived(p, 0, 2)
        gather_on(p, 2, toks[p].at[0, 2], info_all.at[p, 2, ids])

    pl.semaphore_signal(line_sem, inc=1, device_id=near[6], device_id_type=MESH)
    pl.semaphore_wait(line_sem, 1)

    later = (iota((tok, tok), 0) < iota((tok, tok), 1)).astype(BF16)

    def where_in(p, d_core, s1, s2, s3):
        at = [None] * 3
        for axis, s in zip(AXES[p], (s1, s2, s3)):
            at[axis] = s
        return (d_core, *at)

    def build(p, b):
        t, blk = toks[p], blks[p]
        d3 = AXES[p][2]
        dest = iota((8, tok), 0)
        expert_id = number(dest >> 2, {d3: dest & 3}).astype(F32)[None]
        mark = jnp.zeros((4, 8, tok), F32)
        for j in range(top):
            mark = jnp.where(info_all[p, pl.ds(4 * b, 4), j:j + 1, :] == expert_id, 1.0, mark)
        mark = mark.reshape(32, tok)
        place = jnp.dot(mark.astype(BF16), later, preferred_element_type=F32)
        places[...] = jnp.where(mark > 0, place, -1.0)
        if p == 0:
            wide = [jnp.zeros((32, tok), F32)] * 4
            wide[b] = mark
            wide = jnp.concatenate(wide, axis=0).astype(BF16)
            cnt_out[b] = lax.dot_general(jnp.ones((8, tok), BF16), wide, (((1,), (1,)), ((), ())), preferred_element_type=F32)
            cnt_in[0, b] = cnt_out[b]

            @pl.loop(1, 8)
            def _(d):
                send(cnt_out.at[b], cnt_in.at[d, b], cnt_send, cnt_recv, device(lax.div(d, 4), {d3: lax.rem(d, 4)}))

        @pl.loop(0, 4)
        def _(a):
            place = places[pl.ds(a * 8, 8), :]
            pick = place[:, None, :] == iota((8, slots, tok), 1).astype(F32)
            pick = jnp.where(pick, 1.0, 0.0).reshape(8 * slots, tok).astype(BF16)
            rows = jnp.dot(pick, t[b, a], preferred_element_type=F32).astype(BF16).reshape(8, slots, cols[p][1])
            blk[b, :, a] = rows
            recv[where_in(p, 0, a, b, 0) + (slice(None), part(p))] = rows[0]

        for h in range(2):
            @pl.loop(1, 8)
            def _(d):
                d_core, s3 = lax.div(d, 4), lax.rem(d, 4)
                high = {AXES[p][0]: h, AXES[p][1]: b // 2, AXES[p][2]: lax.div(s3, 2)}
                cube = high[Z] * 4 + high[Y] * 2 + high[X]
                send(blk.at[b, d, pl.ds(2 * h, 2)],
                     recv.at[where_in(p, d_core, pl.ds(2 * h, 2), b, s3) + (slice(None), part(p))],
                     blk_send.at[p], blk_recv.at[p, cube], device(d_core, {AXES[p][2]: s3}))

    def relay(p, step, a):
        t, to = toks[p], device(0, {AXES[p][1]: step})
        arrived(p, step, a)
        send(info_all.at[p, 4 * step + a, ids], info_all.at[p, 8 + a, ids], info_send_b.at[p], info_recv.at[p, 8 + a], to)
        send(t.at[step, a], t.at[2, a], tok_send_b.at[p], tok_recv.at[p, 8 + a], to)

    for p in range(3):
        relay(p, 1, 0)
    for p in range(3):
        build(p, 0)

    for p, step, a in [(p, step, a) for step, a in ((3, 1), (3, 3), (1, 2)) for p in range(3)]:
        relay(p, step, a)

    for step, rest in ((1, (1, 3)), (3, (0, 2))):
        for p in range(3):
            for a in rest:
                arrived(p, step, a)
            build(p, step)

    def halves(j):
        return (lax.div(j, 4), lax.rem(lax.div(j, 2), 2), lax.rem(j, 2))

    def wait_blocks(p, h3, refs, sem):
        @pl.when(h3 == 0)
        def _():
            wait_for(refs.at[0, pl.ds(0, 3)], sem)

        @pl.when(h3 == 1)
        def _():
            wait_for(refs.at[0, pl.ds(0, 4)], sem)

    def expert(j):
        high = halves(j)
        pair = [pl.ds(2 * h, 2) for h in high]
        for p in range(3):
            wait_blocks(p, high[AXES[p][2]], blks[p], blk_recv.at[p, j])
        cube = (slice(None), *pair)
        x = recv[cube].reshape(16 * slots, width)
        hidden = jax.nn.gelu(jnp.dot(x, w_in[...], preferred_element_type=F32)).astype(BF16)
        o = jnp.dot(hidden, w_out[...], preferred_element_type=F32).astype(BF16)
        recv[cube] = o.reshape(2, 2, 2, 2, slots, width)

    def drop(j):
        high = halves(j)
        cube = (slice(None), *[pl.ds(2 * h, 2) for h in high])
        rows = 16 * slots
        r = iota((rows, N), 0)
        i = r // slots
        taker = number((i >> 3) & 1, {Z: 4 - (2 * high[Z] + ((i >> 2) & 1)), Y: 4 - (2 * high[Y] + ((i >> 1) & 1)), X: 4 - (2 * high[X] + (i & 1))})
        c = iota((rows, N), 1)
        d1, d2, d3 = AXES[0]
        source = number((c >> 2) & 1, {d1: 4 - ((c >> 3) & 3), d2: 4 - (c >> 5), d3: 4 - (c & 3)})
        before = jnp.sum(jnp.where(source < taker, cnt_row[...], 0.0), axis=1, keepdims=True)
        keep = before + (iota((rows, 1), 0) % slots).astype(F32) < float(cap)
        o = recv[cube].reshape(rows, width)
        recv[cube] = jnp.where(keep, o, jnp.zeros_like(o)).reshape(2, 2, 2, 2, slots, width)

    def hand_out(j):
        high = halves(j)
        pair = [pl.ds(2 * h, 2) for h in high]
        for p in range(3):
            d3 = AXES[p][2]
            rest = [pair[a] for a in range(3) if a != d3]

            def along(s3):
                return tuple(s3 if a == d3 else pair[a] for a in range(3))

            @pl.when(high[d3] == 0)
            def _():
                mids[p][(*rest, 0)] = recv[(0, *along(0), slice(None), part(p))]

            @pl.loop(jnp.where(high[d3] == 0, 1, 0), 4)
            def _(i):
                d_core, s3 = lax.div(i, 2), 2 * high[d3] + lax.rem(i, 2)
                send(recv.at[(d_core, *along(s3), slice(None), part(p))], mids[p].at[(*rest, d_core * 4 + s3)],
                     mid_send.at[p], mid_recv.at[p, j], device(d_core, {d3: 4 - s3}))

    def middle(p, s1, s2):
        d1, d2 = AXES[p][:2]
        return (s1, s2) if d1 < d2 else (s2, s1)

    def second(p, s1, s2, sem):
        send(mids[p].at[middle(p, s1, s2)], ends[p].at[s1, s2], end_send.at[p], end_recv.at[p, sem], device(0, {AXES[p][1]: 4 - s2}))

    def pass_on(j):
        high = halves(j)
        for p in range(3):
            d1, d2, d3 = AXES[p]

            @pl.when(high[d3] == 0)
            def _():
                wait_blocks(p, 1, blks[p], mid_recv.at[p, j + (4, 2, 1)[d3]])
                wait_blocks(p, 0, blks[p], mid_recv.at[p, j])
                first = pl.ds(2 * high[d1], 2)

                @pl.when(high[d2] == 0)
                def _():
                    ends[p][first, 0] = mids[p][middle(p, first, 0)]

                @pl.loop(jnp.where(high[d2] == 0, 1, 2 * high[d2]), 2 * high[d2] + 2)
                def _(s2):
                    @pl.when(high[d1] == 1)
                    def _():
                        second(p, pl.ds(2, 2), s2, 2)

                    @pl.when(high[d1] == 0)
                    def _():
                        second(p, pl.ds(1, 1), s2, 1)

    def weigh(p):
        d1, d2, d3 = AXES[p]
        e = iota((32, tok), 0)
        expert_id = number((e >> 2) & 1, {d2: e >> 3, d3: e & 3}).astype(F32)

        @pl.loop(0, 4)
        def _(s1):
            ids, gts = info_all[p, s1, :top], info_all[p, s1, top:]
            mark = jnp.zeros((32, tok), F32)
            gate = jnp.zeros((32, tok), F32)
            for j in range(top):
                hit = ids[j:j + 1, :] == expert_id
                mark = jnp.where(hit, 1.0, mark)
                gate = jnp.where(hit, gts[j:j + 1, :], gate)
            place = jnp.dot(mark.astype(BF16), later, preferred_element_type=F32)
            place = jnp.where(mark > 0, place, -1.0)
            scale = jnp.where(place[:, None, :] == iota((32, slots, tok), 1).astype(F32), gate[:, None, :], 0.0)
            scale = scale.reshape(32 * slots, tok).T
            high = scale.astype(BF16)
            left = scale - high.astype(F32)
            mid = left.astype(BF16)
            low = (left - mid.astype(F32)).astype(BF16)
            scales[4 * p + s1] = jnp.concatenate([high, mid, low], axis=0)

    def combine(p, s1):
        rows = ends[p][s1].reshape(32 * slots, cols[p][1])
        mixed = jnp.dot(scales[4 * p + s1], rows, preferred_element_type=F32)
        mixed = mixed[:tok] + (mixed[tok:2 * tok] + mixed[2 * tok:])
        d1, low, high = AXES[p][0], pl.ds(0, half), pl.ds(half, half)
        if s1 == 0:
            acc[:, part(p)] = tokens_ref[:, part(p)].astype(F32) + mixed
            return
        sums[p][s1 - 1] = mixed
        if s1 == 2:
            send(sums[p].at[1, low], gots[p].at[1, low], sum_send.at[p], sum_recv.at[p, 1], device(0, {d1: 3}))
            send(sums[p].at[1, high], gots[p].at[1, high], sum_send.at[p], sum_recv.at[p, 3], device(0, {d1: 1}))
            return
        rows, sem = (low, 1) if s1 == 1 else (high, 3)
        wait_for(gots[p].at[1, rows], sum_recv.at[p, sem])
        sums[p][s1 - 1, rows] = sums[p][s1 - 1, rows] + gots[p][1, rows]
        send(sums[p].at[s1 - 1], gots[p].at[s1 - 1], sum_send.at[p], sum_recv.at[p, s1 - 1], device(0, {d1: 4 - s1}))

    for p in range(3):
        for a in range(4):
            arrived(p, 2, a)
        build(p, 2)

    load_in.wait()
    load_out.wait()
    pl.loop(0, 1)(expert)

    wait_for(cnt_in.at[pl.ds(1, 7)], cnt_recv)
    row = jnp.zeros((1, N), F32)
    for d in range(8):
        both = sum(cnt_in[d, b][:1] for b in range(4))
        row = row + jnp.where(iota((1, N), 1) % 8 == d, both, 0.0)
    cnt_row[...] = row
    pl.loop(0, 1)(drop)
    pl.loop(0, 1)(hand_out)

    @pl.loop(0, 7)
    def _(i):
        expert(7 - i)
        drop(7 - i)
        hand_out(7 - i)

        @pl.when(i > 2)
        def _():
            pass_on(10 - i)

    @pl.loop(0, 4)
    def _(i):
        pass_on(3 - i)

    for s2 in (1, 3, 2):
        for p in range(3):
            second(p, pl.ds(0, 1), s2, 0)

    for p in range(3):
        weigh(p)
    for p in range(3):
        wait_for(ends[p].at[pl.ds(2, 2), pl.ds(1, 3)], end_recv.at[p, 2])
        combine(p, 2)
    for p in range(3):
        combine(p, 3)
    for p in range(3):
        wait_for(ends[p].at[pl.ds(1, 1), pl.ds(1, 3)], end_recv.at[p, 1])
        combine(p, 1)
    for p in range(3):
        wait_for(ends[p].at[pl.ds(0, 1), pl.ds(1, 3)], end_recv.at[p, 0])
        combine(p, 0)

    for p in range(3):
        total = acc[:, part(p)]
        for i in (0, 2):
            wait_for(gots[p].at[i], sum_recv.at[p, i])
            total = total + gots[p][i]
        out_ref[:, part(p)] = total.astype(BF16)

    wait_for(cnt_in.at[pl.ds(1, 7)], cnt_send)
    for p in range(3):
        wait_for(info_all.at[p, pl.ds(0, 3)], info_send_a.at[p])
        wait_for(info_all.at[p, pl.ds(0, 12), ids], info_send_b.at[p])
        wait_for(toks[p].at[0, pl.ds(0, 3)], tok_send_a.at[p])
        wait_for(toks[p].at[pl.ds(0, 3)], tok_send_b.at[p])
        wait_for(blks[p].at[:, pl.ds(1, 7)], blk_send.at[p])
        wait_for(mids[p].at[:, :, pl.ds(1, 7)], mid_send.at[p])
        wait_for(ends[p].at[:, pl.ds(1, 3)], end_send.at[p])
        wait_for(sums[p], sum_send.at[p])


def solution(mesh):
    def device_fn(tokens, expert_ids, gate_weights, w_in, w_out):
        tok, width = tokens.shape
        top = expert_ids.shape[1]
        ff = w_in.shape[2]
        cap = tok * top
        slots = 2 * tok * top // N
        tiles = width // 128
        sizes = [128 * (tiles // 3 + (1 if p < tiles % 3 else 0)) for p in range(3)]
        cols = [(sum(sizes[:p]), sizes[p]) for p in range(3)]
        vmem = pl.BlockSpec(memory_space=pltpu.VMEM)
        anyspace = pl.BlockSpec(memory_space=pl.ANY)
        dma = pltpu.SemaphoreType.DMA
        return pl.pallas_call(
            functools.partial(kernel, cols, cap, slots),
            out_shape=jax.ShapeDtypeStruct((tok, width), BF16),
            in_specs=[vmem, vmem, vmem, anyspace, anyspace],
            out_specs=vmem,
            scratch_shapes=[
                pltpu.VMEM((width, ff), BF16),
                pltpu.VMEM((ff, width), BF16),
                *[pltpu.VMEM((4, 4, tok, s), BF16) for s in sizes],
                *[pltpu.VMEM((4, 8, 4, slots, s), BF16) for s in sizes],
                pltpu.VMEM((2, 4, 4, 4, slots, width), BF16),
                *[pltpu.VMEM((4, 4, 8, slots, s), BF16) for s in sizes],
                *[pltpu.VMEM((4, 4, 8, slots, s), BF16) for s in sizes],
                *[pltpu.VMEM((3, tok, s), F32) for s in sizes],
                *[pltpu.VMEM((3, tok, s), F32) for s in sizes],
                pltpu.VMEM((2 * top, tok), F32),
                pltpu.VMEM((3, 16, 2 * top, tok), F32),
                pltpu.VMEM((32, tok), F32),
                pltpu.VMEM((12, 3 * tok, 32 * slots), BF16),
                pltpu.VMEM((4, 8, N), F32),
                pltpu.VMEM((8, 4, 8, N), F32),
                pltpu.VMEM((1, N), F32),
                pltpu.VMEM((tok, width), F32),
                dma((2,)), dma((3,)), dma((3,)), dma((3, 16)), dma, dma, pltpu.SemaphoreType.REGULAR, dma((3,)), dma((3,)), dma((3, 16)),
                dma((3,)), dma((3, 8)), dma((3,)), dma((3, 8)), dma((3,)), dma((3, 3)), dma((3,)), dma((3, 4)),
            ],
            compiler_params=pltpu.CompilerParams(collective_id=0, has_side_effects=True, vmem_limit_bytes=67043328),
            name='expert_layer',
        )(tokens, expert_ids.T, gate_weights.T, w_in.reshape(width, ff), w_out.reshape(ff, width))

    token_spec = P(('data', 'row', 'col'), None)
    expert_spec = P(GRID_AXES, None, None)
    return jax.shard_map(device_fn, mesh=mesh, in_specs=(token_spec, token_spec, token_spec, expert_spec, expert_spec), out_specs=token_spec, check_vma=False)
```

```python
import functools

import jax
import jax.numpy as jnp
from jax import lax
from jax.experimental import pallas as pl
from jax.experimental.pallas import tpu as pltpu
from jax.sharding import PartitionSpec as P

GRID_AXES = ('row', 'col')
F32 = jnp.float32
BF16 = jnp.bfloat16
I32 = jnp.int32
SIDE = 4
N = 2 * SIDE ** 3
MESH = pl.DeviceIdType.MESH
Z, Y, X = 0, 1, 2
AXES = ((Z, Y, X), (Y, X, Z), (X, Z, Y))


def iota(shape, dim):
    return lax.broadcasted_iota(I32, shape, dim)


def kernel(cols, cap, slots, tokens_ref, ids_ref, gates_ref, w_in_hbm, w_out_hbm, out_ref,
           w_in, w_out, tok0, tok1, tok2, blk0, blk1, blk2, recv, mid0, mid1, mid2, end0, end1, end2,
           sum0, sum1, sum2, got0, got1, got2, info, info_all, places, scales, cnt_out, cnt_in, cnt_row, acc,
           w_sem, info_send_a, info_send_b, info_recv, cnt_send, cnt_recv, line_sem, tok_send_a, tok_send_b, tok_recv,
           blk_send, blk_recv, mid_send, mid_recv, end_send, end_recv, sum_send, sum_recv):
    toks, blks = (tok0, tok1, tok2), (blk0, blk1, blk2)
    mids, ends = (mid0, mid1, mid2), (end0, end1, end2)
    sums, gots = (sum0, sum1, sum2), (got0, got1, got2)
    tok, width = tokens_ref.shape
    top = ids_ref.shape[0]
    data = lax.axis_index('data')
    core = lax.axis_index('row')
    col = lax.axis_index('col')
    here = (lax.div(col, 16), lax.rem(lax.div(col, 4), 4), lax.rem(col, 4))
    me = core * 64 + col
    weight = (16, 4, 1)

    def device(d_core, d):
        at = [lax.rem(here[a] + d[a], 4) if a in d else here[a] for a in range(3)]
        return (data, lax.rem(core + d_core, 2), at[0] * 16 + at[1] * 4 + at[2])

    def number(d_core, d):
        n = ((core + d_core) & 1) * 64
        for a in range(3):
            n = n + (((here[a] + d[a]) & 3) if a in d else here[a]) * weight[a]
        return n

    def part(p):
        return pl.ds(cols[p][0], cols[p][1])

    def send(src, dst, send_sem, recv_sem, to):
        pltpu.make_async_remote_copy(src, dst, send_sem, recv_sem, device_id=to, device_id_type=MESH).start()

    def wait_for(ref, sem):
        pltpu.make_async_copy(ref, ref, sem).wait()

    load_in = pltpu.make_async_copy(w_in_hbm, w_in, w_sem.at[0])
    load_out = pltpu.make_async_copy(w_out_hbm, w_out, w_sem.at[1])

    near = [device(0, {a: step}) for a in range(3) for step in (1, 3)] + [device(1, {})]
    barrier = pltpu.get_barrier_semaphore()
    for to in near:
        pl.semaphore_signal(barrier, inc=1, device_id=to, device_id_type=MESH)
    load_in.start()
    load_out.start()
    info[:top] = ids_ref[...].astype(F32)
    info[top:] = gates_ref[...]
    pl.semaphore_wait(barrier, len(near))

    for p in range(3):
        for step in (1, 3):
            to = device(0, {AXES[p][0]: step})
            send(info, info_all.at[p, step], info_send_a.at[p], info_recv.at[p, step], to)
            send(tokens_ref.at[:, part(p)], toks[p].at[0, step], tok_send_a.at[p], tok_recv.at[p, step], to)

    ids = pl.ds(0, top)

    def gather_on(p, a, src, ids_src):
        for step in (1, 3):
            to = device(0, {AXES[p][1]: step})
            send(ids_src, info_all.at[p, 4 * step + a, ids], info_send_b.at[p], info_recv.at[p, 4 * step + a], to)
            send(src, toks[p].at[step, a], tok_send_b.at[p], tok_recv.at[p, 4 * step + a], to)

    for p in range(3):
        gather_on(p, 0, tokens_ref.at[:, part(p)], info.at[ids])
    for p in range(3):
        toks[p][0, 0] = tokens_ref[:, part(p)]
        info_all[p, 0] = info[...]

    def arrived(p, b, a):
        what = info_all.at[p, a] if b == 0 else info_all.at[p, 4 * b + a, ids]
        wait_for(what, info_recv.at[p, 4 * b + a])
        wait_for(toks[p].at[b, a], tok_recv.at[p, 4 * b + a])

    half = tok // 2
    for p in range(3):
        t = toks[p]
        for step, rows in ((1, pl.ds(0, half)), (3, pl.ds(half, half))):
            arrived(p, 0, step)
            to = device(0, {AXES[p][0]: step})
            if step == 1:
                send(info_all.at[p, 1], info_all.at[p, 2], info_send_a.at[p], info_recv.at[p, 2], to)
            send(t.at[0, step, rows], t.at[0, 2, rows], tok_send_a.at[p], tok_recv.at[p, 2], to)
            gather_on(p, step, t.at[0, step], info_all.at[p, step, ids])

    for p in range(3):
        arrived(p, 0, 2)
        gather_on(p, 2, toks[p].at[0, 2], info_all.at[p, 2, ids])

    pl.semaphore_signal(line_sem, inc=1, device_id=near[6], device_id_type=MESH)
    pl.semaphore_wait(line_sem, 1)

    later = (iota((tok, tok), 0) < iota((tok, tok), 1)).astype(BF16)

    def where_in(p, d_core, s1, s2, s3):
        at = [None] * 3
        for axis, s in zip(AXES[p], (s1, s2, s3)):
            at[axis] = s
        return (d_core, *at)

    def build(p, b):
        t, blk = toks[p], blks[p]
        d3 = AXES[p][2]
        dest = iota((8, tok), 0)
        expert_id = number(dest >> 2, {d3: dest & 3}).astype(F32)[None]
        mark = jnp.zeros((4, 8, tok), F32)
        for j in range(top):
            mark = jnp.where(info_all[p, pl.ds(4 * b, 4), j:j + 1, :] == expert_id, 1.0, mark)
        mark = mark.reshape(32, tok)
        place = jnp.dot(mark.astype(BF16), later, preferred_element_type=F32)
        places[...] = jnp.where(mark > 0, place, -1.0)
        if p == 0:
            wide = [jnp.zeros((32, tok), F32)] * 4
            wide[b] = mark
            wide = jnp.concatenate(wide, axis=0).astype(BF16)
            cnt_out[b] = lax.dot_general(jnp.ones((8, tok), BF16), wide, (((1,), (1,)), ((), ())), preferred_element_type=F32)
            cnt_in[0, b] = cnt_out[b]

            @pl.loop(1, 8)
            def _(d):
                send(cnt_out.at[b], cnt_in.at[d, b], cnt_send, cnt_recv, device(lax.div(d, 4), {d3: lax.rem(d, 4)}))

        @pl.loop(0, 4)
        def _(a):
            place = places[pl.ds(a * 8, 8), :]
            pick = place[:, None, :] == iota((8, slots, tok), 1).astype(F32)
            pick = jnp.where(pick, 1.0, 0.0).reshape(8 * slots, tok).astype(BF16)
            rows = jnp.dot(pick, t[b, a], preferred_element_type=F32).astype(BF16).reshape(8, slots, cols[p][1])
            blk[b, :, a] = rows
            recv[where_in(p, 0, a, b, 0) + (slice(None), part(p))] = rows[0]

        for h in range(2):
            @pl.loop(1, 8)
            def _(d):
                d_core, s3 = lax.div(d, 4), lax.rem(d, 4)
                high = {AXES[p][0]: h, AXES[p][1]: b // 2, AXES[p][2]: lax.div(s3, 2)}
                cube = high[Z] * 4 + high[Y] * 2 + high[X]
                send(blk.at[b, d, pl.ds(2 * h, 2)],
                     recv.at[where_in(p, d_core, pl.ds(2 * h, 2), b, s3) + (slice(None), part(p))],
                     blk_send.at[p], blk_recv.at[p, cube], device(d_core, {AXES[p][2]: s3}))

    def relay(p, step, a):
        t, to = toks[p], device(0, {AXES[p][1]: step})
        arrived(p, step, a)
        send(info_all.at[p, 4 * step + a, ids], info_all.at[p, 8 + a, ids], info_send_b.at[p], info_recv.at[p, 8 + a], to)
        send(t.at[step, a], t.at[2, a], tok_send_b.at[p], tok_recv.at[p, 8 + a], to)

    for p in range(3):
        relay(p, 1, 0)
    for p in range(3):
        build(p, 0)

    for p, step, a in [(p, step, a) for step, a in ((3, 1), (3, 3), (1, 2)) for p in range(3)]:
        relay(p, step, a)

    for step, rest in ((1, (1, 3)), (3, (0, 2))):
        for p in range(3):
            for a in rest:
                arrived(p, step, a)
            build(p, step)

    def halves(j):
        return (lax.div(j, 4), lax.rem(lax.div(j, 2), 2), lax.rem(j, 2))

    def wait_blocks(p, h3, refs, sem):
        @pl.when(h3 == 0)
        def _():
            wait_for(refs.at[0, pl.ds(0, 3)], sem)

        @pl.when(h3 == 1)
        def _():
            wait_for(refs.at[0, pl.ds(0, 4)], sem)

    def expert(j):
        high = halves(j)
        pair = [pl.ds(2 * h, 2) for h in high]
        for p in range(3):
            wait_blocks(p, high[AXES[p][2]], blks[p], blk_recv.at[p, j])
        cube = (slice(None), *pair)
        x = recv[cube].reshape(16 * slots, width)
        hidden = jax.nn.gelu(jnp.dot(x, w_in[...], preferred_element_type=F32)).astype(BF16)
        o = jnp.dot(hidden, w_out[...], preferred_element_type=F32).astype(BF16)
        recv[cube] = o.reshape(2, 2, 2, 2, slots, width)

    def drop(j):
        high = halves(j)
        cube = (slice(None), *[pl.ds(2 * h, 2) for h in high])
        rows = 16 * slots
        r = iota((rows, N), 0)
        i = r // slots
        taker = number((i >> 3) & 1, {Z: 4 - (2 * high[Z] + ((i >> 2) & 1)), Y: 4 - (2 * high[Y] + ((i >> 1) & 1)), X: 4 - (2 * high[X] + (i & 1))})
        c = iota((rows, N), 1)
        d1, d2, d3 = AXES[0]
        source = number((c >> 2) & 1, {d1: 4 - ((c >> 3) & 3), d2: 4 - (c >> 5), d3: 4 - (c & 3)})
        before = jnp.sum(jnp.where(source < taker, cnt_row[...], 0.0), axis=1, keepdims=True)
        keep = before + (iota((rows, 1), 0) % slots).astype(F32) < float(cap)
        o = recv[cube].reshape(rows, width)
        recv[cube] = jnp.where(keep, o, jnp.zeros_like(o)).reshape(2, 2, 2, 2, slots, width)

    def hand_out(j):
        high = halves(j)
        pair = [pl.ds(2 * h, 2) for h in high]
        for p in range(3):
            d3 = AXES[p][2]
            rest = [pair[a] for a in range(3) if a != d3]

            def along(s3):
                return tuple(s3 if a == d3 else pair[a] for a in range(3))

            @pl.when(high[d3] == 0)
            def _():
                mids[p][(*rest, 0)] = recv[(0, *along(0), slice(None), part(p))]

            @pl.loop(jnp.where(high[d3] == 0, 1, 0), 4)
            def _(i):
                d_core, s3 = lax.div(i, 2), 2 * high[d3] + lax.rem(i, 2)
                send(recv.at[(d_core, *along(s3), slice(None), part(p))], mids[p].at[(*rest, d_core * 4 + s3)],
                     mid_send.at[p], mid_recv.at[p, j], device(d_core, {d3: 4 - s3}))

    def middle(p, s1, s2):
        d1, d2 = AXES[p][:2]
        return (s1, s2) if d1 < d2 else (s2, s1)

    def second(p, s1, s2, sem):
        send(mids[p].at[middle(p, s1, s2)], ends[p].at[s1, s2], end_send.at[p], end_recv.at[p, sem], device(0, {AXES[p][1]: 4 - s2}))

    def pass_on(j):
        high = halves(j)
        for p in range(3):
            d1, d2, d3 = AXES[p]

            @pl.when(high[d3] == 0)
            def _():
                wait_blocks(p, 1, blks[p], mid_recv.at[p, j + (4, 2, 1)[d3]])
                wait_blocks(p, 0, blks[p], mid_recv.at[p, j])
                first = pl.ds(2 * high[d1], 2)

                @pl.when(high[d2] == 0)
                def _():
                    ends[p][first, 0] = mids[p][middle(p, first, 0)]

                @pl.loop(jnp.where(high[d2] == 0, 1, 2 * high[d2]), 2 * high[d2] + 2)
                def _(s2):
                    @pl.when(high[d1] == 1)
                    def _():
                        second(p, pl.ds(2, 2), s2, 2)

                    @pl.when(high[d1] == 0)
                    def _():
                        second(p, pl.ds(1, 1), s2, 1)

    def weigh(p):
        d1, d2, d3 = AXES[p]
        e = iota((32, tok), 0)
        expert_id = number((e >> 2) & 1, {d2: e >> 3, d3: e & 3}).astype(F32)

        @pl.loop(0, 4)
        def _(s1):
            ids, gts = info_all[p, s1, :top], info_all[p, s1, top:]
            mark = jnp.zeros((32, tok), F32)
            gate = jnp.zeros((32, tok), F32)
            for j in range(top):
                hit = ids[j:j + 1, :] == expert_id
                mark = jnp.where(hit, 1.0, mark)
                gate = jnp.where(hit, gts[j:j + 1, :], gate)
            place = jnp.dot(mark.astype(BF16), later, preferred_element_type=F32)
            place = jnp.where(mark > 0, place, -1.0)
            scale = jnp.where(place[:, None, :] == iota((32, slots, tok), 1).astype(F32), gate[:, None, :], 0.0)
            scale = scale.reshape(32 * slots, tok).T
            high = scale.astype(BF16)
            left = scale - high.astype(F32)
            mid = left.astype(BF16)
            low = (left - mid.astype(F32)).astype(BF16)
            scales[4 * p + s1] = jnp.concatenate([high, mid, low], axis=0)

    def combine(p, s1):
        rows = ends[p][s1].reshape(32 * slots, cols[p][1])
        mixed = jnp.dot(scales[4 * p + s1], rows, preferred_element_type=F32)
        mixed = mixed[:tok] + (mixed[tok:2 * tok] + mixed[2 * tok:])
        d1, low, high = AXES[p][0], pl.ds(0, half), pl.ds(half, half)
        if s1 == 0:
            acc[:, part(p)] = tokens_ref[:, part(p)].astype(F32) + mixed
            return
        sums[p][s1 - 1] = mixed
        if s1 == 2:
            send(sums[p].at[1, low], gots[p].at[1, low], sum_send.at[p], sum_recv.at[p, 1], device(0, {d1: 3}))
            send(sums[p].at[1, high], gots[p].at[1, high], sum_send.at[p], sum_recv.at[p, 3], device(0, {d1: 1}))
            return
        rows, sem = (low, 1) if s1 == 1 else (high, 3)
        wait_for(gots[p].at[1, rows], sum_recv.at[p, sem])
        sums[p][s1 - 1, rows] = sums[p][s1 - 1, rows] + gots[p][1, rows]
        send(sums[p].at[s1 - 1], gots[p].at[s1 - 1], sum_send.at[p], sum_recv.at[p, s1 - 1], device(0, {d1: 4 - s1}))

    for p in range(3):
        for a in range(4):
            arrived(p, 2, a)
        build(p, 2)

    load_in.wait()
    load_out.wait()
    pl.loop(0, 1)(expert)

    wait_for(cnt_in.at[pl.ds(1, 7)], cnt_recv)
    row = jnp.zeros((1, N), F32)
    for d in range(8):
        both = sum(cnt_in[d, b][:1] for b in range(4))
        row = row + jnp.where(iota((1, N), 1) % 8 == d, both, 0.0)
    cnt_row[...] = row
    pl.loop(0, 1)(drop)
    pl.loop(0, 1)(hand_out)

    @pl.loop(0, 7)
    def _(i):
        expert(7 - i)
        drop(7 - i)
        hand_out(7 - i)

        @pl.when(i > 2)
        def _():
            pass_on(10 - i)

    @pl.loop(0, 4)
    def _(i):
        pass_on(3 - i)

    for p in range(3):
        weigh(p)
    for p in range(3):
        wait_for(ends[p].at[pl.ds(2, 2), pl.ds(1, 3)], end_recv.at[p, 2])
        combine(p, 2)

    for s2 in (1, 3, 2):
        for p in range(3):
            second(p, pl.ds(0, 1), s2, 0)

    for p in range(3):
        combine(p, 3)
    for p in range(3):
        wait_for(ends[p].at[pl.ds(1, 1), pl.ds(1, 3)], end_recv.at[p, 1])
        combine(p, 1)
    for p in range(3):
        wait_for(ends[p].at[pl.ds(0, 1), pl.ds(1, 3)], end_recv.at[p, 0])
        combine(p, 0)

    for p in range(3):
        total = acc[:, part(p)]
        for i in (0, 2):
            wait_for(gots[p].at[i], sum_recv.at[p, i])
            total = total + gots[p][i]
        out_ref[:, part(p)] = total.astype(BF16)

    wait_for(cnt_in.at[pl.ds(1, 7)], cnt_send)
    for p in range(3):
        wait_for(info_all.at[p, pl.ds(0, 3)], info_send_a.at[p])
        wait_for(info_all.at[p, pl.ds(0, 12), ids], info_send_b.at[p])
        wait_for(toks[p].at[0, pl.ds(0, 3)], tok_send_a.at[p])
        wait_for(toks[p].at[pl.ds(0, 3)], tok_send_b.at[p])
        wait_for(blks[p].at[:, pl.ds(1, 7)], blk_send.at[p])
        wait_for(mids[p].at[:, :, pl.ds(1, 7)], mid_send.at[p])
        wait_for(ends[p].at[:, pl.ds(1, 3)], end_send.at[p])
        wait_for(sums[p], sum_send.at[p])


def solution(mesh):
    def device_fn(tokens, expert_ids, gate_weights, w_in, w_out):
        tok, width = tokens.shape
        top = expert_ids.shape[1]
        ff = w_in.shape[2]
        cap = tok * top
        slots = 2 * tok * top // N
        tiles = width // 128
        sizes = [128 * (tiles // 3 + (1 if p < tiles % 3 else 0)) for p in range(3)]
        cols = [(sum(sizes[:p]), sizes[p]) for p in range(3)]
        vmem = pl.BlockSpec(memory_space=pltpu.VMEM)
        anyspace = pl.BlockSpec(memory_space=pl.ANY)
        dma = pltpu.SemaphoreType.DMA
        return pl.pallas_call(
            functools.partial(kernel, cols, cap, slots),
            out_shape=jax.ShapeDtypeStruct((tok, width), BF16),
            in_specs=[vmem, vmem, vmem, anyspace, anyspace],
            out_specs=vmem,
            scratch_shapes=[
                pltpu.VMEM((width, ff), BF16),
                pltpu.VMEM((ff, width), BF16),
                *[pltpu.VMEM((4, 4, tok, s), BF16) for s in sizes],
                *[pltpu.VMEM((4, 8, 4, slots, s), BF16) for s in sizes],
                pltpu.VMEM((2, 4, 4, 4, slots, width), BF16),
                *[pltpu.VMEM((4, 4, 8, slots, s), BF16) for s in sizes],
                *[pltpu.VMEM((4, 4, 8, slots, s), BF16) for s in sizes],
                *[pltpu.VMEM((3, tok, s), F32) for s in sizes],
                *[pltpu.VMEM((3, tok, s), F32) for s in sizes],
                pltpu.VMEM((2 * top, tok), F32),
                pltpu.VMEM((3, 16, 2 * top, tok), F32),
                pltpu.VMEM((32, tok), F32),
                pltpu.VMEM((12, 3 * tok, 32 * slots), BF16),
                pltpu.VMEM((4, 8, N), F32),
                pltpu.VMEM((8, 4, 8, N), F32),
                pltpu.VMEM((1, N), F32),
                pltpu.VMEM((tok, width), F32),
                dma((2,)), dma((3,)), dma((3,)), dma((3, 16)), dma, dma, pltpu.SemaphoreType.REGULAR, dma((3,)), dma((3,)), dma((3, 16)),
                dma((3,)), dma((3, 8)), dma((3,)), dma((3, 8)), dma((3,)), dma((3, 3)), dma((3,)), dma((3, 4)),
            ],
            compiler_params=pltpu.CompilerParams(collective_id=0, has_side_effects=True, vmem_limit_bytes=67043328),
            name='expert_layer',
        )(tokens, expert_ids.T, gate_weights.T, w_in.reshape(width, ff), w_out.reshape(ff, width))

    token_spec = P(('data', 'row', 'col'), None)
    expert_spec = P(GRID_AXES, None, None)
    return jax.shard_map(device_fn, mesh=mesh, in_specs=(token_spec, token_spec, token_spec, expert_spec, expert_spec), out_specs=token_spec, check_vma=False)
```

```python
import functools

import jax
import jax.numpy as jnp
from jax import lax
from jax.experimental import pallas as pl
from jax.experimental.pallas import tpu as pltpu
from jax.sharding import PartitionSpec as P

GRID_AXES = ('row', 'col')
F32 = jnp.float32
BF16 = jnp.bfloat16
I32 = jnp.int32
SIDE = 4
N = 2 * SIDE ** 3
MESH = pl.DeviceIdType.MESH
Z, Y, X = 0, 1, 2
AXES = ((Z, Y, X), (Y, X, Z), (X, Z, Y))


def iota(shape, dim):
    return lax.broadcasted_iota(I32, shape, dim)


def kernel(cols, back_cols, cap, slots, tokens_ref, ids_ref, gates_ref, w_in_hbm, w_out_hbm, out_ref,
           w_in, w_out, tok0, tok1, tok2, blk0, blk1, blk2, recv, mid0, mid1, mid2, end0, end1, end2,
           sum0, sum1, sum2, got0, got1, got2, info, info_all, places, scales, cnt_out, cnt_in, cnt_row, acc,
           w_sem, info_send_a, info_send_b, info_recv, cnt_send, cnt_recv, line_sem, tok_send_a, tok_send_b, tok_recv,
           blk_send, blk_recv, mid_send, mid_recv, end_send, end_recv, sum_send, sum_recv):
    toks, blks = (tok0, tok1, tok2), (blk0, blk1, blk2)
    mids, ends = (mid0, mid1, mid2), (end0, end1, end2)
    sums, gots = (sum0, sum1, sum2), (got0, got1, got2)
    tok, width = tokens_ref.shape
    top = ids_ref.shape[0]
    data = lax.axis_index('data')
    core = lax.axis_index('row')
    col = lax.axis_index('col')
    here = (lax.div(col, 16), lax.rem(lax.div(col, 4), 4), lax.rem(col, 4))
    me = core * 64 + col
    weight = (16, 4, 1)

    def device(d_core, d):
        at = [lax.rem(here[a] + d[a], 4) if a in d else here[a] for a in range(3)]
        return (data, lax.rem(core + d_core, 2), at[0] * 16 + at[1] * 4 + at[2])

    def number(d_core, d):
        n = ((core + d_core) & 1) * 64
        for a in range(3):
            n = n + (((here[a] + d[a]) & 3) if a in d else here[a]) * weight[a]
        return n

    def part(p):
        return pl.ds(cols[p][0], cols[p][1])

    def send(src, dst, send_sem, recv_sem, to):
        pltpu.make_async_remote_copy(src, dst, send_sem, recv_sem, device_id=to, device_id_type=MESH).start()

    def wait_for(ref, sem):
        pltpu.make_async_copy(ref, ref, sem).wait()

    load_in = pltpu.make_async_copy(w_in_hbm, w_in, w_sem.at[0])
    load_out = pltpu.make_async_copy(w_out_hbm, w_out, w_sem.at[1])

    near = [device(0, {a: step}) for a in range(3) for step in (1, 3)] + [device(1, {})]
    barrier = pltpu.get_barrier_semaphore()
    for to in near:
        pl.semaphore_signal(barrier, inc=1, device_id=to, device_id_type=MESH)
    load_in.start()
    load_out.start()
    info[:top] = ids_ref[...].astype(F32)
    info[top:] = gates_ref[...]
    pl.semaphore_wait(barrier, len(near))

    for p in range(3):
        for step in (1, 3):
            to = device(0, {AXES[p][0]: step})
            send(info, info_all.at[p, step], info_send_a.at[p], info_recv.at[p, step], to)
            send(tokens_ref.at[:, part(p)], toks[p].at[0, step], tok_send_a.at[p], tok_recv.at[p, step], to)

    ids = pl.ds(0, top)

    def gather_on(p, a, src, ids_src):
        for step in (1, 3):
            to = device(0, {AXES[p][1]: step})
            send(ids_src, info_all.at[p, 4 * step + a, ids], info_send_b.at[p], info_recv.at[p, 4 * step + a], to)
            send(src, toks[p].at[step, a], tok_send_b.at[p], tok_recv.at[p, 4 * step + a], to)

    for p in range(3):
        gather_on(p, 0, tokens_ref.at[:, part(p)], info.at[ids])
    for p in range(3):
        toks[p][0, 0] = tokens_ref[:, part(p)]
        info_all[p, 0] = info[...]

    def arrived(p, b, a):
        what = info_all.at[p, a] if b == 0 else info_all.at[p, 4 * b + a, ids]
        wait_for(what, info_recv.at[p, 4 * b + a])
        wait_for(toks[p].at[b, a], tok_recv.at[p, 4 * b + a])

    half = tok // 2
    for p in range(3):
        t = toks[p]
        for step, rows in ((1, pl.ds(0, half)), (3, pl.ds(half, half))):
            arrived(p, 0, step)
            to = device(0, {AXES[p][0]: step})
            if step == 1:
                send(info_all.at[p, 1], info_all.at[p, 2], info_send_a.at[p], info_recv.at[p, 2], to)
            send(t.at[0, step, rows], t.at[0, 2, rows], tok_send_a.at[p], tok_recv.at[p, 2], to)
            gather_on(p, step, t.at[0, step], info_all.at[p, step, ids])

    for p in range(3):
        arrived(p, 0, 2)
        gather_on(p, 2, toks[p].at[0, 2], info_all.at[p, 2, ids])

    pl.semaphore_signal(line_sem, inc=1, device_id=near[6], device_id_type=MESH)
    pl.semaphore_wait(line_sem, 1)

    later = (iota((tok, tok), 0) < iota((tok, tok), 1)).astype(BF16)

    def where_in(p, d_core, s1, s2, s3):
        at = [None] * 3
        for axis, s in zip(AXES[p], (s1, s2, s3)):
            at[axis] = s
        return (d_core, *at)

    def build(p, b):
        t, blk = toks[p], blks[p]
        d3 = AXES[p][2]
        dest = iota((8, tok), 0)
        expert_id = number(dest >> 2, {d3: dest & 3}).astype(F32)[None]
        mark = jnp.zeros((4, 8, tok), F32)
        for j in range(top):
            mark = jnp.where(info_all[p, pl.ds(4 * b, 4), j:j + 1, :] == expert_id, 1.0, mark)
        mark = mark.reshape(32, tok)
        place = jnp.dot(mark.astype(BF16), later, preferred_element_type=F32)
        places[...] = jnp.where(mark > 0, place, -1.0)
        if p == 0:
            wide = [jnp.zeros((32, tok), F32)] * 4
            wide[b] = mark
            wide = jnp.concatenate(wide, axis=0).astype(BF16)
            cnt_out[b] = lax.dot_general(jnp.ones((8, tok), BF16), wide, (((1,), (1,)), ((), ())), preferred_element_type=F32)
            cnt_in[0, b] = cnt_out[b]

            @pl.loop(1, 8)
            def _(d):
                send(cnt_out.at[b], cnt_in.at[d, b], cnt_send, cnt_recv, device(lax.div(d, 4), {d3: lax.rem(d, 4)}))

        @pl.loop(0, 4)
        def _(a):
            place = places[pl.ds(a * 8, 8), :]
            pick = place[:, None, :] == iota((8, slots, tok), 1).astype(F32)
            pick = jnp.where(pick, 1.0, 0.0).reshape(8 * slots, tok).astype(BF16)
            rows = jnp.dot(pick, t[b, a], preferred_element_type=F32).astype(BF16).reshape(8, slots, cols[p][1])
            blk[b, :, a] = rows
            recv[where_in(p, 0, a, b, 0) + (slice(None), part(p))] = rows[0]

        for h in range(2):
            @pl.loop(1, 8)
            def _(d):
                d_core, s3 = lax.div(d, 4), lax.rem(d, 4)
                high = {AXES[p][0]: h, AXES[p][1]: b // 2, AXES[p][2]: lax.div(s3, 2)}
                cube = high[Z] * 4 + high[Y] * 2 + high[X]
                send(blk.at[b, d, pl.ds(2 * h, 2)],
                     recv.at[where_in(p, d_core, pl.ds(2 * h, 2), b, s3) + (slice(None), part(p))],
                     blk_send.at[p], blk_recv.at[p, cube], device(d_core, {AXES[p][2]: s3}))

    def relay(p, step, a):
        t, to = toks[p], device(0, {AXES[p][1]: step})
        arrived(p, step, a)
        send(info_all.at[p, 4 * step + a, ids], info_all.at[p, 8 + a, ids], info_send_b.at[p], info_recv.at[p, 8 + a], to)
        send(t.at[step, a], t.at[2, a], tok_send_b.at[p], tok_recv.at[p, 8 + a], to)

    for p in range(3):
        relay(p, 1, 0)
    for p in range(3):
        build(p, 0)

    for p, step, a in [(p, step, a) for step, a in ((3, 1), (3, 3), (1, 2)) for p in range(3)]:
        relay(p, step, a)

    for step, rest in ((1, (1, 3)), (3, (0, 2))):
        for p in range(3):
            for a in rest:
                arrived(p, step, a)
            build(p, step)

    def halves(j):
        return (lax.div(j, 4), lax.rem(lax.div(j, 2), 2), lax.rem(j, 2))

    def wait_blocks(p, h3, refs, sem):
        @pl.when(h3 == 0)
        def _():
            wait_for(refs.at[0, pl.ds(0, 3)], sem)

        @pl.when(h3 == 1)
        def _():
            wait_for(refs.at[0, pl.ds(0, 4)], sem)

    def expert(j):
        high = halves(j)
        pair = [pl.ds(2 * h, 2) for h in high]
        for p in range(3):
            wait_blocks(p, high[AXES[p][2]], blks[p], blk_recv.at[p, j])
        cube = (slice(None), *pair)
        x = recv[cube].reshape(16 * slots, width)
        hidden = jax.nn.gelu(jnp.dot(x, w_in[...], preferred_element_type=F32)).astype(BF16)
        o = jnp.dot(hidden, w_out[...], preferred_element_type=F32).astype(BF16)
        recv[cube] = o.reshape(2, 2, 2, 2, slots, width)

    def drop(j):
        high = halves(j)
        cube = (slice(None), *[pl.ds(2 * h, 2) for h in high])
        rows = 16 * slots
        r = iota((rows, N), 0)
        i = r // slots
        taker = number((i >> 3) & 1, {Z: 4 - (2 * high[Z] + ((i >> 2) & 1)), Y: 4 - (2 * high[Y] + ((i >> 1) & 1)), X: 4 - (2 * high[X] + (i & 1))})
        c = iota((rows, N), 1)
        d1, d2, d3 = AXES[0]
        source = number((c >> 2) & 1, {d1: 4 - ((c >> 3) & 3), d2: 4 - (c >> 5), d3: 4 - (c & 3)})
        before = jnp.sum(jnp.where(source < taker, cnt_row[...], 0.0), axis=1, keepdims=True)
        keep = before + (iota((rows, 1), 0) % slots).astype(F32) < float(cap)
        o = recv[cube].reshape(rows, width)
        recv[cube] = jnp.where(keep, o, jnp.zeros_like(o)).reshape(2, 2, 2, 2, slots, width)

    def back_part(p):
        return pl.ds(back_cols[p][0], back_cols[p][1])

    def wait_mid(p, blocks, sem):
        wait_for(mids[p].at[0, pl.ds(0, 2), pl.ds(0, blocks // 2)], sem)

    def hand_out(j):
        high = halves(j)
        pair = [pl.ds(2 * h, 2) for h in high]
        for p in range(3):
            d3 = AXES[p][2]
            rest = [pair[a] for a in range(3) if a != d3]

            def along(s3):
                return tuple(s3 if a == d3 else pair[a] for a in range(3))

            @pl.when(high[d3] == 0)
            def _():
                mids[p][(*rest, 0)] = recv[(0, *along(0), slice(None), back_part(p))]

            @pl.loop(jnp.where(high[d3] == 0, 1, 0), 4)
            def _(i):
                d_core, s3 = lax.div(i, 2), 2 * high[d3] + lax.rem(i, 2)
                send(recv.at[(d_core, *along(s3), slice(None), back_part(p))], mids[p].at[(*rest, d_core * 4 + s3)],
                     mid_send.at[p], mid_recv.at[p, j], device(d_core, {d3: 4 - s3}))

    def middle(p, s1, s2):
        d1, d2 = AXES[p][:2]
        return (s1, s2) if d1 < d2 else (s2, s1)

    def second(p, s1, s2, sem):
        send(mids[p].at[middle(p, s1, s2)], ends[p].at[s1, s2], end_send.at[p], end_recv.at[p, sem], device(0, {AXES[p][1]: 4 - s2}))

    def pass_on(j):
        high = halves(j)
        for p in range(3):
            d1, d2, d3 = AXES[p]

            @pl.when(high[d3] == 0)
            def _():
                wait_mid(p, 16, mid_recv.at[p, j + (4, 2, 1)[d3]])
                wait_mid(p, 12, mid_recv.at[p, j])
                first = pl.ds(2 * high[d1], 2)

                @pl.when(high[d2] == 0)
                def _():
                    ends[p][first, 0] = mids[p][middle(p, first, 0)]

                @pl.loop(jnp.where(high[d2] == 0, 1, 2 * high[d2]), 2 * high[d2] + 2)
                def _(s2):
                    @pl.when(high[d1] == 1)
                    def _():
                        second(p, pl.ds(2, 2), s2, 2)

                    @pl.when(high[d1] == 0)
                    def _():
                        second(p, pl.ds(1, 1), s2, 1)

    def weigh(p):
        d1, d2, d3 = AXES[p]
        e = iota((32, tok), 0)
        expert_id = number((e >> 2) & 1, {d2: e >> 3, d3: e & 3}).astype(F32)

        @pl.loop(0, 4)
        def _(s1):
            ids, gts = info_all[p, s1, :top], info_all[p, s1, top:]
            mark = jnp.zeros((32, tok), F32)
            gate = jnp.zeros((32, tok), F32)
            for j in range(top):
                hit = ids[j:j + 1, :] == expert_id
                mark = jnp.where(hit, 1.0, mark)
                gate = jnp.where(hit, gts[j:j + 1, :], gate)
            place = jnp.dot(mark.astype(BF16), later, preferred_element_type=F32)
            place = jnp.where(mark > 0, place, -1.0)
            scale = jnp.where(place[:, None, :] == iota((32, slots, tok), 1).astype(F32), gate[:, None, :], 0.0)
            scale = scale.reshape(32 * slots, tok).T
            high = scale.astype(BF16)
            left = scale - high.astype(F32)
            mid = left.astype(BF16)
            low = (left - mid.astype(F32)).astype(BF16)
            scales[4 * p + s1] = jnp.concatenate([high, mid, low], axis=0)

    def combine(p, s1):
        rows = ends[p][s1].reshape(32 * slots, back_cols[p][1])
        mixed = jnp.dot(scales[4 * p + s1], rows, preferred_element_type=F32)
        mixed = mixed[:tok] + (mixed[tok:2 * tok] + mixed[2 * tok:])
        d1, low, high = AXES[p][0], pl.ds(0, half), pl.ds(half, half)
        if s1 == 0:
            acc[:, back_part(p)] = tokens_ref[:, back_part(p)].astype(F32) + mixed
            return
        sums[p][s1 - 1] = mixed
        if s1 == 2:
            send(sums[p].at[1, low], gots[p].at[1, low], sum_send.at[p], sum_recv.at[p, 1], device(0, {d1: 3}))
            send(sums[p].at[1, high], gots[p].at[1, high], sum_send.at[p], sum_recv.at[p, 3], device(0, {d1: 1}))
            return
        rows, sem = (low, 1) if s1 == 1 else (high, 3)
        wait_for(gots[p].at[1, rows], sum_recv.at[p, sem])
        sums[p][s1 - 1, rows] = sums[p][s1 - 1, rows] + gots[p][1, rows]
        send(sums[p].at[s1 - 1], gots[p].at[s1 - 1], sum_send.at[p], sum_recv.at[p, s1 - 1], device(0, {d1: 4 - s1}))

    for p in range(3):
        for a in range(4):
            arrived(p, 2, a)
        build(p, 2)

    load_in.wait()
    load_out.wait()
    pl.loop(0, 1)(expert)

    wait_for(cnt_in.at[pl.ds(1, 7)], cnt_recv)
    row = jnp.zeros((1, N), F32)
    for d in range(8):
        both = sum(cnt_in[d, b][:1] for b in range(4))
        row = row + jnp.where(iota((1, N), 1) % 8 == d, both, 0.0)
    cnt_row[...] = row
    pl.loop(0, 1)(drop)
    pl.loop(0, 1)(hand_out)

    @pl.loop(0, 7)
    def _(i):
        expert(7 - i)
        drop(7 - i)
        hand_out(7 - i)

        @pl.when(i > 2)
        def _():
            pass_on(10 - i)

    @pl.loop(0, 4)
    def _(i):
        pass_on(3 - i)

    for p in range(3):
        weigh(p)
    for p in range(3):
        wait_for(ends[p].at[pl.ds(2, 2), pl.ds(1, 3)], end_recv.at[p, 2])
        combine(p, 2)

    for s2 in (1, 3, 2):
        for p in range(3):
            second(p, pl.ds(0, 1), s2, 0)

    for p in range(3):
        combine(p, 3)
    for p in range(3):
        wait_for(ends[p].at[pl.ds(1, 1), pl.ds(1, 3)], end_recv.at[p, 1])
        combine(p, 1)
    for p in range(3):
        wait_for(ends[p].at[pl.ds(0, 1), pl.ds(1, 3)], end_recv.at[p, 0])
        combine(p, 0)

    for p in range(3):
        total = acc[:, back_part(p)]
        for i in (0, 2):
            wait_for(gots[p].at[i], sum_recv.at[p, i])
            total = total + gots[p][i]
        out_ref[:, back_part(p)] = total.astype(BF16)

    wait_for(cnt_in.at[pl.ds(1, 7)], cnt_send)
    for p in range(3):
        wait_for(info_all.at[p, pl.ds(0, 3)], info_send_a.at[p])
        wait_for(info_all.at[p, pl.ds(0, 12), ids], info_send_b.at[p])
        wait_for(toks[p].at[0, pl.ds(0, 3)], tok_send_a.at[p])
        wait_for(toks[p].at[pl.ds(0, 3)], tok_send_b.at[p])
        wait_for(blks[p].at[:, pl.ds(1, 7)], blk_send.at[p])
        wait_for(mids[p].at[:, :, pl.ds(1, 7)], mid_send.at[p])
        wait_for(ends[p].at[:, pl.ds(1, 3)], end_send.at[p])
        wait_for(sums[p], sum_send.at[p])


def solution(mesh):
    def device_fn(tokens, expert_ids, gate_weights, w_in, w_out):
        tok, width = tokens.shape
        top = expert_ids.shape[1]
        ff = w_in.shape[2]
        cap = tok * top
        slots = 2 * tok * top // N
        tiles = width // 128
        sizes = [128 * (tiles // 3 + (1 if p < tiles % 3 else 0)) for p in range(3)]
        cols = [(sum(sizes[:p]), sizes[p]) for p in range(3)]
        back = sizes[::-1]
        back_cols = [(sum(back[:p]), back[p]) for p in range(3)]
        vmem = pl.BlockSpec(memory_space=pltpu.VMEM)
        anyspace = pl.BlockSpec(memory_space=pl.ANY)
        dma = pltpu.SemaphoreType.DMA
        return pl.pallas_call(
            functools.partial(kernel, cols, back_cols, cap, slots),
            out_shape=jax.ShapeDtypeStruct((tok, width), BF16),
            in_specs=[vmem, vmem, vmem, anyspace, anyspace],
            out_specs=vmem,
            scratch_shapes=[
                pltpu.VMEM((width, ff), BF16),
                pltpu.VMEM((ff, width), BF16),
                *[pltpu.VMEM((4, 4, tok, s), BF16) for s in sizes],
                *[pltpu.VMEM((4, 8, 4, slots, s), BF16) for s in sizes],
                pltpu.VMEM((2, 4, 4, 4, slots, width), BF16),
                *[pltpu.VMEM((4, 4, 8, slots, s), BF16) for s in back],
                *[pltpu.VMEM((4, 4, 8, slots, s), BF16) for s in back],
                *[pltpu.VMEM((3, tok, s), F32) for s in back],
                *[pltpu.VMEM((3, tok, s), F32) for s in back],
                pltpu.VMEM((2 * top, tok), F32),
                pltpu.VMEM((3, 16, 2 * top, tok), F32),
                pltpu.VMEM((32, tok), F32),
                pltpu.VMEM((12, 3 * tok, 32 * slots), BF16),
                pltpu.VMEM((4, 8, N), F32),
                pltpu.VMEM((8, 4, 8, N), F32),
                pltpu.VMEM((1, N), F32),
                pltpu.VMEM((tok, width), F32),
                dma((2,)), dma((3,)), dma((3,)), dma((3, 16)), dma, dma, pltpu.SemaphoreType.REGULAR, dma((3,)), dma((3,)), dma((3, 16)),
                dma((3,)), dma((3, 8)), dma((3,)), dma((3, 8)), dma((3,)), dma((3, 3)), dma((3,)), dma((3, 4)),
            ],
            compiler_params=pltpu.CompilerParams(collective_id=0, has_side_effects=True, vmem_limit_bytes=67043328),
            name='expert_layer',
        )(tokens, expert_ids.T, gate_weights.T, w_in.reshape(width, ff), w_out.reshape(ff, width))

    token_spec = P(('data', 'row', 'col'), None)
    expert_spec = P(GRID_AXES, None, None)
    return jax.shard_map(device_fn, mesh=mesh, in_specs=(token_spec, token_spec, token_spec, expert_spec, expert_spec), out_specs=token_spec, check_vma=False)
```
